32 devices in a mesh: shard: 4 (over y, x), replica: 8 (over z, core).
Axes of the slice: x: 2, y: 2, z: 4, core: 2. Of those that a mesh axis runs over, the one named last changes fastest.
Arguments:
- tokens: bfloat16 [8192, 1536], P(('shard', 'replica')), may hold values from -6 to 6
- cotangent: bfloat16 [8192, 1536], P(('shard', 'replica')), may hold values from -6 to 6
- seq_lengths: int32 [64], replicated, may hold values from 0 to 256, as said below
- seq_device: int32 [64], replicated, may hold values from 0 to 31
- seq_offsets: int32 [64], replicated, may hold values from 0 to 1
- norm_attn: bfloat16 [1, 1536], P(None, 'shard'), may hold values from 0.5 to 1.5
- w_qkv: bfloat16 [1, 1536, 3072], P(None, 'shard'), may hold values from -0.15625 to 0.15625
- w_out: bfloat16 [1, 1536, 1536], P(None, 'shard'), may hold values from -0.625 to 0.625
- norm_mlp: bfloat16 [1, 1536], P(None, 'shard'), may hold values from 0.5 to 1.5
- w_gate_up: bfloat16 [1, 1536, 8192], P(None, 'shard'), may hold values from -0.15625 to 0.15625
- w_down: bfloat16 [1, 4096, 1536], P(None, 'shard'), may hold values from -0.125 to 0.125
Outputs:
- result: bfloat16 [8192, 1536], P(('shard', 'replica'))
- grad_tokens: float32 [8192, 1536], P(('shard', 'replica'))
- grad_norm_attn: float32 [1, 1536], P(None, 'shard')
- grad_w_qkv: float32 [1, 1536, 3072], P(None, 'shard')
- grad_w_out: float32 [1, 1536, 1536], P(None, 'shard')
- grad_norm_mlp: float32 [1, 1536], P(None, 'shard')
- grad_w_gate_up: float32 [1, 1536, 8192], P(None, 'shard')
- grad_w_down: float32 [1, 4096, 1536], P(None, 'shard')
The draws below stay inside these ranges and needn't reach their ends.
Inputs may be any that keep to these rules, and one draw needn't show every extreme that they name: `seq_lengths`: each device is named by exactly 2 entries. A sequence lies within blocks 2p and 2p + 1 of its device for some p; sequences of one device never share a row; length 0 marks an unused entry. In every draw some device is full, its every pair of blocks holding one sequence of length 256.
All inputs are finite; a program needn't handle non-finite values.
Results may differ from the reference program's by a relative error of at most 0.02.
Values may be sent and summed in bfloat16 or wider, within the bound.
A program may use at most 320 MiB of HBM per device.

```python
import math
import jax
import jax.numpy as jnp
from jax import lax

D = 1536
HEADS = 16
KV_HEADS = 8
HEAD = 96
FF = 4096
LAYERS = 1
BLOCK = 128
BLK_DEV = 2
TOKENS = 8192
N_SHARD = 4
N_REPLICA = 8


def sequence_plan(key):
    devices = N_SHARD * N_REPLICA
    pairs = BLK_DEV // 2
    base_key = jax.random.fold_in(key, 4099)
    keys_list = jax.random.split(base_key, 5)
    order = jax.random.permutation(keys_list[0], devices).astype(jnp.int32)
    kind = jax.random.randint(keys_list[1], (devices, pairs), 0, 4)
    longer = jax.random.randint(keys_list[2], (devices, pairs), BLOCK + 1, 2 * BLOCK + 1)
    shorter = jax.random.randint(keys_list[3], (devices, pairs, 2), 1, BLOCK + 1)
    side = jax.random.randint(keys_list[4], (devices, pairs), 0, 2)
    first_group = (jnp.arange(devices) == 0)[:, None]
    kind = jnp.where(first_group, 0, kind)
    longer = jnp.where(first_group, 2 * BLOCK, longer)
    first_len = jnp.where(kind <= 1, longer, shorter[..., 0])
    second_len = jnp.where(kind == 3, shorter[..., 1], 0)
    pair_base = 2 * jnp.arange(pairs, dtype=jnp.int32)[None, :]
    first_off = pair_base + jnp.where(kind == 2, side, 0)
    second_off = jnp.broadcast_to(pair_base + 1, kind.shape)
    lengths = jnp.stack([first_len, second_len], axis=-1).reshape(-1).astype(jnp.int32)
    offsets = jnp.stack([first_off, second_off], axis=-1).reshape(-1).astype(jnp.int32)
    owners = jnp.broadcast_to(order[:, None], (devices, BLK_DEV)).reshape(-1).astype(jnp.int32)
    return (lengths, owners, offsets)


def draw_seq_lengths(key, part):
    return sequence_plan(key)[0]


def draw_seq_device(key, part):
    return sequence_plan(key)[1]


def draw_seq_offsets(key, part):
    return sequence_plan(key)[2]


def strengthened(entries, key, source, target, blocks, factor):
    def block_of(dim):
        return (jnp.arange(entries.shape[dim]) // (entries.shape[dim] // blocks)).reshape((-1,) + (1,) * (entries.ndim - 1 - dim))

    one_side = jax.random.permutation(key, blocks)[block_of(target)]
    other_side = (block_of(target) + blocks // 2) % blocks
    return jnp.where((block_of(source) == one_side) | (block_of(source) == other_side), factor * entries, entries)


def level_of(rng, dims, pieces, low, top_value):
    gain, own = 1.0, jax.random.fold_in(rng, 6)
    for dim, blocks in pieces:
        steps = jnp.exp(jax.random.uniform(jax.random.fold_in(own, dim), (blocks,), jnp.float32, low / len(pieces), top_value / len(pieces)))
        gain = gain * jnp.repeat(steps, dims[dim] // blocks).reshape([-1 if axis == dim else 1 for axis in range(len(dims))])
    return gain


def noise(rng, shape, scale, bound, shards=(), kind=jnp.bfloat16):
    level = level_of(rng, shape, shards, -0.22, 0.18) if shards else 1.0
    values = jax.random.normal(rng, shape, jnp.float32) * scale * level
    return jnp.minimum(jnp.maximum(values, -bound), bound).astype(kind)


def noise_with(rng, dims, scale, most, cuts, heavy, held_as=jnp.bfloat16):
    drawn = scale * jax.random.normal(rng, dims, jnp.float32)
    if cuts:
        drawn = drawn * level_of(rng, dims, cuts, -0.22, 0.18)
    return jnp.clip(strengthened(drawn, jax.random.fold_in(rng, 3), *heavy), -most, most).astype(held_as)


def setup_inputs(seed: int = 0) -> dict:
    arg_keys = jax.random.split(jax.random.key(seed), 12)
    tokens = noise(arg_keys[0], (TOKENS, D), 1.0, 6.0, ((0, 32),))
    cotangent = noise_with(arg_keys[1], (TOKENS, D), 1.0, 6.0, ((0, 32),), (0, 1, 32, 2.75))
    seq_lengths = draw_seq_lengths(jax.random.fold_in(arg_keys[11], 71), 0)
    seq_device = draw_seq_device(jax.random.fold_in(arg_keys[11], 71), 0)
    seq_offsets = draw_seq_offsets(jax.random.fold_in(arg_keys[11], 71), 0)
    norm_attn = jnp.clip(1.0 + 0.1 * jax.random.normal(arg_keys[5], (LAYERS, D), jnp.float32), 0.5, 1.5).astype(jnp.bfloat16)
    w_qkv = noise(arg_keys[6], (LAYERS, D, (HEADS + 2 * KV_HEADS) * HEAD), D ** -0.5, 0.15625, ((1, 4),))
    w_out = noise(arg_keys[7], (LAYERS, HEADS * HEAD, D), (HEADS * HEAD // 16) ** -0.5, 0.625, ((1, 4),))
    norm_mlp = jnp.clip(1.0 + 0.1 * jax.random.normal(arg_keys[8], (LAYERS, D), jnp.float32), 0.5, 1.5).astype(jnp.bfloat16)
    w_gate_up = noise(arg_keys[9], (LAYERS, D, 2 * FF), D ** -0.5, 0.15625, ((1, 4),))
    w_down = noise(arg_keys[10], (LAYERS, FF, D), (FF // 2) ** -0.5, 0.125, ((1, 4),))
    return {"tokens": tokens, "cotangent": cotangent, "seq_lengths": seq_lengths, "seq_device": seq_device, "seq_offsets": seq_offsets, "norm_attn": norm_attn, "w_qkv": w_qkv, "w_out": w_out, "norm_mlp": norm_mlp, "w_gate_up": w_gate_up, "w_down": w_down}


epsilon = 1e-05
rope_base = 100000.0
highest = lax.Precision.HIGHEST

@jax.custom_vjp
def low(v):
    return lax.optimization_barrier(v.astype(jnp.bfloat16)).astype(jnp.float32)

@jax.custom_vjp
def low_back(v):
    return v

def low_keep(v):
    return (low(v), None)

def low_pass(kept, grad):
    return (grad,)

def back_keep(v):
    return (v, None)

def back_low(kept, grad):
    return (low(grad),)
low.defvjp(low_keep, low_pass)
low_back.defvjp(back_keep, back_low)

def rms_scale(field):
    return lax.rsqrt(lax.optimization_barrier(jnp.mean(field * field, axis=-1, keepdims=True)) + epsilon)

def rotate(field):
    half = field.shape[-1] // 2
    return jnp.concatenate([-field[..., half:], field[..., :half]], axis=-1)

def rope_tables(position):
    half = HEAD // 2
    freqs = rope_base ** (-(jnp.arange(half, dtype=jnp.float32) * 2.0) / HEAD)
    angles = position.astype(jnp.float32)[:, None] * freqs[None, :]
    cosine = jnp.cos(angles)
    sine = jnp.sin(angles)
    return (jnp.concatenate([cosine, cosine], axis=-1), jnp.concatenate([sine, sine], axis=-1))

def locate(owner, local, seq_lengths, seq_device, seq_offsets):
    starts = seq_offsets * BLOCK
    labels = jnp.arange(seq_lengths.shape[0], dtype=jnp.int32)
    hits = (seq_device[None, :] == owner[:, None]) & (local[:, None] >= starts[None, :]) & (local[:, None] < (starts + seq_lengths)[None, :])
    segment = lax.optimization_barrier(jnp.max(jnp.where(hits, labels[None, :], -1), axis=1))
    begin = lax.optimization_barrier(jnp.sum(jnp.where(hits, starts[None, :], 0), axis=1))
    return (segment, local - begin)

def attend(queries, keys, values, segment):
    scores = jnp.einsum('qkgd,pkd->kgqp', queries, keys, precision=highest) * HEAD ** (-0.5)
    scores = low_back(scores)
    index = jnp.arange(segment.shape[0], dtype=jnp.int32)
    allowed = (segment[:, None] == segment[None, :]) & (index[None, :] <= index[:, None])
    scores = jnp.where(allowed, scores, -1e+30)
    top = lax.optimization_barrier(jnp.max(scores, axis=-1, keepdims=True))
    total = jnp.log(lax.optimization_barrier(jnp.sum(jnp.exp(scores - top), axis=-1, keepdims=True))) + top
    weights = low(jnp.exp(scores - total))
    return jnp.einsum('kgqp,pkd->qkgd', weights, values, precision=highest)

def layer_forward(field, params, segment, cosine, sine, groups, rows_dev):
    gain_attn, w_project, w_output, gain_mlp, w_gateup, w_lower = params
    rows_all = field.shape[0]
    width_q = HEADS * HEAD
    width_k = KV_HEADS * HEAD
    per = HEADS // KV_HEADS
    normed = low(field * rms_scale(field) * gain_attn[None, :])
    project = low_back(jnp.dot(normed, w_project, precision=highest))
    queries = project[:, :width_q].reshape(rows_all, HEADS, HEAD)
    keys = project[:, width_q:width_q + width_k].reshape(rows_all, KV_HEADS, HEAD)
    values = project[:, width_q + width_k:].reshape(rows_all, KV_HEADS, HEAD)
    queries = low(queries * cosine[:, None, :] + rotate(queries) * sine[:, None, :])
    keys = low(keys * cosine[:, None, :] + rotate(keys) * sine[:, None, :])
    values = low(values)
    queries = queries.reshape(groups, rows_dev, KV_HEADS, per, HEAD)
    keys = keys.reshape(groups, rows_dev, KV_HEADS, HEAD)
    values = values.reshape(groups, rows_dev, KV_HEADS, HEAD)
    segments = segment.reshape(groups, rows_dev)
    checked = jax.checkpoint(attend)
    mixed = lax.map(lambda part: checked(part[0], part[1], part[2], part[3]), (queries, keys, values, segments))
    mixed = low(low_back(mixed.reshape(rows_all, width_q)))
    field = field + low_back(jnp.dot(mixed, w_output, precision=highest))
    normed = low(field * rms_scale(field) * gain_mlp[None, :])
    gate_up = low_back(jnp.dot(normed, w_gateup, precision=highest))
    hidden = low(jax.nn.silu(gate_up[:, :FF]) * gate_up[:, FF:])
    return field + low_back(jnp.dot(hidden, w_lower, precision=highest))

def forward(field, params, segment, cosine, sine, live, groups, rows_dev):
    for layer in range(LAYERS):
        layer_params = tuple((weight[layer] for weight in params))
        field = layer_forward(field, layer_params, segment, cosine, sine, groups, rows_dev)
    return field * live[:, None]

def reference(tokens, cotangent, seq_lengths, seq_device, seq_offsets, norm_attn, w_qkv, w_out, norm_mlp, w_gate_up, w_down):
    devices = N_SHARD * N_REPLICA
    rows_dev = BLK_DEV * BLOCK
    groups = math.gcd(devices, max(1, 4096 // rows_dev))
    count = devices // groups
    span = groups * rows_dev
    params = (norm_attn.astype(jnp.float32), w_qkv.astype(jnp.float32), w_out.astype(jnp.float32), norm_mlp.astype(jnp.float32), w_gate_up.astype(jnp.float32), w_down.astype(jnp.float32))

    def one_group(carry, group_index):
        first = group_index * span
        field = lax.dynamic_slice_in_dim(tokens, first, span, 0).astype(jnp.float32)
        upstream = lax.dynamic_slice_in_dim(cotangent, first, span, 0).astype(jnp.float32)
        flat = jnp.arange(span, dtype=jnp.int32)
        owner = group_index * groups + flat // rows_dev
        local = flat % rows_dev
        segment, position = locate(owner, local, seq_lengths, seq_device, seq_offsets)
        live = (segment >= 0).astype(jnp.float32)
        cosine, sine = rope_tables(position)

        def run(field_in, weights):
            return forward(field_in, weights, segment, cosine, sine, live, groups, rows_dev)
        output, pullback = jax.vjp(run, field, params)
        grad_field, grad_params = pullback(upstream * live[:, None])
        carry = jax.tree.map(jnp.add, carry, grad_params)
        return (carry, (output.astype(jnp.bfloat16), grad_field))
    zeros = jax.tree.map(jnp.zeros_like, params)
    totals, outputs = lax.scan(one_group, zeros, jnp.arange(count, dtype=jnp.int32))
    result = outputs[0].reshape(-1, D)
    grad_tokens = outputs[1].reshape(-1, D)
    return (result, grad_tokens, totals[0], totals[1], totals[2], totals[3], totals[4], totals[5])
```

```python
import functools

import jax
import jax.numpy as jnp
from jax import lax
from jax.experimental import pallas as pl
from jax.experimental.pallas import tpu as pltpu
from jax.sharding import PartitionSpec as P

HEADS = 16
KV_HEADS = 8
HEAD = 96
FF = 4096
BLOCK = 128


epsilon = 1e-05
rope_base = 100000.0


def rms_scale(field):
    return lax.rsqrt(jnp.mean(field * field, axis=-1, keepdims=True) + epsilon)


def rotate(field):
    half = field.shape[-1] // 2
    return jnp.concatenate([-field[..., half:], field[..., :half]], axis=-1)


def rope_tables(position):
    half = HEAD // 2
    freqs = rope_base ** (-(jnp.arange(half, dtype=jnp.float32) * 2.0) / HEAD)
    angles = position.astype(jnp.float32)[:, None] * freqs[None, :]
    cosine = jnp.cos(angles)
    sine = jnp.sin(angles)
    return (jnp.concatenate([cosine, cosine], axis=-1), jnp.concatenate([sine, sine], axis=-1))


def locate(device, seq_lengths, seq_device, seq_offsets, rows):
    starts = seq_offsets * BLOCK
    local = jnp.arange(rows, dtype=jnp.int32)
    labels = jnp.arange(seq_lengths.shape[0], dtype=jnp.int32)
    hits = (
        (seq_device[None, :] == device)
        & (local[:, None] >= starts[None, :])
        & (local[:, None] < (starts + seq_lengths)[None, :])
    )
    segment = jnp.max(jnp.where(hits, labels[None, :], -1), axis=1)
    begin = jnp.sum(jnp.where(hits, starts[None, :], 0), axis=1)
    return (segment, local - begin)


def mask_of(segment):
    local = jnp.arange(segment.shape[0], dtype=jnp.int32)
    return (segment[:, None] == segment[None, :]) & (local[None, :] <= local[:, None])


def mul(left, right):
    return jnp.dot(left, right, preferred_element_type=jnp.float32)


def contract_rows(left, right):
    return lax.dot_general(
        left, right, (((0,), (0,)), ((), ())), preferred_element_type=jnp.float32
    )


def contract_cols(left, right):
    return lax.dot_general(
        left, right, (((1,), (1,)), ((), ())), preferred_element_type=jnp.float32
    )


def norm_rows(field, gain):
    scale = rms_scale(field)
    normed = (field * scale * gain.astype(jnp.float32)[None, :]).astype(jnp.bfloat16)
    return (scale, normed)


def norm_back(grad_normed, field, scale, gain):
    normed = field * scale
    grad_gain = jnp.sum(grad_normed * normed, axis=0)
    inner = grad_normed * gain[None, :]
    grad_field = scale * (inner - normed * jnp.mean(inner * normed, axis=-1, keepdims=True))
    return (grad_field, grad_gain)


def split_project(project, q_heads, k_heads, cosine, sine):
    rows = project.shape[0]
    width_q = q_heads * HEAD
    width_k = k_heads * HEAD
    queries = project[:, :width_q].reshape(rows, q_heads, HEAD)
    keys = project[:, width_q : width_q + width_k].reshape(rows, k_heads, HEAD)
    values_b = project[:, width_q + width_k :].reshape(rows, k_heads, HEAD).astype(jnp.bfloat16)
    queries_b = (queries * cosine[:, None, :] + rotate(queries) * sine[:, None, :]).astype(
        jnp.bfloat16
    )
    keys_b = (keys * cosine[:, None, :] + rotate(keys) * sine[:, None, :]).astype(jnp.bfloat16)
    return (queries_b, keys_b, values_b)


def join_grads(grad_queries, grad_keys, grad_values, cosine, sine):
    rows = grad_queries.shape[0]
    grad_queries = grad_queries * cosine[:, None, :] - rotate(grad_queries * sine[:, None, :])
    grad_keys = grad_keys * cosine[:, None, :] - rotate(grad_keys * sine[:, None, :])
    return jnp.concatenate(
        [
            grad_queries.reshape(rows, -1),
            grad_keys.reshape(rows, -1),
            grad_values.reshape(rows, -1),
        ],
        axis=1,
    ).astype(jnp.bfloat16)


def attention_scores(queries_b, keys_b, allowed):
    rows = queries_b.shape[0]
    kv_count = keys_b.shape[1]
    grouped = queries_b.reshape(rows, kv_count, queries_b.shape[1] // kv_count, HEAD)
    scores = jnp.einsum(
        "qkgd,pkd->kgqp", grouped, keys_b, preferred_element_type=jnp.float32
    ) * HEAD ** (-0.5)
    return jnp.where(allowed, scores, -1e30)


def attend_forward(queries_b, keys_b, values_b, allowed):
    rows = queries_b.shape[0]
    scores = attention_scores(queries_b, keys_b, allowed)
    top = jnp.max(scores, axis=-1, keepdims=True)
    total = jnp.log(jnp.sum(jnp.exp(scores - top), axis=-1, keepdims=True)) + top
    weights_b = jnp.exp(scores - total).astype(jnp.bfloat16)
    mixed = jnp.einsum("kgqp,pkd->qkgd", weights_b, values_b, preferred_element_type=jnp.float32)
    return (mixed.reshape(rows, -1).astype(jnp.bfloat16), total)


def attend_backward(grad_mixed_b, queries_b, keys_b, values_b, total, allowed):
    rows = queries_b.shape[0]
    q_heads = queries_b.shape[1]
    kv_count = keys_b.shape[1]
    per = q_heads // kv_count
    factor = HEAD ** (-0.5)
    grad_mixed = grad_mixed_b.reshape(rows, kv_count, per, HEAD)
    weights = jnp.exp(attention_scores(queries_b, keys_b, allowed) - total)
    weights_b = weights.astype(jnp.bfloat16)
    grad_values = jnp.einsum(
        "kgqp,qkgd->pkd", weights_b, grad_mixed, preferred_element_type=jnp.float32
    )
    grad_weights = jnp.einsum(
        "qkgd,pkd->kgqp", grad_mixed, values_b, preferred_element_type=jnp.float32
    )
    grad_scores = weights * (grad_weights - jnp.sum(weights * grad_weights, axis=-1, keepdims=True))
    grad_scores_b = grad_scores.astype(jnp.bfloat16)
    grouped = queries_b.reshape(rows, kv_count, per, HEAD)
    grad_queries = jnp.einsum(
        "kgqp,pkd->qkgd", grad_scores_b, keys_b, preferred_element_type=jnp.float32
    )
    grad_queries = grad_queries.reshape(rows, q_heads, HEAD) * factor
    grad_keys = (
        jnp.einsum("kgqp,qkgd->pkd", grad_scores_b, grouped, preferred_element_type=jnp.float32)
        * factor
    )
    return (grad_queries, grad_keys, grad_values)


def gate_back(grad_hidden, gate, upper):
    sigma = jax.nn.sigmoid(gate)
    grad_gate = grad_hidden * upper * sigma * (1.0 + gate * (1.0 - sigma))
    grad_upper = grad_hidden * (gate * sigma)
    return (grad_gate.astype(jnp.bfloat16), grad_upper.astype(jnp.bfloat16))


class Group:
    def __init__(self, n_shard, n_replica):
        self.n_shard = n_shard
        self.n_replica = n_replica
        self.replica = lax.axis_index("replica")
        self.core = self.replica % 2
        self.pair = (self.replica // 2) % 2

    def swap(self, array, bit):
        return lax.ppermute(
            array, "replica", [(i, i ^ bit) for i in range(self.n_replica)]
        )

    def split(self, array):
        half = array.shape[1] // 2
        keep = lax.dynamic_slice_in_dim(array, self.core * half, half, 1)
        send = lax.dynamic_slice_in_dim(array, (1 - self.core) * half, half, 1)
        return keep, send

    def both(self, array):
        return jnp.concatenate([array, self.swap(array, 1)], axis=0)

    def both_half(self, array):
        keep, send = self.split(array)
        return jnp.concatenate([keep, self.swap(send, 1)], axis=0)

    def reduce(self, grad):
        owned = lax.psum_scatter(grad, "shard", scatter_dimension=0, tiled=True)
        rows = owned.shape[0] // 2
        keep = lax.dynamic_slice_in_dim(owned, self.pair * rows, rows, 0)
        send = lax.dynamic_slice_in_dim(owned, (1 - self.pair) * rows, rows, 0)
        part = keep + self.swap(send, 2)
        bit = 4
        while bit < self.n_replica:
            part = part + self.swap(part, bit)
            bit *= 2
        other = self.swap(part, 2)
        half = jnp.where(
            self.pair == 0,
            jnp.concatenate([part, other], axis=0),
            jnp.concatenate([other, part], axis=0),
        )
        across = self.swap(half, 1)
        return jnp.where(
            self.core == 0,
            jnp.concatenate([half, across], axis=1),
            jnp.concatenate([across, half], axis=1),
        ).astype(jnp.float32)


MESH = pl.DeviceIdType.MESH


def submasks(order, step):
    masks = [0]
    for bit in order[:step]:
        masks += [mask | bit for mask in masks]
    return masks


def greet(partners):
    barrier = pltpu.get_barrier_semaphore()
    for partner in partners:
        pl.semaphore_signal(barrier, inc=1, device_id=partner, device_id_type=MESH)
    pl.semaphore_wait(barrier, len(partners))


class Item:
    def __init__(self, n_shard, own, full, cols, single, sems):
        self.shard, replica = lax.axis_index("shard"), lax.axis_index("replica")
        self.replica = replica
        core, pair = lax.rem(replica, 2), lax.rem(replica // 2, 2)
        self.bits = [1 << i for i in range(n_shard.bit_length() - 1)]
        self.n_shard = n_shard
        self.own, self.full, self.cols = own, full, cols
        self.rows = own.shape[0]
        self.load_sem, self.local_sem, self.send_sem, self.recv_sem = sems
        half = self.rows // 2
        common = half - 2 * single
        base = core * half
        self.parts = [
            (base + pair * (single + common), single, self.bits),
            (base + single, common, self.bits[1:] + self.bits[:1]),
        ]
        self.mate = (base + (1 - pair) * (single + common), single)
        self.half = (base, half)
        self.other_half = ((1 - core) * half, half)
        self.number = {}
        self.waited, self.started = set(), {}

    def index(self, key):
        return self.number.setdefault(key, len(self.number))

    def window(self, mask, span):
        start = pl.multiple_of((self.shard ^ mask) * self.rows + span[0], 16)
        return self.full.at[pl.ds(start, span[1]), self.cols]

    def send(self, key, src, dst, device):
        if key in self.started:
            return
        index = self.index(key)
        copy = pltpu.make_async_remote_copy(
            src_ref=src,
            dst_ref=dst,
            send_sem=self.send_sem.at[index],
            recv_sem=self.recv_sem.at[index],
            device_id=device,
            device_id_type=MESH,
        )
        copy.start()
        self.started[key] = copy

    def landed(self, key, span):
        if key in self.waited:
            return
        self.waited.add(key)
        window = self.window(key[2], span)
        pltpu.make_async_remote_copy(
            src_ref=window,
            dst_ref=window,
            send_sem=self.send_sem.at[self.index(key)],
            recv_sem=self.recv_sem.at[self.index(key)],
            device_id={"replica": self.replica ^ 1},
            device_id_type=MESH,
        ).wait_recv()

    def load(self, source):
        self.loading = pltpu.make_async_copy(source.at[:, self.cols], self.own.at[:, self.cols], self.load_sem)
        self.loading.start()

    def over_shard(self, part, step, mask):
        start, size, order = self.parts[part]
        bit = order[step]
        window = self.window(mask, (start, size))
        src = window
        if mask == 0:
            src = self.own.at[pl.ds(pl.multiple_of(start, 16), size), self.cols]
        self.send(("shard", part, mask | bit), src, window, {"shard": self.shard ^ bit})

    def first(self):
        self.loading.wait()
        for step in range(len(self.bits)):
            for part in range(2):
                self.over_shard(part, step, 0)
        start = pl.multiple_of(self.shard * self.rows, 16)
        self.placing = pltpu.make_async_copy(
            self.own.at[:, self.cols], self.full.at[pl.ds(start, self.rows), self.cols], self.local_sem
        )
        self.placing.start()

    def arrive(self, part, mask):
        span = self.parts[part][:2]
        self.landed(("shard", part, mask), span)
        if part == 0:
            window = self.window(mask, span)
            self.send(("pair", 0, mask), window, window, {"replica": self.replica ^ 2})

    def relay(self):
        for step in range(1, len(self.bits)):
            for part in range(2):
                for mask in submasks(self.parts[part][2], step)[1:]:
                    self.arrive(part, mask)
                    self.over_shard(part, step, mask)

    def pass_on(self):
        for mask in range(1, self.n_shard):
            self.arrive(0, mask)

    def across(self):
        for mask in range(1, self.n_shard):
            self.arrive(1, mask)
            self.landed(("pair", 0, mask), self.mate)
            window = self.window(mask, self.half)
            self.send(("core", 0, mask), window, window, {"replica": self.replica ^ 1})

    def finish(self):
        for mask in range(1, self.n_shard):
            self.landed(("core", 0, mask), self.other_half)
        for copy in self.started.values():
            copy.wait_send()
        self.placing.wait()


def round_to(value, unit):
    return max(unit, int(value / unit + 0.5) * unit)


def gather_kernel(n_shard, n_weights, plan, *refs):
    weights, gain = refs[:n_weights], refs[n_weights]
    fulls, gains = refs[n_weights + 1 : 2 * n_weights + 1], refs[2 * n_weights + 1]
    owns = refs[2 * n_weights + 2 : 3 * n_weights + 2]
    load_sem, local_sem, send_sem, recv_sem, gain_send, gain_recv, gain_sem = refs[3 * n_weights + 2 :]
    shard, replica = lax.axis_index("shard"), lax.axis_index("replica")
    items = []
    for n, (weight, start, size, single) in enumerate(plan):
        item = Item(
            n_shard,
            owns[weight],
            fulls[weight],
            pl.ds(start, size),
            single,
            (load_sem.at[n], local_sem.at[n], send_sem.at[n], recv_sem.at[n]),
        )
        item.load(weights[weight])
        items.append(item)
    gain_own = pltpu.make_async_copy(gain, gains.at[shard], gain_sem)
    gain_own.start()
    greet(
        [{"shard": shard ^ mask} for mask in range(1, n_shard)]
        + [{"replica": replica ^ 1}, {"replica": replica ^ 2}]
    )
    phases = [Item.first, Item.relay, Item.pass_on, Item.across, Item.finish]
    gain_copies = []
    for time in range(len(items) + len(phases) - 1):
        for late, phase in enumerate(phases):
            if 0 <= time - late < len(items):
                phase(items[time - late])
        if time == 0:
            for mask in range(1, n_shard):
                copy = pltpu.make_async_remote_copy(
                    src_ref=gain,
                    dst_ref=gains.at[shard],
                    send_sem=gain_send.at[mask - 1],
                    recv_sem=gain_recv.at[mask - 1],
                    device_id={"shard": shard ^ mask},
                    device_id_type=MESH,
                )
                copy.start()
                gain_copies.append(copy)
    for mask, copy in enumerate(gain_copies, 1):
        copy.wait_send()
        pltpu.make_async_remote_copy(
            src_ref=gain,
            dst_ref=gains.at[shard ^ mask],
            send_sem=gain_send.at[mask - 1],
            recv_sem=gain_recv.at[mask - 1],
            device_id={"shard": shard ^ mask},
            device_id_type=MESH,
        ).wait_recv()
    gain_own.wait()


def gather_all(n_shard, weights, gain):
    def single(weight, share):
        return round_to(weight.shape[0] // 2 * share, 16)

    qkv, out, gate_up, down = weights
    wide = gate_up.shape[1] // 2
    plan = [
        (2, 0, wide, single(gate_up, 0.25)),
        (2, wide, wide, single(gate_up, 0.25)),
        (3, 0, down.shape[1], single(down, 0.25)),
        (0, 0, qkv.shape[1], single(qkv, 0.333)),
        (1, 0, out.shape[1], single(out, 0.333)),
    ]
    copies = 4 * (n_shard - 1)
    n = len(plan)
    anywhere = pl.BlockSpec(memory_space=pl.ANY)
    return pl.pallas_call(
        functools.partial(gather_kernel, n_shard, len(weights), plan),
        out_shape=[
            jax.ShapeDtypeStruct((w.shape[0] * n_shard, w.shape[1]), w.dtype) for w in weights
        ]
        + [jax.ShapeDtypeStruct((n_shard,) + gain.shape, gain.dtype)],
        in_specs=[anywhere] * (len(weights) + 1),
        out_specs=[anywhere] * (len(weights) + 1),
        scratch_shapes=[pltpu.VMEM(w.shape, w.dtype) for w in weights]
        + [
            pltpu.SemaphoreType.DMA((n,)),
            pltpu.SemaphoreType.DMA((n,)),
            pltpu.SemaphoreType.DMA((n, copies)),
            pltpu.SemaphoreType.DMA((n, copies)),
            pltpu.SemaphoreType.DMA((n_shard - 1,)),
            pltpu.SemaphoreType.DMA((n_shard - 1,)),
            pltpu.SemaphoreType.DMA,
        ],
        compiler_params=pltpu.CompilerParams(collective_id=1, has_side_effects=True),
        name="gather_weights",
    )(*weights, gain)


def body(
    n_shard,
    n_replica,
    tokens,
    cotangent,
    seq_lengths,
    seq_device,
    seq_offsets,
    norm_attn,
    w_qkv,
    w_out,
    norm_mlp,
    w_gate_up,
    w_down,
):
    rows, model = tokens.shape
    group = Group(n_shard, n_replica)
    w_qkv, w_out, w_gate_up, w_down = w_qkv[0], w_out[0], w_gate_up[0], w_down[0]
    owned_rows = w_qkv.shape[0]

    device = lax.axis_index(("shard", "replica"))
    segment, position = locate(device, seq_lengths, seq_device, seq_offsets, rows)
    live = (segment >= 0).astype(jnp.float32)[:, None]
    field = tokens.astype(jnp.float32)
    cosine, sine = rope_tables(position)
    allowed = mask_of(segment)

    w_qkv, w_out, w_gate_up, w_down, gains = gather_all(
        n_shard,
        (w_qkv, w_out, w_gate_up, w_down),
        jnp.concatenate([norm_attn, norm_mlp], axis=0).astype(jnp.float32),
    )
    gains = gains.transpose(1, 0, 2).reshape(2, model)
    gain_attn, gain_mlp = gains[0], gains[1]

    scale_a, normed_a = norm_rows(field, gain_attn)
    project = mul(normed_a, w_qkv)
    queries_b, keys_b, values_b = split_project(project, HEADS, KV_HEADS, cosine, sine)
    mixed, total = attend_forward(queries_b, keys_b, values_b, allowed)
    middle = field + mul(mixed, w_out)
    scale_m, normed_m = norm_rows(middle, gain_mlp)
    pre = mul(normed_m, w_gate_up)
    gate, upper = pre[:, :FF], pre[:, FF:]
    hidden = (jax.nn.silu(gate) * upper).astype(jnp.bfloat16)
    after = middle + mul(hidden, w_down)
    result = (after * live).astype(jnp.bfloat16)

    grad_field = cotangent.astype(jnp.float32) * live
    grad_branch = grad_field.astype(jnp.bfloat16)
    grad_down = group.reduce(
        contract_rows(group.both(hidden), group.both_half(grad_branch)).astype(jnp.bfloat16)
    )
    grad_hidden = contract_cols(grad_branch, w_down)
    grad_pre = jnp.concatenate(gate_back(grad_hidden, gate, upper), axis=1)
    grad_gate_up = group.reduce(
        contract_rows(group.both(normed_m), group.both_half(grad_pre)).astype(jnp.bfloat16)
    )
    grad_input, grad_gain_mlp = norm_back(
        contract_cols(grad_pre, w_gate_up), middle, scale_m, gain_mlp
    )
    grad_middle = grad_field + grad_input

    grad_branch = grad_middle.astype(jnp.bfloat16)
    grad_mixed = contract_cols(grad_branch, w_out).astype(jnp.bfloat16)
    grad_queries, grad_keys, grad_values = attend_backward(
        grad_mixed, queries_b, keys_b, values_b, total, allowed
    )
    grad_project = join_grads(grad_queries, grad_keys, grad_values, cosine, sine)
    grad_qkv = group.reduce(
        contract_rows(group.both(normed_a), group.both_half(grad_project)).astype(jnp.bfloat16)
    )
    grad_out = group.reduce(
        contract_rows(group.both(mixed), group.both_half(grad_branch)).astype(jnp.bfloat16)
    )
    grad_input, grad_gain_attn = norm_back(
        contract_cols(grad_project, w_qkv), field, scale_a, gain_attn
    )
    grad_tokens = grad_middle + grad_input

    gain_sums = lax.psum(jnp.stack([grad_gain_attn, grad_gain_mlp]), ("shard", "replica"))
    gain_own = lax.dynamic_slice_in_dim(
        gain_sums, lax.axis_index("shard") * owned_rows, owned_rows, 1
    )
    return (
        result,
        grad_tokens,
        gain_own[0:1],
        grad_qkv[None],
        grad_out[None],
        gain_own[1:2],
        grad_gate_up[None],
        grad_down[None],
    )


def solution(mesh):
    n_shard = mesh.shape["shard"]
    n_replica = mesh.shape["replica"]
    placed = (
        P(("shard", "replica"), None),
        P(("shard", "replica"), None),
        P(),
        P(),
        P(),
        P(None, "shard"),
        P(None, "shard", None),
        P(None, "shard", None),
        P(None, "shard"),
        P(None, "shard", None),
        P(None, "shard", None),
    )

    def run(*args):
        return body(n_shard, n_replica, *args)

    return jax.shard_map(
        run,
        mesh=mesh,
        in_specs=placed,
        out_specs=(
            P(("shard", "replica"), None),
            P(("shard", "replica"), None),
            P(None, "shard"),
            P(None, "shard", None),
            P(None, "shard", None),
            P(None, "shard"),
            P(None, "shard", None),
            P(None, "shard", None),
        ),
        check_vma=False,
    )
```

```python
import functools

import jax
import jax.numpy as jnp
from jax import lax
from jax.experimental import pallas as pl
from jax.experimental.pallas import tpu as pltpu
from jax.sharding import PartitionSpec as P

HEADS = 16
KV_HEADS = 8
HEAD = 96
FF = 4096
BLOCK = 128

epsilon = 1e-05
rope_base = 100000.0


def rms_scale(field):
    return lax.rsqrt(jnp.mean(field * field, axis=-1, keepdims=True) + epsilon)


def rotate(field):
    half = field.shape[-1] // 2
    return jnp.concatenate([-field[..., half:], field[..., :half]], axis=-1)


def rope_tables(position):
    half = HEAD // 2
    freqs = rope_base ** (-(jnp.arange(half, dtype=jnp.float32) * 2.0) / HEAD)
    angles = position.astype(jnp.float32)[:, None] * freqs[None, :]
    cosine = jnp.cos(angles)
    sine = jnp.sin(angles)
    return (jnp.concatenate([cosine, cosine], axis=-1), jnp.concatenate([sine, sine], axis=-1))


def locate(device, seq_lengths, seq_device, seq_offsets, rows):
    starts = seq_offsets * BLOCK
    local = jnp.arange(rows, dtype=jnp.int32)
    labels = jnp.arange(seq_lengths.shape[0], dtype=jnp.int32)
    hits = (
        (seq_device[None, :] == device)
        & (local[:, None] >= starts[None, :])
        & (local[:, None] < (starts + seq_lengths)[None, :])
    )
    segment = jnp.max(jnp.where(hits, labels[None, :], -1), axis=1)
    begin = jnp.sum(jnp.where(hits, starts[None, :], 0), axis=1)
    return (segment, local - begin)


def mask_of(segment):
    local = jnp.arange(segment.shape[0], dtype=jnp.int32)
    return (segment[:, None] == segment[None, :]) & (local[None, :] <= local[:, None])


def mul(left, right):
    return jnp.dot(left, right, preferred_element_type=jnp.float32)


def contract_rows(left, right):
    return lax.dot_general(
        left, right, (((0,), (0,)), ((), ())), preferred_element_type=jnp.float32
    )


def contract_cols(left, right):
    return lax.dot_general(
        left, right, (((1,), (1,)), ((), ())), preferred_element_type=jnp.float32
    )


def norm_rows(field, gain):
    scale = rms_scale(field)
    normed = (field * scale * gain.astype(jnp.float32)[None, :]).astype(jnp.bfloat16)
    return (scale, normed)


def norm_back(grad_normed, field, scale, gain):
    normed = field * scale
    grad_gain = jnp.sum(grad_normed * normed, axis=0)
    inner = grad_normed * gain[None, :]
    grad_field = scale * (inner - normed * jnp.mean(inner * normed, axis=-1, keepdims=True))
    return (grad_field, grad_gain)


def split_project(project, q_heads, k_heads, cosine, sine):
    rows = project.shape[0]
    width_q = q_heads * HEAD
    width_k = k_heads * HEAD
    queries = project[:, :width_q].reshape(rows, q_heads, HEAD)
    keys = project[:, width_q : width_q + width_k].reshape(rows, k_heads, HEAD)
    values_b = project[:, width_q + width_k :].reshape(rows, k_heads, HEAD).astype(jnp.bfloat16)
    queries_b = (queries * cosine[:, None, :] + rotate(queries) * sine[:, None, :]).astype(
        jnp.bfloat16
    )
    keys_b = (keys * cosine[:, None, :] + rotate(keys) * sine[:, None, :]).astype(jnp.bfloat16)
    return (queries_b, keys_b, values_b)


def join_grads(grad_queries, grad_keys, grad_values, cosine, sine):
    rows = grad_queries.shape[0]
    grad_queries = grad_queries * cosine[:, None, :] - rotate(grad_queries * sine[:, None, :])
    grad_keys = grad_keys * cosine[:, None, :] - rotate(grad_keys * sine[:, None, :])
    return jnp.concatenate(
        [
            grad_queries.reshape(rows, -1),
            grad_keys.reshape(rows, -1),
            grad_values.reshape(rows, -1),
        ],
        axis=1,
    ).astype(jnp.bfloat16)


def attention_scores(queries_b, keys_b, allowed):
    rows = queries_b.shape[0]
    kv_count = keys_b.shape[1]
    grouped = queries_b.reshape(rows, kv_count, queries_b.shape[1] // kv_count, HEAD)
    scores = jnp.einsum(
        "qkgd,pkd->kgqp", grouped, keys_b, preferred_element_type=jnp.float32
    ) * HEAD ** (-0.5)
    return jnp.where(allowed, scores, -1e30)


def attend_forward(queries_b, keys_b, values_b, allowed):
    rows = queries_b.shape[0]
    scores = attention_scores(queries_b, keys_b, allowed)
    top = jnp.max(scores, axis=-1, keepdims=True)
    total = jnp.log(jnp.sum(jnp.exp(scores - top), axis=-1, keepdims=True)) + top
    weights_b = jnp.exp(scores - total).astype(jnp.bfloat16)
    mixed = jnp.einsum("kgqp,pkd->qkgd", weights_b, values_b, preferred_element_type=jnp.float32)
    return (mixed.reshape(rows, -1).astype(jnp.bfloat16), total)


def attend_backward(grad_mixed_b, queries_b, keys_b, values_b, total, allowed):
    rows = queries_b.shape[0]
    q_heads = queries_b.shape[1]
    kv_count = keys_b.shape[1]
    per = q_heads // kv_count
    factor = HEAD ** (-0.5)
    grad_mixed = grad_mixed_b.reshape(rows, kv_count, per, HEAD)
    weights = jnp.exp(attention_scores(queries_b, keys_b, allowed) - total)
    weights_b = weights.astype(jnp.bfloat16)
    grad_values = jnp.einsum(
        "kgqp,qkgd->pkd", weights_b, grad_mixed, preferred_element_type=jnp.float32
    )
    grad_weights = jnp.einsum(
        "qkgd,pkd->kgqp", grad_mixed, values_b, preferred_element_type=jnp.float32
    )
    grad_scores = weights * (grad_weights - jnp.sum(weights * grad_weights, axis=-1, keepdims=True))
    grad_scores_b = grad_scores.astype(jnp.bfloat16)
    grouped = queries_b.reshape(rows, kv_count, per, HEAD)
    grad_queries = jnp.einsum(
        "kgqp,pkd->qkgd", grad_scores_b, keys_b, preferred_element_type=jnp.float32
    )
    grad_queries = grad_queries.reshape(rows, q_heads, HEAD) * factor
    grad_keys = (
        jnp.einsum("kgqp,qkgd->pkd", grad_scores_b, grouped, preferred_element_type=jnp.float32)
        * factor
    )
    return (grad_queries, grad_keys, grad_values)


def gate_back(grad_hidden, gate, upper):
    sigma = jax.nn.sigmoid(gate)
    grad_gate = grad_hidden * upper * sigma * (1.0 + gate * (1.0 - sigma))
    grad_upper = grad_hidden * (gate * sigma)
    return (grad_gate.astype(jnp.bfloat16), grad_upper.astype(jnp.bfloat16))


MESH = pl.DeviceIdType.MESH


def submasks(order, step):
    masks = [0]
    for bit in order[:step]:
        masks += [mask | bit for mask in masks]
    return masks


def greet(partners):
    barrier = pltpu.get_barrier_semaphore()
    for partner in partners:
        pl.semaphore_signal(barrier, inc=1, device_id=partner, device_id_type=MESH)
    pl.semaphore_wait(barrier, len(partners))


class Item:
    def __init__(self, n_shard, own, full, cols, single, sems):
        self.shard, replica = lax.axis_index("shard"), lax.axis_index("replica")
        self.replica = replica
        core, pair = lax.rem(replica, 2), lax.rem(replica // 2, 2)
        self.bits = [1 << i for i in range(n_shard.bit_length() - 1)]
        self.n_shard = n_shard
        self.own, self.full, self.cols = own, full, cols
        self.rows = own.shape[0]
        self.load_sem, self.local_sem, self.send_sem, self.recv_sem = sems
        half = self.rows // 2
        common = half - 2 * single
        base = core * half
        self.parts = [
            (base + pair * (single + common), single, self.bits),
            (base + single, common, self.bits[1:] + self.bits[:1]),
        ]
        self.mate = (base + (1 - pair) * (single + common), single)
        self.half = (base, half)
        self.other_half = ((1 - core) * half, half)
        self.number = {}
        self.waited, self.started = set(), {}

    def index(self, key):
        return self.number.setdefault(key, len(self.number))

    def window(self, mask, span):
        start = pl.multiple_of((self.shard ^ mask) * self.rows + span[0], 16)
        return self.full.at[pl.ds(start, span[1]), self.cols]

    def send(self, key, src, dst, device):
        if key in self.started:
            return
        index = self.index(key)
        copy = pltpu.make_async_remote_copy(
            src_ref=src,
            dst_ref=dst,
            send_sem=self.send_sem.at[index],
            recv_sem=self.recv_sem.at[index],
            device_id=device,
            device_id_type=MESH,
        )
        copy.start()
        self.started[key] = copy

    def landed(self, key, span):
        if key in self.waited:
            return
        self.waited.add(key)
        window = self.window(key[2], span)
        pltpu.make_async_remote_copy(
            src_ref=window,
            dst_ref=window,
            send_sem=self.send_sem.at[self.index(key)],
            recv_sem=self.recv_sem.at[self.index(key)],
            device_id={"replica": self.replica ^ 1},
            device_id_type=MESH,
        ).wait_recv()

    def load(self, source):
        self.loading = pltpu.make_async_copy(source.at[:, self.cols], self.own.at[:, self.cols], self.load_sem)
        self.loading.start()

    def over_shard(self, part, step, mask):
        start, size, order = self.parts[part]
        bit = order[step]
        window = self.window(mask, (start, size))
        src = window
        if mask == 0:
            src = self.own.at[pl.ds(pl.multiple_of(start, 16), size), self.cols]
        self.send(("shard", part, mask | bit), src, window, {"shard": self.shard ^ bit})

    def first(self):
        self.loading.wait()
        for step in range(len(self.bits)):
            for part in range(2):
                self.over_shard(part, step, 0)
        start = pl.multiple_of(self.shard * self.rows, 16)
        self.placing = pltpu.make_async_copy(
            self.own.at[:, self.cols], self.full.at[pl.ds(start, self.rows), self.cols], self.local_sem
        )
        self.placing.start()

    def arrive(self, part, mask):
        span = self.parts[part][:2]
        self.landed(("shard", part, mask), span)
        if part == 0:
            window = self.window(mask, span)
            self.send(("pair", 0, mask), window, window, {"replica": self.replica ^ 2})

    def relay(self):
        for step in range(1, len(self.bits)):
            for part in range(2):
                for mask in submasks(self.parts[part][2], step)[1:]:
                    self.arrive(part, mask)
                    self.over_shard(part, step, mask)

    def pass_on(self):
        for mask in range(1, self.n_shard):
            self.arrive(0, mask)

    def across(self):
        for mask in range(1, self.n_shard):
            self.arrive(1, mask)
            self.landed(("pair", 0, mask), self.mate)
            window = self.window(mask, self.half)
            self.send(("core", 0, mask), window, window, {"replica": self.replica ^ 1})

    def finish(self):
        for mask in range(1, self.n_shard):
            self.landed(("core", 0, mask), self.other_half)
        for copy in self.started.values():
            copy.wait_send()
        self.placing.wait()


def round_to(value, unit):
    return max(unit, int(value / unit + 0.5) * unit)


def gather_kernel(n_shard, n_weights, plan, *refs):
    weights, gain = refs[:n_weights], refs[n_weights]
    fulls, gains = refs[n_weights + 1 : 2 * n_weights + 1], refs[2 * n_weights + 1]
    owns = refs[2 * n_weights + 2 : 3 * n_weights + 2]
    load_sem, local_sem, send_sem, recv_sem, gain_send, gain_recv, gain_sem = refs[3 * n_weights + 2 :]
    shard, replica = lax.axis_index("shard"), lax.axis_index("replica")
    items = []
    for n, (weight, start, size, single) in enumerate(plan):
        item = Item(
            n_shard,
            owns[weight],
            fulls[weight],
            pl.ds(start, size),
            single,
            (load_sem.at[n], local_sem.at[n], send_sem.at[n], recv_sem.at[n]),
        )
        item.load(weights[weight])
        items.append(item)
    gain_own = pltpu.make_async_copy(gain, gains.at[shard], gain_sem)
    gain_own.start()
    greet(
        [{"shard": shard ^ mask} for mask in range(1, n_shard)]
        + [{"replica": replica ^ 1}, {"replica": replica ^ 2}]
    )
    phases = [Item.first, Item.relay, Item.pass_on, Item.across, Item.finish]
    gain_copies = []
    for time in range(len(items) + len(phases) - 1):
        for late, phase in enumerate(phases):
            if 0 <= time - late < len(items):
                phase(items[time - late])
        if time == 0:
            for mask in range(1, n_shard):
                copy = pltpu.make_async_remote_copy(
                    src_ref=gain,
                    dst_ref=gains.at[shard],
                    send_sem=gain_send.at[mask - 1],
                    recv_sem=gain_recv.at[mask - 1],
                    device_id={"shard": shard ^ mask},
                    device_id_type=MESH,
                )
                copy.start()
                gain_copies.append(copy)
    for mask, copy in enumerate(gain_copies, 1):
        copy.wait_send()
        pltpu.make_async_remote_copy(
            src_ref=gain,
            dst_ref=gains.at[shard ^ mask],
            send_sem=gain_send.at[mask - 1],
            recv_sem=gain_recv.at[mask - 1],
            device_id={"shard": shard ^ mask},
            device_id_type=MESH,
        ).wait_recv()
    gain_own.wait()


def gather_all(n_shard, weights, gain):
    def single(weight, share):
        return round_to(weight.shape[0] // 2 * share, 16)

    qkv, out, gate_up, down = weights
    wide = gate_up.shape[1] // 2
    plan = [
        (2, 0, wide, single(gate_up, 0.25)),
        (2, wide, wide, single(gate_up, 0.25)),
        (3, 0, down.shape[1], single(down, 0.25)),
        (0, 0, qkv.shape[1], single(qkv, 0.333)),
        (1, 0, out.shape[1], single(out, 0.333)),
    ]
    copies = 4 * (n_shard - 1)
    n = len(plan)
    anywhere = pl.BlockSpec(memory_space=pl.ANY)
    return pl.pallas_call(
        functools.partial(gather_kernel, n_shard, len(weights), plan),
        out_shape=[
            jax.ShapeDtypeStruct((w.shape[0] * n_shard, w.shape[1]), w.dtype) for w in weights
        ]
        + [jax.ShapeDtypeStruct((n_shard,) + gain.shape, gain.dtype)],
        in_specs=[anywhere] * (len(weights) + 1),
        out_specs=[anywhere] * (len(weights) + 1),
        scratch_shapes=[pltpu.VMEM(w.shape, w.dtype) for w in weights]
        + [
            pltpu.SemaphoreType.DMA((n,)),
            pltpu.SemaphoreType.DMA((n,)),
            pltpu.SemaphoreType.DMA((n, copies)),
            pltpu.SemaphoreType.DMA((n, copies)),
            pltpu.SemaphoreType.DMA((n_shard - 1,)),
            pltpu.SemaphoreType.DMA((n_shard - 1,)),
            pltpu.SemaphoreType.DMA,
        ],
        compiler_params=pltpu.CompilerParams(collective_id=1, has_side_effects=True),
        name="gather_weights",
    )(*weights, gain)


SLOTS = 5


class Pipe:
    def __init__(self, n_shard, n_replica, begin, count, block, deliver, bufs, sems):
        self.shard, self.replica = lax.axis_index("shard"), lax.axis_index("replica")
        chip = self.replica // 2
        self.inner = lax.rem(chip, 2) != lax.rem(chip // 2, 2)
        self.steps = n_shard.bit_length() - 1
        self.swaps = [6] + [1 << k for k in range(3, n_replica.bit_length() - 1)]
        self.begin, self.count, self.block, self.deliver = begin, count, block, deliver
        bufs = list(bufs)
        self.out = [bufs.pop(0) for _ in range(self.steps)]
        self.into = [bufs.pop(0) for _ in range(self.steps)]
        self.kept = [bufs.pop(0) for _ in range(max(1, self.steps - 1))]
        self.fold_out, self.fold_in, self.total = bufs.pop(0), bufs.pop(0), bufs.pop(0)
        self.swap_out = [bufs.pop(0) for _ in self.swaps]
        self.swap_in = [bufs.pop(0) for _ in self.swaps]
        self.final, self.across = bufs.pop(0), bufs.pop(0)
        self.send_sem, self.recv_sem, self.local_sem = sems
        self.last = self.steps + 2 + len(self.swaps)

    @staticmethod
    def scratch(n_shard, n_replica, rows, cols, dtype):
        steps = n_shard.bit_length() - 1
        swaps = n_replica.bit_length() - 3
        blocks = [n_shard >> (k + 1) for k in range(steps)]
        shapes = [pltpu.VMEM((SLOTS, b, rows, cols), dtype) for b in blocks * 2]
        shapes += [
            pltpu.VMEM((SLOTS, max(1, b // 2), rows, cols), jnp.float32)
            for b in blocks[: max(1, steps - 1)]
        ]
        one = (SLOTS, rows, cols)
        shapes += [pltpu.VMEM(one, dtype)] * 2 + [pltpu.VMEM(one, jnp.float32)]
        shapes += [pltpu.VMEM(one, dtype)] * (2 * swaps + 2)
        kinds = steps + swaps + 3
        return shapes, [
            pltpu.SemaphoreType.DMA((kinds, SLOTS)),
            pltpu.SemaphoreType.DMA((kinds, SLOTS)),
            pltpu.SemaphoreType.DMA((2, SLOTS)),
        ]

    def bit(self, chunk, step):
        return 1 << lax.rem(step + lax.rem(chunk, 2), self.steps)

    def mask(self, chunk, entry):
        found = 0
        for step in range(self.steps):
            if (entry >> step) & 1:
                found = found | self.bit(chunk, step)
        return found

    def copy(self, kind, slot, src, dst, device):
        return pltpu.make_async_remote_copy(
            src_ref=src.at[slot],
            dst_ref=dst.at[slot],
            send_sem=self.send_sem.at[kind, slot],
            recv_sem=self.recv_sem.at[kind, slot],
            device_id=device,
            device_id_type=MESH,
        )

    def halving(self, step, chunk, slot):
        device = {"shard": self.shard ^ self.bit(chunk, step)}
        return self.copy(step, slot, self.out[step], self.into[step], device)

    def folding(self, slot):
        return self.copy(
            self.steps, slot, self.fold_out, self.fold_in, {"replica": self.replica ^ 2}
        )

    def swapping(self, number, slot):
        device = {"replica": self.replica ^ self.swaps[number]}
        return self.copy(
            self.steps + 1 + number, slot, self.swap_out[number], self.swap_in[number], device
        )

    def unfolding(self, slot):
        kind = self.steps + 1 + len(self.swaps)
        return self.copy(kind, slot, self.final, self.final, {"replica": self.replica ^ 2})

    def crossing(self, slot):
        kind = self.steps + 2 + len(self.swaps)
        return self.copy(kind, slot, self.final, self.across, {"replica": self.replica ^ 1})

    def stage(self, number, chunk, slot):
        steps, swaps = self.steps, len(self.swaps)
        dtype = self.final.dtype
        if number == 0:
            for entry in range(1, 1 << steps, 2):
                self.out[0][slot, entry >> 1] = self.block(chunk, self.mask(chunk, entry)).astype(dtype)
            self.halving(0, chunk, slot).start()
        elif number <= steps:
            sums = []
            for entry in range(1 << (steps - number)):
                if number == 1:
                    sums.append(self.block(chunk, self.mask(chunk, 2 * entry)))
                else:
                    sums.append(self.kept[number - 2][slot, entry])
            self.halving(number - 1, chunk, slot).wait()
            for entry, value in enumerate(sums):
                value = value + self.into[number - 1][slot, entry].astype(jnp.float32)
                if number == steps:
                    @pl.when(self.inner)
                    def _(value=value):
                        self.total[slot] = value

                    @pl.when(jnp.logical_not(self.inner))
                    def _(value=value):
                        self.fold_out[slot] = value.astype(dtype)
                        self.folding(slot).start()
                elif entry & 1:
                    self.out[number][slot, entry >> 1] = value.astype(dtype)
                else:
                    self.kept[number - 1][slot, entry >> 1] = value
            if number < steps:
                self.halving(number, chunk, slot).start()
        elif number == steps + 1:
            @pl.when(self.inner)
            def _():
                self.folding(slot).wait_recv()
                value = self.total[slot] + self.fold_in[slot].astype(jnp.float32)
                self.swap_out[0][slot] = value.astype(dtype)
                self.swapping(0, slot).start()

            @pl.when(jnp.logical_not(self.inner))
            def _():
                self.folding(slot).wait_send()
        elif number <= steps + 1 + swaps:
            @pl.when(self.inner)
            def _():
                done = number - steps - 2
                self.swapping(done, slot).wait()
                value = self.swap_out[done][slot].astype(jnp.float32) + self.swap_in[done][
                    slot
                ].astype(jnp.float32)
                if done + 1 < swaps:
                    self.swap_out[done + 1][slot] = value.astype(dtype)
                    self.swapping(done + 1, slot).start()
                else:
                    self.final[slot] = value.astype(dtype)
                    self.unfolding(slot).start()
        elif number == self.last:
            @pl.when(jnp.logical_not(self.inner))
            def _():
                self.unfolding(slot).wait_recv()

            self.crossing(slot).start()
            self.deliver(chunk, 0, self.final.at[slot], self.local_sem.at[0, slot], True)
        else:
            @pl.when(self.inner)
            def _():
                self.unfolding(slot).wait_send()

            self.crossing(slot).wait()
            self.deliver(chunk, 1, self.across.at[slot], self.local_sem.at[1, slot], True)
            self.deliver(chunk, 0, self.final.at[slot], self.local_sem.at[0, slot], False)
            self.deliver(chunk, 1, self.across.at[slot], self.local_sem.at[1, slot], False)

    def run(self, time):
        for number in range(self.last + 2):
            chunk = time - self.begin - number

            @pl.when((chunk >= 0) & (chunk < self.count))
            def _(number=number, chunk=chunk):
                self.stage(number, chunk, lax.rem(chunk, SLOTS))

    def length(self):
        return self.begin + self.count + self.last + 1


DEEP_COLS = 128
WIDE_COLS = 256


def reduce_kernel(n_shard, n_replica, halves, *refs):
    refs = list(refs)
    take = lambda n: [refs.pop(0) for _ in range(n)]
    lefts, rights, (gain_in,) = take(4), take(4), take(1)
    outs, (gain_out,) = take(4), take(1)
    deep_left, deep_right, wide_left, wide_right = take(4)
    load_sem, pass_send, pass_recv = take(3)
    n_bufs = (len(refs) - 9) // 3
    deep_bufs, deep_sems = take(n_bufs), take(3)
    wide_bufs, wide_sems = take(n_bufs), take(3)
    gain_bufs, gain_sems = take(n_bufs), take(3)
    shard, replica = lax.axis_index("shard"), lax.axis_index("replica")
    core = lax.rem(replica, 2)
    rows = lefts[0].shape[1]
    model = lefts[1].shape[0]
    deep_rows, wide_rows = outs[0].shape[0], outs[1].shape[0]

    place_left = [deep_left] + [wide_left.at[pl.ds(k * model, model)] for k in range(3)]
    starts = [0, 0, halves[1], halves[1] + halves[2]]
    place_right = [
        (deep_right if k == 0 else wide_right).at[:, pl.ds(starts[k], halves[k])] for k in range(4)
    ]
    loads, passes = [], []
    greet(
        [{"shard": shard ^ (1 << k)} for k in range(n_shard.bit_length() - 1)]
        + [{"replica": replica ^ mask} for mask in [1, 2, 6]]
        + [{"replica": replica ^ (1 << k)} for k in range(3, n_replica.bit_length() - 1)]
    )
    for k in range(4):
        mine = pl.ds(pl.multiple_of(core * halves[k], 128), halves[k])
        other = pl.ds(pl.multiple_of((1 - core) * halves[k], 128), halves[k])
        sources = [
            (lefts[k], place_left[k].at[:, pl.ds(0, rows)]),
            (rights[k].at[:, mine], place_right[k].at[pl.ds(0, rows)]),
        ]
        for n, (src, dst) in enumerate(sources):
            loads.append(pltpu.make_async_copy(src, dst, load_sem.at[2 * k + n]))
            loads[-1].start()
        sources = [
            (lefts[k], place_left[k].at[:, pl.ds(rows, rows)]),
            (rights[k].at[:, other], place_right[k].at[pl.ds(rows, rows)]),
        ]
        for n, (src, dst) in enumerate(sources):
            passes.append(
                pltpu.make_async_remote_copy(
                    src_ref=src,
                    dst_ref=dst,
                    send_sem=pass_send.at[2 * k + n],
                    recv_sem=pass_recv.at[2 * k + n],
                    device_id={"replica": replica ^ 1},
                    device_id_type=MESH,
                )
            )
            passes[-1].start()

    def arrived(first, end):
        for k in range(2 * first, 2 * end):
            loads[k].wait()
            passes[k].wait()

    def deep_block(chunk, mask):
        left = deep_left[pl.ds(pl.multiple_of((shard ^ mask) * deep_rows, 16), deep_rows), :]
        right = deep_right[:, pl.ds(pl.multiple_of(chunk * DEEP_COLS, 128), DEEP_COLS)]
        return jnp.dot(left, right, preferred_element_type=jnp.float32)

    bounds = [starts[k] // WIDE_COLS for k in (2, 3)]

    def wide_block(chunk, mask):
        weight = (chunk >= bounds[0]).astype(jnp.int32) + (chunk >= bounds[1]).astype(jnp.int32)
        start = weight * model + (shard ^ mask) * wide_rows
        left = wide_left[pl.ds(pl.multiple_of(start, 16), wide_rows), :]
        right = wide_right[:, pl.ds(pl.multiple_of(chunk * WIDE_COLS, 128), WIDE_COLS)]
        return jnp.dot(left, right, preferred_element_type=jnp.float32)

    def gain_block(chunk, mask):
        return gain_in[shard ^ mask]

    def put(out, start, size, src, sem, begin):
        copy = pltpu.make_async_copy(src, out.at[:, pl.ds(pl.multiple_of(start, 128), size)], sem)
        if begin:
            copy.start()
        else:
            copy.wait()

    def deep_deliver(chunk, side, src, sem, begin):
        half = jnp.where(side == 0, core, 1 - core) * halves[0]
        put(outs[0], half + chunk * DEEP_COLS, DEEP_COLS, src, sem, begin)

    def wide_deliver(chunk, side, src, sem, begin):
        edges = [0] + bounds + [wide_right.shape[1] // WIDE_COLS]
        half = core if side == 0 else 1 - core
        for k in range(3):
            @pl.when((chunk >= edges[k]) & (chunk < edges[k + 1]))
            def _(k=k):
                start = half * halves[k + 1] + (chunk - edges[k]) * WIDE_COLS
                put(outs[k + 1], start, WIDE_COLS, src, sem, begin)

    def gain_deliver(chunk, side, src, sem, begin):
        if side == 1 and begin:
            gain_out[...] = gain_pipe.final[0] + src[...]

    n_deep = halves[0] // DEEP_COLS
    n_wide = wide_right.shape[1] // WIDE_COLS
    size = (n_shard, n_replica)
    deep = Pipe(*size, 0, n_deep, deep_block, deep_deliver, deep_bufs, deep_sems)
    wide = Pipe(*size, n_deep, n_wide, wide_block, wide_deliver, wide_bufs, wide_sems)
    gain_pipe = Pipe(*size, 1, 1, gain_block, gain_deliver, gain_bufs, gain_sems)
    arrived(0, 1)

    def step(time, carry):
        @pl.when(time == n_deep)
        def _():
            arrived(1, 4)

        deep.run(time)
        gain_pipe.run(time)
        wide.run(time)
        return carry

    lax.fori_loop(0, wide.length(), step, 0)


def reduce_all(n_shard, n_replica, lefts, rights, gain_grads):
    rows = lefts[0].shape[1]
    halves = [right.shape[1] // 2 for right in rights]
    owned = [left.shape[0] // n_shard for left in lefts]
    model = lefts[1].shape[0]
    anywhere = pl.BlockSpec(memory_space=pl.ANY)
    whole = pl.BlockSpec(memory_space=pltpu.VMEM)
    size = (n_shard, n_replica)
    deep_bufs, deep_sems = Pipe.scratch(*size, owned[0], DEEP_COLS, jnp.bfloat16)
    wide_bufs, wide_sems = Pipe.scratch(*size, owned[1], WIDE_COLS, jnp.bfloat16)
    gain_bufs, gain_sems = Pipe.scratch(*size, *gain_grads.shape[1:], jnp.float32)
    return pl.pallas_call(
        functools.partial(reduce_kernel, n_shard, n_replica, halves),
        out_shape=[
            jax.ShapeDtypeStruct((own, right.shape[1]), jnp.bfloat16)
            for own, right in zip(owned, rights)
        ]
        + [jax.ShapeDtypeStruct(gain_grads.shape[1:], jnp.float32)],
        in_specs=[anywhere] * 8 + [whole],
        out_specs=[anywhere] * 4 + [whole],
        scratch_shapes=[
            pltpu.VMEM((lefts[0].shape[0], 2 * rows), jnp.bfloat16),
            pltpu.VMEM((2 * rows, halves[0]), jnp.bfloat16),
            pltpu.VMEM((3 * model, 2 * rows), jnp.bfloat16),
            pltpu.VMEM((2 * rows, sum(halves[1:])), jnp.bfloat16),
            pltpu.SemaphoreType.DMA((8,)),
            pltpu.SemaphoreType.DMA((8,)),
            pltpu.SemaphoreType.DMA((8,)),
            *deep_bufs,
            *deep_sems,
            *wide_bufs,
            *wide_sems,
            *gain_bufs,
            *gain_sems,
        ],
        compiler_params=pltpu.CompilerParams(
            collective_id=2, has_side_effects=True, vmem_limit_bytes=66_000_000
        ),
        name="reduce_gradients",
    )(*lefts, *rights, gain_grads)


def body(
    n_shard,
    n_replica,
    tokens,
    cotangent,
    seq_lengths,
    seq_device,
    seq_offsets,
    norm_attn,
    w_qkv,
    w_out,
    norm_mlp,
    w_gate_up,
    w_down,
):
    rows, model = tokens.shape
    w_qkv, w_out, w_gate_up, w_down = w_qkv[0], w_out[0], w_gate_up[0], w_down[0]
    owned_rows = w_qkv.shape[0]

    device = lax.axis_index(("shard", "replica"))
    segment, position = locate(device, seq_lengths, seq_device, seq_offsets, rows)
    live = (segment >= 0).astype(jnp.float32)[:, None]
    field = tokens.astype(jnp.float32)
    cosine, sine = rope_tables(position)
    allowed = mask_of(segment)

    w_qkv, w_out, w_gate_up, w_down, gains = gather_all(
        n_shard,
        (w_qkv, w_out, w_gate_up, w_down),
        jnp.concatenate([norm_attn, norm_mlp], axis=0).astype(jnp.float32),
    )
    gains = gains.transpose(1, 0, 2).reshape(2, model)
    gain_attn, gain_mlp = gains[0], gains[1]

    scale_a, normed_a = norm_rows(field, gain_attn)
    project = mul(normed_a, w_qkv)
    queries_b, keys_b, values_b = split_project(project, HEADS, KV_HEADS, cosine, sine)
    mixed, total = attend_forward(queries_b, keys_b, values_b, allowed)
    middle = field + mul(mixed, w_out)
    scale_m, normed_m = norm_rows(middle, gain_mlp)
    pre = mul(normed_m, w_gate_up)
    gate, upper = pre[:, :FF], pre[:, FF:]
    hidden = (jax.nn.silu(gate) * upper).astype(jnp.bfloat16)
    after = middle + mul(hidden, w_down)
    result = (after * live).astype(jnp.bfloat16)

    grad_field = cotangent.astype(jnp.float32) * live
    grad_last = grad_field.astype(jnp.bfloat16)
    grad_hidden = contract_cols(grad_last, w_down)
    grad_pre = jnp.concatenate(gate_back(grad_hidden, gate, upper), axis=1)
    grad_input, grad_gain_mlp = norm_back(
        contract_cols(grad_pre, w_gate_up), middle, scale_m, gain_mlp
    )
    grad_middle = grad_field + grad_input

    grad_branch = grad_middle.astype(jnp.bfloat16)
    grad_mixed = contract_cols(grad_branch, w_out).astype(jnp.bfloat16)
    grad_queries, grad_keys, grad_values = attend_backward(
        grad_mixed, queries_b, keys_b, values_b, total, allowed
    )
    grad_project = join_grads(grad_queries, grad_keys, grad_values, cosine, sine)
    grad_input, grad_gain_attn = norm_back(
        contract_cols(grad_project, w_qkv), field, scale_a, gain_attn
    )
    grad_tokens = grad_middle + grad_input

    gain_grads = jnp.stack([grad_gain_attn, grad_gain_mlp]).reshape(2, n_shard, owned_rows)
    gain_grads = jnp.pad(gain_grads.transpose(1, 0, 2), ((0, 0), (0, 6), (0, 0)))
    grad_down, grad_gate_up, grad_qkv, grad_out, gain_own = reduce_all(
        n_shard,
        n_replica,
        [hidden.T, normed_m.T, normed_a.T, mixed.T],
        [grad_last, grad_pre, grad_project, grad_branch],
        gain_grads,
    )
    grad_down, grad_gate_up, grad_qkv, grad_out = [
        grad.astype(jnp.float32) for grad in (grad_down, grad_gate_up, grad_qkv, grad_out)
    ]
    return (
        result,
        grad_tokens,
        gain_own[0:1],
        grad_qkv[None],
        grad_out[None],
        gain_own[1:2],
        grad_gate_up[None],
        grad_down[None],
    )


def solution(mesh):
    n_shard = mesh.shape["shard"]
    n_replica = mesh.shape["replica"]
    placed = (
        P(("shard", "replica"), None),
        P(("shard", "replica"), None),
        P(),
        P(),
        P(),
        P(None, "shard"),
        P(None, "shard", None),
        P(None, "shard", None),
        P(None, "shard"),
        P(None, "shard", None),
        P(None, "shard", None),
    )

    def run(*args):
        return body(n_shard, n_replica, *args)

    return jax.shard_map(
        run,
        mesh=mesh,
        in_specs=placed,
        out_specs=(
            P(("shard", "replica"), None),
            P(("shard", "replica"), None),
            P(None, "shard"),
            P(None, "shard", None),
            P(None, "shard", None),
            P(None, "shard"),
            P(None, "shard", None),
            P(None, "shard", None),
        ),
        check_vma=False,
    )
```

```python
import functools

import jax
import jax.numpy as jnp
from jax import lax
from jax.experimental import pallas as pl
from jax.experimental.pallas import tpu as pltpu
from jax.sharding import PartitionSpec as P

HEADS = 16
KV_HEADS = 8
HEAD = 96
FF = 4096
BLOCK = 128

epsilon = 1e-05
rope_base = 100000.0


def rms_scale(field):
    return lax.rsqrt(jnp.mean(field * field, axis=-1, keepdims=True) + epsilon)


def rotate(field):
    half = field.shape[-1] // 2
    return jnp.concatenate([-field[..., half:], field[..., :half]], axis=-1)


def rope_tables(position):
    half = HEAD // 2
    freqs = rope_base ** (-(jnp.arange(half, dtype=jnp.float32) * 2.0) / HEAD)
    angles = position.astype(jnp.float32)[:, None] * freqs[None, :]
    cosine = jnp.cos(angles)
    sine = jnp.sin(angles)
    return (jnp.concatenate([cosine, cosine], axis=-1), jnp.concatenate([sine, sine], axis=-1))


def locate(device, seq_lengths, seq_device, seq_offsets, rows):
    starts = seq_offsets * BLOCK
    local = jnp.arange(rows, dtype=jnp.int32)
    labels = jnp.arange(seq_lengths.shape[0], dtype=jnp.int32)
    hits = (
        (seq_device[None, :] == device)
        & (local[:, None] >= starts[None, :])
        & (local[:, None] < (starts + seq_lengths)[None, :])
    )
    segment = jnp.max(jnp.where(hits, labels[None, :], -1), axis=1)
    begin = jnp.sum(jnp.where(hits, starts[None, :], 0), axis=1)
    return (segment, local - begin)


def mask_of(segment):
    local = jnp.arange(segment.shape[0], dtype=jnp.int32)
    return (segment[:, None] == segment[None, :]) & (local[None, :] <= local[:, None])


def contract_rows(left, right):
    return lax.dot_general(
        left, right, (((0,), (0,)), ((), ())), preferred_element_type=jnp.float32
    )


def contract_cols(left, right):
    return lax.dot_general(
        left, right, (((1,), (1,)), ((), ())), preferred_element_type=jnp.float32
    )


def norm_back(grad_normed, field, scale, gain):
    normed = field * scale
    grad_gain = jnp.sum(grad_normed * normed, axis=0)
    inner = grad_normed * gain[None, :]
    grad_field = scale * (inner - normed * jnp.mean(inner * normed, axis=-1, keepdims=True))
    return (grad_field, grad_gain)


def join_grads(grad_queries, grad_keys, grad_values, cosine, sine):
    rows = grad_queries.shape[0]
    grad_queries = grad_queries * cosine[:, None, :] - rotate(grad_queries * sine[:, None, :])
    grad_keys = grad_keys * cosine[:, None, :] - rotate(grad_keys * sine[:, None, :])
    return jnp.concatenate(
        [
            grad_queries.reshape(rows, -1),
            grad_keys.reshape(rows, -1),
            grad_values.reshape(rows, -1),
        ],
        axis=1,
    ).astype(jnp.bfloat16)


def attention_scores(queries_b, keys_b, allowed):
    rows = queries_b.shape[0]
    kv_count = keys_b.shape[1]
    grouped = queries_b.reshape(rows, kv_count, queries_b.shape[1] // kv_count, HEAD)
    scores = jnp.einsum(
        "qkgd,pkd->kgqp", grouped, keys_b, preferred_element_type=jnp.float32
    ) * HEAD ** (-0.5)
    return jnp.where(allowed, scores, -1e30)


def attend_backward(grad_mixed_b, queries_b, keys_b, values_b, total, allowed):
    rows = queries_b.shape[0]
    q_heads = queries_b.shape[1]
    kv_count = keys_b.shape[1]
    per = q_heads // kv_count
    factor = HEAD ** (-0.5)
    grad_mixed = grad_mixed_b.reshape(rows, kv_count, per, HEAD)
    weights = jnp.exp(attention_scores(queries_b, keys_b, allowed) - total)
    weights_b = weights.astype(jnp.bfloat16)
    grad_values = jnp.einsum(
        "kgqp,qkgd->pkd", weights_b, grad_mixed, preferred_element_type=jnp.float32
    )
    grad_weights = jnp.einsum(
        "qkgd,pkd->kgqp", grad_mixed, values_b, preferred_element_type=jnp.float32
    )
    grad_scores = weights * (grad_weights - jnp.sum(weights * grad_weights, axis=-1, keepdims=True))
    grad_scores_b = grad_scores.astype(jnp.bfloat16)
    grouped = queries_b.reshape(rows, kv_count, per, HEAD)
    grad_queries = jnp.einsum(
        "kgqp,pkd->qkgd", grad_scores_b, keys_b, preferred_element_type=jnp.float32
    )
    grad_queries = grad_queries.reshape(rows, q_heads, HEAD) * factor
    grad_keys = (
        jnp.einsum("kgqp,qkgd->pkd", grad_scores_b, grouped, preferred_element_type=jnp.float32)
        * factor
    )
    return (grad_queries, grad_keys, grad_values)


def gate_back(grad_hidden, gate, upper):
    sigma = jax.nn.sigmoid(gate)
    grad_gate = grad_hidden * upper * sigma * (1.0 + gate * (1.0 - sigma))
    grad_upper = grad_hidden * (gate * sigma)
    return (grad_gate.astype(jnp.bfloat16), grad_upper.astype(jnp.bfloat16))


MESH = pl.DeviceIdType.MESH


def submasks(order, step):
    masks = [0]
    for bit in order[:step]:
        masks += [mask | bit for mask in masks]
    return masks


def greet(partners):
    barrier = pltpu.get_barrier_semaphore()
    for partner in partners:
        pl.semaphore_signal(barrier, inc=1, device_id=partner, device_id_type=MESH)
    pl.semaphore_wait(barrier, len(partners))


class Item:
    def __init__(self, n_shard, own, full, cols, single, sems):
        self.shard, replica = lax.axis_index("shard"), lax.axis_index("replica")
        self.replica = replica
        core, pair = lax.rem(replica, 2), lax.rem(replica // 2, 2)
        self.bits = [1 << i for i in range(n_shard.bit_length() - 1)]
        self.n_shard = n_shard
        self.own, self.full, self.cols = own, full, cols
        self.rows = own.shape[0]
        self.load_sem, self.local_sem, self.send_sem, self.recv_sem = sems
        half = self.rows // 2
        common = half - 2 * single
        base = core * half
        self.parts = [
            (base + pair * (single + common), single, self.bits),
            (base + single, common, self.bits[1:] + self.bits[:1]),
        ]
        self.mate = (base + (1 - pair) * (single + common), single)
        self.half = (base, half)
        self.other_half = ((1 - core) * half, half)
        self.number = {}
        self.waited, self.started = set(), {}

    def index(self, key):
        return self.number.setdefault(key, len(self.number))

    def window(self, mask, span):
        start = pl.multiple_of((self.shard ^ mask) * self.rows + span[0], 16)
        return self.full.at[pl.ds(start, span[1]), self.cols]

    def send(self, key, src, dst, device):
        if key in self.started:
            return
        index = self.index(key)
        copy = pltpu.make_async_remote_copy(
            src_ref=src,
            dst_ref=dst,
            send_sem=self.send_sem.at[index],
            recv_sem=self.recv_sem.at[index],
            device_id=device,
            device_id_type=MESH,
        )
        copy.start()
        self.started[key] = copy

    def landed(self, key, span):
        if key in self.waited:
            return
        self.waited.add(key)
        window = self.window(key[2], span)
        pltpu.make_async_remote_copy(
            src_ref=window,
            dst_ref=window,
            send_sem=self.send_sem.at[self.index(key)],
            recv_sem=self.recv_sem.at[self.index(key)],
            device_id={"replica": self.replica ^ 1},
            device_id_type=MESH,
        ).wait_recv()

    def load(self, source):
        self.loading = pltpu.make_async_copy(source.at[:, self.cols], self.own.at[:, self.cols], self.load_sem)
        self.loading.start()

    def over_shard(self, part, step, mask):
        start, size, order = self.parts[part]
        bit = order[step]
        window = self.window(mask, (start, size))
        src = window
        if mask == 0:
            src = self.own.at[pl.ds(pl.multiple_of(start, 16), size), self.cols]
        self.send(("shard", part, mask | bit), src, window, {"shard": self.shard ^ bit})

    def first(self):
        self.loading.wait()
        for step in range(len(self.bits)):
            for part in range(2):
                self.over_shard(part, step, 0)
        start = pl.multiple_of(self.shard * self.rows, 16)
        self.placing = pltpu.make_async_copy(
            self.own.at[:, self.cols], self.full.at[pl.ds(start, self.rows), self.cols], self.local_sem
        )
        self.placing.start()

    def arrive(self, part, mask):
        span = self.parts[part][:2]
        self.landed(("shard", part, mask), span)
        if part == 0:
            window = self.window(mask, span)
            self.send(("pair", 0, mask), window, window, {"replica": self.replica ^ 2})

    def relay(self):
        for step in range(1, len(self.bits)):
            for part in range(2):
                for mask in submasks(self.parts[part][2], step)[1:]:
                    self.arrive(part, mask)
                    self.over_shard(part, step, mask)

    def pass_on(self):
        for mask in range(1, self.n_shard):
            self.arrive(0, mask)

    def across(self):
        for mask in range(1, self.n_shard):
            self.arrive(1, mask)
            self.landed(("pair", 0, mask), self.mate)
            window = self.window(mask, self.half)
            self.send(("core", 0, mask), window, window, {"replica": self.replica ^ 1})

    def complete(self):
        for mask in range(1, self.n_shard):
            self.landed(("core", 0, mask), self.other_half)
        self.placing.wait()

    def finish(self):
        for copy in self.started.values():
            copy.wait_send()


def round_to(value, unit):
    return max(unit, int(value / unit + 0.5) * unit)


def scaled_rows(field):
    return field * lax.rsqrt(jnp.mean(field * field, axis=-1, keepdims=True) + epsilon)


QUAD = 4 * HEAD
TILE = 512


def forward_kernel(n_shard, plan, stages, *refs):
    refs = list(refs)
    take = lambda n: [refs.pop(0) for _ in range(n)]
    weights, (gain, tokens, cosine, sine, mask) = take(4), take(5)
    fulls = take(4)
    turned_a, turned_o, turned_m, turned_h, roped, lse, middle, gate_up, gains = take(9)
    owns, (gain_all, w_qkv, w_out, tiles) = take(4), take(4)
    field, normed, project, q_heads, k_heads, v_heads, mixed = take(7)
    out_a, out_o, out_m, out_h, out_roped, out_lse, pre = take(7)
    load_sem, local_sem, send_sem, recv_sem, gain_send, gain_recv, gain_sem, tile_sem, out_sem = take(9)
    shard, replica = lax.axis_index("shard"), lax.axis_index("replica")
    rows, model = tokens.shape
    owned = gain.shape[1]

    items = []
    for n, (weight, start, size, single) in enumerate(plan):
        item = Item(
            n_shard,
            owns[weight],
            fulls[weight],
            pl.ds(start, size),
            single,
            (load_sem.at[n], local_sem.at[n], send_sem.at[n], recv_sem.at[n]),
        )
        item.load(weights[weight])
        items.append(item)
    gain_own = pltpu.make_async_copy(gain, gain_all.at[shard], gain_sem.at[0])
    gain_own.start()
    greet(
        [{"shard": shard ^ other} for other in range(1, n_shard)]
        + [{"replica": replica ^ 1}, {"replica": replica ^ 2}]
    )

    def gain_copy(other, index):
        return pltpu.make_async_remote_copy(
            src_ref=gain,
            dst_ref=gain_all.at[index],
            send_sem=gain_send.at[other - 1],
            recv_sem=gain_recv.at[other - 1],
            device_id={"shard": shard ^ other},
            device_id_type=MESH,
        )

    for other in range(1, n_shard):
        gain_copy(other, shard).start()

    leaving = []

    def leave(src, dst):
        copy = pltpu.make_async_copy(src, dst, out_sem.at[len(leaving)])
        copy.start()
        leaving.append(copy)

    def norm(row):
        value = scaled_rows(field[...])
        for other in range(n_shard):
            span = slice(other * owned, (other + 1) * owned)
            normed[:, span] = (value[:, span] * gain_all[other, row : row + 1, :]).astype(jnp.bfloat16)

    def fetch(weight, index, start, dst):
        copy = pltpu.make_async_copy(
            fulls[weight].at[:, pl.ds(start, dst.shape[1])], dst, tile_sem.at[index]
        )
        copy.start()
        return copy

    def begin():
        gain_own.wait()
        for other in range(1, n_shard):
            gain_copy(other, shard ^ other).wait()
        leave(gain_all, gains)
        field[...] = tokens[...].astype(jnp.float32)
        norm(0)
        out_a[...] = normed[...].astype(jnp.float32).T.astype(jnp.bfloat16)
        leave(out_a, turned_a)

    def projections():
        loads = [
            fetch(0, n, n * TILE, w_qkv.at[:, pl.ds(n * TILE, TILE)])
            for n in range(w_qkv.shape[1] // TILE)
        ]
        for n, load in enumerate(loads):
            load.wait()
            span = pl.ds(n * TILE, TILE)
            project[:, span] = jnp.dot(
                normed[...], w_qkv[:, span], preferred_element_type=jnp.float32
            )

    lane = lax.broadcasted_iota(jnp.int32, (rows, QUAD), 1)
    first_half = lax.rem(lane, HEAD) < HEAD // 2
    in_head = lax.broadcasted_iota(jnp.int32, (rows, 128), 1) < HEAD

    def rope():
        for quad, heads in enumerate([q_heads] * 4 + [k_heads] * 2 + [v_heads] * 2):
            span = slice(quad * QUAD, (quad + 1) * QUAD)
            value = project[:, span]
            if quad < 6:
                turned = jnp.where(
                    first_half,
                    -pltpu.roll(value, QUAD - HEAD // 2, 1),
                    pltpu.roll(value, HEAD // 2, 1),
                )
                value = value * cosine[...] + turned * sine[...]
            out_roped[:, span] = value.astype(jnp.bfloat16)
            base = [0, 4, 8, 12, 0, 4, 0, 4][quad]
            for n in range(4):
                moved = value if n == 0 else pltpu.roll(value, QUAD - n * HEAD, 1)
                heads[base + n] = jnp.where(in_head, moved[:, :128], 0.0).astype(jnp.bfloat16)
        leave(out_roped, roped)
        out_lse[...] = jnp.zeros_like(out_lse)

    def attend(quad):
        allowed = mask[...] > 0.5
        spot = lax.broadcasted_iota(jnp.int32, (rows, 128), 1)
        total = jnp.zeros((rows, QUAD), jnp.float32)
        for n in range(4):
            query = q_heads[4 * quad + n]
            key = k_heads[2 * quad + n // 2]
            scores = lax.dot_general(
                query, key, (((1,), (1,)), ((), ())), preferred_element_type=jnp.float32
            ) * HEAD ** (-0.5)
            scores = jnp.where(allowed, scores, -1e30)
            top = jnp.max(scores, axis=-1, keepdims=True)
            size = jnp.log(jnp.sum(jnp.exp(scores - top), axis=-1, keepdims=True)) + top
            share = jnp.exp(scores - size).astype(jnp.bfloat16)
            part = jnp.dot(
                share, v_heads[2 * quad + n // 2], preferred_element_type=jnp.float32
            )
            part = jnp.concatenate([part, jnp.zeros((rows, QUAD - 128), jnp.float32)], axis=1)
            total = total + (part if n == 0 else pltpu.roll(part, n * HEAD, 1))
            out_lse[...] += jnp.where(spot == 4 * quad + n, size, 0.0)
        mixed[:, quad * QUAD : (quad + 1) * QUAD] = total.astype(jnp.bfloat16)
        span = slice(quad * QUAD, (quad + 1) * QUAD)
        out_o[span, :] = total.T.astype(jnp.bfloat16)

    def attended():
        leave(out_o, turned_o)
        leave(out_lse, lse)

    def output():
        load = fetch(1, 0, 0, w_out)
        load.wait()
        for n in range(model // TILE):
            span = pl.ds(n * TILE, TILE)
            field[:, span] += jnp.dot(
                mixed[...], w_out[:, span], preferred_element_type=jnp.float32
            )
        leave(field, middle)
        norm(1)
        out_m[...] = normed[...].astype(jnp.float32).T.astype(jnp.bfloat16)
        leave(out_m, turned_m)

    hidden_units = gate_up.shape[1] // 2
    pairs = {}

    def fetch_pair(n):
        pairs[n] = [
            fetch(2, 2 * (n % 2) + k, k * hidden_units + n * TILE, tiles.at[n % 2, k])
            for k in range(2)
        ]

    def feed(n, last):
        if n not in pairs:
            fetch_pair(n)
        if n < last:
            fetch_pair(n + 1)
        for load in pairs[n]:
            load.wait()
        slot = n % 2
        if n >= 2:
            for copy in stored[n - 2]:
                copy.wait()
        both = []
        for k in range(2):
            value = jnp.dot(normed[...], tiles[slot, k], preferred_element_type=jnp.float32)
            pre[slot, k] = value
            both.append(value)
        gate, upper = both
        hidden = gate * jax.nn.sigmoid(gate) * upper
        out_h[n * TILE : (n + 1) * TILE, :] = hidden.T.astype(jnp.bfloat16)
        stored[n] = []
        for k in range(2):
            copy = pltpu.make_async_copy(
                pre.at[slot, k],
                gate_up.at[:, pl.ds(k * hidden_units + n * TILE, TILE)],
                tile_sem.at[4 + 2 * slot + k],
            )
            copy.start()
            stored[n].append(copy)

    stored = {}
    half = hidden_units // TILE // 2
    work = {
        "begin": begin,
        "project": lambda: (projections(), rope()),
        "attend0": lambda: [attend(n) for n in range(2)],
        "attend1": lambda: ([attend(n) for n in range(2, 4)], attended()),
        "output": output,
        "feed0": lambda: [feed(n, half - 1) for n in range(half)],
        "feed1": lambda: [feed(n, 2 * half - 1) for n in range(half, 2 * half)],
    }
    phases = [Item.first, Item.relay, Item.pass_on, Item.across, Item.complete]
    for time in range(len(items) + len(phases) - 1):
        for late, phase in enumerate(phases):
            if 0 <= time - late < len(items):
                phase(items[time - late])
        for name in stages.get(time, ()):
            work[name]()
    leave(out_h, turned_h)
    for item in items:
        item.finish()
    for copies in list(stored.values())[-2:]:
        for copy in copies:
            copy.wait()
    for copy in leaving:
        copy.wait()


def gather_forward(n_shard, weights, gain, tokens, cosine, sine, mask):
    def single(weight, share):
        return round_to(weight.shape[0] // 2 * share, 16)

    qkv, out, gate_up, down = weights
    part = gate_up.shape[1] // 4
    rows, model = tokens.shape
    wide, hidden = gate_up.shape[1], gate_up.shape[1] // 2
    third = [single(weight, 0.333) for weight in weights]
    plan = [
        (0, 0, qkv.shape[1] // 2, third[0]),
        (0, qkv.shape[1] // 2, qkv.shape[1] // 2, third[0]),
        (1, 0, model, third[1]),
        (2, 0, part, third[2]),
        (2, 2 * part, part, third[2]),
        (2, part, part, third[2]),
        (2, 3 * part, part, third[2]),
        (3, 0, model // 2, third[3]),
        (3, model // 2, model // 2, third[3]),
    ]
    stages = {
        0: ["begin"],
        5: ["project"],
        6: ["attend0"],
        7: ["attend1"],
        8: ["output", "feed0"],
        10: ["feed1"],
    }
    copies = 4 * (n_shard - 1)
    n = len(plan)
    anywhere = pl.BlockSpec(memory_space=pl.ANY)
    whole = pl.BlockSpec(memory_space=pltpu.VMEM)
    bf16, f32 = jnp.bfloat16, jnp.float32
    shape = jax.ShapeDtypeStruct
    heads = lambda count: pltpu.VMEM((count, rows, 128), bf16)
    return pl.pallas_call(
        functools.partial(forward_kernel, n_shard, plan, stages),
        out_shape=[shape((w.shape[0] * n_shard, w.shape[1]), w.dtype) for w in weights]
        + [
            shape((model, rows), bf16),
            shape((model, rows), bf16),
            shape((model, rows), bf16),
            shape((hidden, rows), bf16),
            shape((rows, qkv.shape[1]), bf16),
            shape((rows, 128), f32),
            shape((rows, model), f32),
            shape((rows, wide), f32),
            shape((n_shard,) + gain.shape, f32),
        ],
        in_specs=[anywhere] * 4 + [whole] * 5,
        out_specs=[anywhere] * 13,
        scratch_shapes=[pltpu.VMEM(w.shape, w.dtype) for w in weights]
        + [
            pltpu.VMEM((n_shard,) + gain.shape, f32),
            pltpu.VMEM((model, qkv.shape[1]), bf16),
            pltpu.VMEM((model, model), bf16),
            pltpu.VMEM((2, 2, model, TILE), bf16),
            pltpu.VMEM((rows, model), f32),
            pltpu.VMEM((rows, model), bf16),
            pltpu.VMEM((rows, qkv.shape[1]), f32),
            heads(HEADS),
            heads(KV_HEADS),
            heads(KV_HEADS),
            pltpu.VMEM((rows, model), bf16),
            pltpu.VMEM((model, rows), bf16),
            pltpu.VMEM((model, rows), bf16),
            pltpu.VMEM((model, rows), bf16),
            pltpu.VMEM((hidden, rows), bf16),
            pltpu.VMEM((rows, qkv.shape[1]), bf16),
            pltpu.VMEM((rows, 128), f32),
            pltpu.VMEM((2, 2, rows, TILE), f32),
            pltpu.SemaphoreType.DMA((n,)),
            pltpu.SemaphoreType.DMA((n,)),
            pltpu.SemaphoreType.DMA((n, copies)),
            pltpu.SemaphoreType.DMA((n, copies)),
            pltpu.SemaphoreType.DMA((n_shard - 1,)),
            pltpu.SemaphoreType.DMA((n_shard - 1,)),
            pltpu.SemaphoreType.DMA((1,)),
            pltpu.SemaphoreType.DMA((8,)),
            pltpu.SemaphoreType.DMA((16,)),
        ],
        compiler_params=pltpu.CompilerParams(
            collective_id=1, has_side_effects=True, vmem_limit_bytes=66_000_000
        ),
        name="gather_forward",
    )(*weights, gain, tokens, cosine, sine, mask)


SLOTS = 5


class Pipe:
    def __init__(self, n_shard, n_replica, begin, count, block, deliver, bufs, sems):
        self.shard, self.replica = lax.axis_index("shard"), lax.axis_index("replica")
        chip = self.replica // 2
        self.inner = lax.rem(chip, 2) != lax.rem(chip // 2, 2)
        self.steps = n_shard.bit_length() - 1
        self.swaps = [6] + [1 << k for k in range(3, n_replica.bit_length() - 1)]
        self.begin, self.count, self.block, self.deliver = begin, count, block, deliver
        bufs = list(bufs)
        self.out = [bufs.pop(0) for _ in range(self.steps)]
        self.into = [bufs.pop(0) for _ in range(self.steps)]
        self.kept = [bufs.pop(0) for _ in range(max(1, self.steps - 1))]
        self.fold_out, self.fold_in, self.total = bufs.pop(0), bufs.pop(0), bufs.pop(0)
        self.swap_out = [bufs.pop(0) for _ in self.swaps]
        self.swap_in = [bufs.pop(0) for _ in self.swaps]
        self.final, self.across = bufs.pop(0), bufs.pop(0)
        self.send_sem, self.recv_sem, self.local_sem = sems
        self.last = self.steps + 2 + len(self.swaps)

    @staticmethod
    def scratch(n_shard, n_replica, rows, cols, dtype):
        steps = n_shard.bit_length() - 1
        swaps = n_replica.bit_length() - 3
        blocks = [n_shard >> (k + 1) for k in range(steps)]
        shapes = [pltpu.VMEM((SLOTS, b, rows, cols), dtype) for b in blocks * 2]
        shapes += [
            pltpu.VMEM((SLOTS, max(1, b // 2), rows, cols), jnp.float32)
            for b in blocks[: max(1, steps - 1)]
        ]
        one = (SLOTS, rows, cols)
        shapes += [pltpu.VMEM(one, dtype)] * 2 + [pltpu.VMEM(one, jnp.float32)]
        shapes += [pltpu.VMEM(one, dtype)] * (2 * swaps + 2)
        kinds = steps + swaps + 3
        return shapes, [
            pltpu.SemaphoreType.DMA((kinds, SLOTS)),
            pltpu.SemaphoreType.DMA((kinds, SLOTS)),
            pltpu.SemaphoreType.DMA((2, SLOTS)),
        ]

    def bit(self, chunk, step):
        return 1 << lax.rem(step + lax.rem(chunk, 2), self.steps)

    def mask(self, chunk, entry):
        found = 0
        for step in range(self.steps):
            if (entry >> step) & 1:
                found = found | self.bit(chunk, step)
        return found

    def copy(self, kind, slot, src, dst, device):
        return pltpu.make_async_remote_copy(
            src_ref=src.at[slot],
            dst_ref=dst.at[slot],
            send_sem=self.send_sem.at[kind, slot],
            recv_sem=self.recv_sem.at[kind, slot],
            device_id=device,
            device_id_type=MESH,
        )

    def halving(self, step, chunk, slot):
        device = {"shard": self.shard ^ self.bit(chunk, step)}
        return self.copy(step, slot, self.out[step], self.into[step], device)

    def folding(self, slot):
        return self.copy(
            self.steps, slot, self.fold_out, self.fold_in, {"replica": self.replica ^ 2}
        )

    def swapping(self, number, slot):
        device = {"replica": self.replica ^ self.swaps[number]}
        return self.copy(
            self.steps + 1 + number, slot, self.swap_out[number], self.swap_in[number], device
        )

    def unfolding(self, slot):
        kind = self.steps + 1 + len(self.swaps)
        return self.copy(kind, slot, self.final, self.final, {"replica": self.replica ^ 2})

    def crossing(self, slot):
        kind = self.steps + 2 + len(self.swaps)
        return self.copy(kind, slot, self.final, self.across, {"replica": self.replica ^ 1})

    def stage(self, number, chunk, slot):
        steps, swaps = self.steps, len(self.swaps)
        dtype = self.final.dtype
        if number == 0:
            for entry in range(1, 1 << steps, 2):
                self.out[0][slot, entry >> 1] = self.block(chunk, self.mask(chunk, entry)).astype(dtype)
            self.halving(0, chunk, slot).start()
        elif number <= steps:
            sums = []
            for entry in range(1 << (steps - number)):
                if number == 1:
                    sums.append(self.block(chunk, self.mask(chunk, 2 * entry)))
                else:
                    sums.append(self.kept[number - 2][slot, entry])
            self.halving(number - 1, chunk, slot).wait()
            for entry, value in enumerate(sums):
                value = value + self.into[number - 1][slot, entry].astype(jnp.float32)
                if number == steps:
                    @pl.when(self.inner)
                    def _(value=value):
                        self.total[slot] = value

                    @pl.when(jnp.logical_not(self.inner))
                    def _(value=value):
                        self.fold_out[slot] = value.astype(dtype)
                        self.folding(slot).start()
                elif entry & 1:
                    self.out[number][slot, entry >> 1] = value.astype(dtype)
                else:
                    self.kept[number - 1][slot, entry >> 1] = value
            if number < steps:
                self.halving(number, chunk, slot).start()
        elif number == steps + 1:
            @pl.when(self.inner)
            def _():
                self.folding(slot).wait_recv()
                value = self.total[slot] + self.fold_in[slot].astype(jnp.float32)
                self.swap_out[0][slot] = value.astype(dtype)
                self.swapping(0, slot).start()

            @pl.when(jnp.logical_not(self.inner))
            def _():
                self.folding(slot).wait_send()
        elif number <= steps + 1 + swaps:
            @pl.when(self.inner)
            def _():
                done = number - steps - 2
                self.swapping(done, slot).wait()
                value = self.swap_out[done][slot].astype(jnp.float32) + self.swap_in[done][
                    slot
                ].astype(jnp.float32)
                if done + 1 < swaps:
                    self.swap_out[done + 1][slot] = value.astype(dtype)
                    self.swapping(done + 1, slot).start()
                else:
                    self.final[slot] = value.astype(dtype)
                    self.unfolding(slot).start()
        elif number == self.last:
            @pl.when(jnp.logical_not(self.inner))
            def _():
                self.unfolding(slot).wait_recv()

            self.crossing(slot).start()
            self.deliver(chunk, 0, self.final.at[slot], self.local_sem.at[0, slot], True)
        else:
            @pl.when(self.inner)
            def _():
                self.unfolding(slot).wait_send()

            self.crossing(slot).wait()
            self.deliver(chunk, 1, self.across.at[slot], self.local_sem.at[1, slot], True)
            self.deliver(chunk, 0, self.final.at[slot], self.local_sem.at[0, slot], False)
            self.deliver(chunk, 1, self.across.at[slot], self.local_sem.at[1, slot], False)

    def run(self, time):
        for number in range(self.last + 2):
            chunk = time - self.begin - number

            @pl.when((chunk >= 0) & (chunk < self.count))
            def _(number=number, chunk=chunk):
                self.stage(number, chunk, lax.rem(chunk, SLOTS))

    def length(self):
        return self.begin + self.count + self.last + 1


DEEP_COLS = 128
WIDE_COLS = 256


def reduce_kernel(n_shard, n_replica, halves, *refs):
    refs = list(refs)
    take = lambda n: [refs.pop(0) for _ in range(n)]
    lefts, rights, (gain_in,) = take(4), take(4), take(1)
    outs, (gain_out,) = take(4), take(1)
    deep_left, deep_right, wide_left, wide_right = take(4)
    load_sem, pass_send, pass_recv = take(3)
    n_bufs = (len(refs) - 9) // 3
    deep_bufs, deep_sems = take(n_bufs), take(3)
    wide_bufs, wide_sems = take(n_bufs), take(3)
    gain_bufs, gain_sems = take(n_bufs), take(3)
    shard, replica = lax.axis_index("shard"), lax.axis_index("replica")
    core = lax.rem(replica, 2)
    rows = lefts[0].shape[1]
    model = lefts[1].shape[0]
    deep_rows, wide_rows = outs[0].shape[0], outs[1].shape[0]

    place_left = [deep_left] + [wide_left.at[pl.ds(k * model, model)] for k in range(3)]
    starts = [0, 0, halves[1], halves[1] + halves[2]]
    place_right = [
        (deep_right if k == 0 else wide_right).at[:, pl.ds(starts[k], halves[k])] for k in range(4)
    ]
    loads, passes = [], []
    greet(
        [{"shard": shard ^ (1 << k)} for k in range(n_shard.bit_length() - 1)]
        + [{"replica": replica ^ mask} for mask in [1, 2, 6]]
        + [{"replica": replica ^ (1 << k)} for k in range(3, n_replica.bit_length() - 1)]
    )
    for k in range(4):
        mine = pl.ds(pl.multiple_of(core * halves[k], 128), halves[k])
        other = pl.ds(pl.multiple_of((1 - core) * halves[k], 128), halves[k])
        sources = [
            (lefts[k], place_left[k].at[:, pl.ds(0, rows)]),
            (rights[k].at[:, mine], place_right[k].at[pl.ds(0, rows)]),
        ]
        for n, (src, dst) in enumerate(sources):
            loads.append(pltpu.make_async_copy(src, dst, load_sem.at[2 * k + n]))
            loads[-1].start()
        sources = [
            (lefts[k], place_left[k].at[:, pl.ds(rows, rows)]),
            (rights[k].at[:, other], place_right[k].at[pl.ds(rows, rows)]),
        ]
        for n, (src, dst) in enumerate(sources):
            passes.append(
                pltpu.make_async_remote_copy(
                    src_ref=src,
                    dst_ref=dst,
                    send_sem=pass_send.at[2 * k + n],
                    recv_sem=pass_recv.at[2 * k + n],
                    device_id={"replica": replica ^ 1},
                    device_id_type=MESH,
                )
            )
            passes[-1].start()

    def arrived(first, end):
        for k in range(2 * first, 2 * end):
            loads[k].wait()
            passes[k].wait()

    def deep_block(chunk, mask):
        left = deep_left[pl.ds(pl.multiple_of((shard ^ mask) * deep_rows, 16), deep_rows), :]
        right = deep_right[:, pl.ds(pl.multiple_of(chunk * DEEP_COLS, 128), DEEP_COLS)]
        return jnp.dot(left, right, preferred_element_type=jnp.float32)

    bounds = [starts[k] // WIDE_COLS for k in (2, 3)]

    def wide_block(chunk, mask):
        weight = (chunk >= bounds[0]).astype(jnp.int32) + (chunk >= bounds[1]).astype(jnp.int32)
        start = weight * model + (shard ^ mask) * wide_rows
        left = wide_left[pl.ds(pl.multiple_of(start, 16), wide_rows), :]
        right = wide_right[:, pl.ds(pl.multiple_of(chunk * WIDE_COLS, 128), WIDE_COLS)]
        return jnp.dot(left, right, preferred_element_type=jnp.float32)

    def gain_block(chunk, mask):
        return gain_in[shard ^ mask]

    def put(out, start, size, src, sem, begin):
        copy = pltpu.make_async_copy(src, out.at[:, pl.ds(pl.multiple_of(start, 128), size)], sem)
        if begin:
            copy.start()
        else:
            copy.wait()

    def deep_deliver(chunk, side, src, sem, begin):
        half = jnp.where(side == 0, core, 1 - core) * halves[0]
        put(outs[0], half + chunk * DEEP_COLS, DEEP_COLS, src, sem, begin)

    def wide_deliver(chunk, side, src, sem, begin):
        edges = [0] + bounds + [wide_right.shape[1] // WIDE_COLS]
        half = core if side == 0 else 1 - core
        for k in range(3):
            @pl.when((chunk >= edges[k]) & (chunk < edges[k + 1]))
            def _(k=k):
                start = half * halves[k + 1] + (chunk - edges[k]) * WIDE_COLS
                put(outs[k + 1], start, WIDE_COLS, src, sem, begin)

    def gain_deliver(chunk, side, src, sem, begin):
        if side == 1 and begin:
            gain_out[...] = gain_pipe.final[0] + src[...]

    n_deep = halves[0] // DEEP_COLS
    n_wide = wide_right.shape[1] // WIDE_COLS
    size = (n_shard, n_replica)
    deep = Pipe(*size, 0, n_deep, deep_block, deep_deliver, deep_bufs, deep_sems)
    wide = Pipe(*size, n_deep, n_wide, wide_block, wide_deliver, wide_bufs, wide_sems)
    gain_pipe = Pipe(*size, 1, 1, gain_block, gain_deliver, gain_bufs, gain_sems)
    arrived(0, 1)

    def step(time, carry):
        @pl.when(time == n_deep)
        def _():
            arrived(1, 4)

        deep.run(time)
        gain_pipe.run(time)
        wide.run(time)
        return carry

    lax.fori_loop(0, wide.length(), step, 0)


def reduce_all(n_shard, n_replica, lefts, rights, gain_grads):
    rows = lefts[0].shape[1]
    halves = [right.shape[1] // 2 for right in rights]
    owned = [left.shape[0] // n_shard for left in lefts]
    model = lefts[1].shape[0]
    anywhere = pl.BlockSpec(memory_space=pl.ANY)
    whole = pl.BlockSpec(memory_space=pltpu.VMEM)
    size = (n_shard, n_replica)
    deep_bufs, deep_sems = Pipe.scratch(*size, owned[0], DEEP_COLS, jnp.bfloat16)
    wide_bufs, wide_sems = Pipe.scratch(*size, owned[1], WIDE_COLS, jnp.bfloat16)
    gain_bufs, gain_sems = Pipe.scratch(*size, *gain_grads.shape[1:], jnp.float32)
    return pl.pallas_call(
        functools.partial(reduce_kernel, n_shard, n_replica, halves),
        out_shape=[
            jax.ShapeDtypeStruct((own, right.shape[1]), jnp.bfloat16)
            for own, right in zip(owned, rights)
        ]
        + [jax.ShapeDtypeStruct(gain_grads.shape[1:], jnp.float32)],
        in_specs=[anywhere] * 8 + [whole],
        out_specs=[anywhere] * 4 + [whole],
        scratch_shapes=[
            pltpu.VMEM((lefts[0].shape[0], 2 * rows), jnp.bfloat16),
            pltpu.VMEM((2 * rows, halves[0]), jnp.bfloat16),
            pltpu.VMEM((3 * model, 2 * rows), jnp.bfloat16),
            pltpu.VMEM((2 * rows, sum(halves[1:])), jnp.bfloat16),
            pltpu.SemaphoreType.DMA((8,)),
            pltpu.SemaphoreType.DMA((8,)),
            pltpu.SemaphoreType.DMA((8,)),
            *deep_bufs,
            *deep_sems,
            *wide_bufs,
            *wide_sems,
            *gain_bufs,
            *gain_sems,
        ],
        compiler_params=pltpu.CompilerParams(
            collective_id=2, has_side_effects=True, vmem_limit_bytes=66_000_000
        ),
        name="reduce_gradients",
    )(*lefts, *rights, gain_grads)


def body(
    n_shard,
    n_replica,
    tokens,
    cotangent,
    seq_lengths,
    seq_device,
    seq_offsets,
    norm_attn,
    w_qkv,
    w_out,
    norm_mlp,
    w_gate_up,
    w_down,
):
    rows, model = tokens.shape
    w_qkv, w_out, w_gate_up, w_down = w_qkv[0], w_out[0], w_gate_up[0], w_down[0]
    owned_rows = w_qkv.shape[0]

    device = lax.axis_index(("shard", "replica"))
    segment, position = locate(device, seq_lengths, seq_device, seq_offsets, rows)
    live = (segment >= 0).astype(jnp.float32)[:, None]
    field = tokens.astype(jnp.float32)
    cosine, sine = rope_tables(position)
    allowed = mask_of(segment)

    (
        w_qkv,
        w_out,
        w_gate_up,
        w_down,
        normed_a_t,
        mixed_t,
        normed_m_t,
        hidden_t,
        roped,
        total,
        middle,
        pre,
        gains,
    ) = gather_forward(
        n_shard,
        (w_qkv, w_out, w_gate_up, w_down),
        jnp.concatenate([norm_attn, norm_mlp], axis=0).astype(jnp.float32),
        tokens,
        jnp.tile(cosine, (1, 4)),
        jnp.tile(sine, (1, 4)),
        allowed.astype(jnp.float32),
    )
    gains = gains.transpose(1, 0, 2).reshape(2, model)
    gain_attn, gain_mlp = gains[0], gains[1]
    per = HEADS // KV_HEADS
    queries_b = roped[:, : HEADS * HEAD].reshape(rows, HEADS, HEAD)
    keys_b = roped[:, HEADS * HEAD : (HEADS + KV_HEADS) * HEAD].reshape(rows, KV_HEADS, HEAD)
    values_b = roped[:, (HEADS + KV_HEADS) * HEAD :].reshape(rows, KV_HEADS, HEAD)
    total = total[:, :HEADS].T.reshape(KV_HEADS, per, rows, 1)
    scale_a, scale_m = rms_scale(field), rms_scale(middle)
    gate, upper = pre[:, :FF], pre[:, FF:]
    result = ((middle + contract_rows(hidden_t, w_down)) * live).astype(jnp.bfloat16)

    grad_field = cotangent.astype(jnp.float32) * live
    grad_last = grad_field.astype(jnp.bfloat16)
    grad_hidden = contract_cols(grad_last, w_down)
    grad_pre = jnp.concatenate(gate_back(grad_hidden, gate, upper), axis=1)
    grad_input, grad_gain_mlp = norm_back(
        contract_cols(grad_pre, w_gate_up), middle, scale_m, gain_mlp
    )
    grad_middle = grad_field + grad_input

    grad_branch = grad_middle.astype(jnp.bfloat16)
    grad_mixed = contract_cols(grad_branch, w_out).astype(jnp.bfloat16)
    grad_queries, grad_keys, grad_values = attend_backward(
        grad_mixed, queries_b, keys_b, values_b, total, allowed
    )
    grad_project = join_grads(grad_queries, grad_keys, grad_values, cosine, sine)
    grad_input, grad_gain_attn = norm_back(
        contract_cols(grad_project, w_qkv), field, scale_a, gain_attn
    )
    grad_tokens = grad_middle + grad_input

    gain_grads = jnp.stack([grad_gain_attn, grad_gain_mlp]).reshape(2, n_shard, owned_rows)
    gain_grads = jnp.pad(gain_grads.transpose(1, 0, 2), ((0, 0), (0, 6), (0, 0)))
    grad_down, grad_gate_up, grad_qkv, grad_out, gain_own = reduce_all(
        n_shard,
        n_replica,
        [hidden_t, normed_m_t, normed_a_t, mixed_t],
        [grad_last, grad_pre, grad_project, grad_branch],
        gain_grads,
    )
    grad_down, grad_gate_up, grad_qkv, grad_out = [
        grad.astype(jnp.float32) for grad in (grad_down, grad_gate_up, grad_qkv, grad_out)
    ]
    return (
        result,
        grad_tokens,
        gain_own[0:1],
        grad_qkv[None],
        grad_out[None],
        gain_own[1:2],
        grad_gate_up[None],
        grad_down[None],
    )


def solution(mesh):
    n_shard = mesh.shape["shard"]
    n_replica = mesh.shape["replica"]
    placed = (
        P(("shard", "replica"), None),
        P(("shard", "replica"), None),
        P(),
        P(),
        P(),
        P(None, "shard"),
        P(None, "shard", None),
        P(None, "shard", None),
        P(None, "shard"),
        P(None, "shard", None),
        P(None, "shard", None),
    )

    def run(*args):
        return body(n_shard, n_replica, *args)

    return jax.shard_map(
        run,
        mesh=mesh,
        in_specs=placed,
        out_specs=(
            P(("shard", "replica"), None),
            P(("shard", "replica"), None),
            P(None, "shard"),
            P(None, "shard", None),
            P(None, "shard", None),
            P(None, "shard"),
            P(None, "shard", None),
            P(None, "shard", None),
        ),
        check_vma=False,
    )
```

```python
import functools

import jax
import jax.numpy as jnp
from jax import lax
from jax.experimental import pallas as pl
from jax.experimental.pallas import tpu as pltpu
from jax.sharding import PartitionSpec as P

HEADS = 16
KV_HEADS = 8
HEAD = 96
FF = 4096
BLOCK = 128

epsilon = 1e-05
rope_base = 100000.0


def rope_tables(position):
    half = HEAD // 2
    freqs = rope_base ** (-(jnp.arange(half, dtype=jnp.float32) * 2.0) / HEAD)
    angles = position.astype(jnp.float32)[:, None] * freqs[None, :]
    cosine = jnp.cos(angles)
    sine = jnp.sin(angles)
    return (jnp.concatenate([cosine, cosine], axis=-1), jnp.concatenate([sine, sine], axis=-1))


def locate(device, seq_lengths, seq_device, seq_offsets, rows):
    starts = seq_offsets * BLOCK
    local = jnp.arange(rows, dtype=jnp.int32)
    labels = jnp.arange(seq_lengths.shape[0], dtype=jnp.int32)
    hits = (
        (seq_device[None, :] == device)
        & (local[:, None] >= starts[None, :])
        & (local[:, None] < (starts + seq_lengths)[None, :])
    )
    segment = jnp.max(jnp.where(hits, labels[None, :], -1), axis=1)
    begin = jnp.sum(jnp.where(hits, starts[None, :], 0), axis=1)
    return (segment, local - begin)


def mask_of(segment):
    local = jnp.arange(segment.shape[0], dtype=jnp.int32)
    return (segment[:, None] == segment[None, :]) & (local[None, :] <= local[:, None])


def contract_rows(left, right):
    return lax.dot_general(
        left, right, (((0,), (0,)), ((), ())), preferred_element_type=jnp.float32
    )


def gate_back(grad_hidden, gate, upper):
    sigma = jax.nn.sigmoid(gate)
    grad_gate = grad_hidden * upper * sigma * (1.0 + gate * (1.0 - sigma))
    grad_upper = grad_hidden * (gate * sigma)
    return (grad_gate.astype(jnp.bfloat16), grad_upper.astype(jnp.bfloat16))


MESH = pl.DeviceIdType.MESH


def submasks(order, step):
    masks = [0]
    for bit in order[:step]:
        masks += [mask | bit for mask in masks]
    return masks


def greet(partners):
    barrier = pltpu.get_barrier_semaphore()
    for partner in partners:
        pl.semaphore_signal(barrier, inc=1, device_id=partner, device_id_type=MESH)
    pl.semaphore_wait(barrier, len(partners))


class Item:
    def __init__(self, n_shard, own, full, cols, single, sems):
        self.shard, replica = lax.axis_index("shard"), lax.axis_index("replica")
        self.replica = replica
        core, pair = lax.rem(replica, 2), lax.rem(replica // 2, 2)
        self.bits = [1 << i for i in range(n_shard.bit_length() - 1)]
        self.n_shard = n_shard
        self.own, self.full, self.cols = own, full, cols
        self.rows = own.shape[0]
        self.load_sem, self.local_sem, self.send_sem, self.recv_sem = sems
        half = self.rows // 2
        common = half - 2 * single
        base = core * half
        self.parts = [
            (base + pair * (single + common), single, self.bits),
            (base + single, common, self.bits[1:] + self.bits[:1]),
        ]
        self.mate = (base + (1 - pair) * (single + common), single)
        self.half = (base, half)
        self.other_half = ((1 - core) * half, half)
        self.number = {}
        self.waited, self.started = set(), {}

    def index(self, key):
        return self.number.setdefault(key, len(self.number))

    def window(self, mask, span):
        start = pl.multiple_of((self.shard ^ mask) * self.rows + span[0], 16)
        return self.full.at[pl.ds(start, span[1]), self.cols]

    def send(self, key, src, dst, device):
        if key in self.started:
            return
        index = self.index(key)
        copy = pltpu.make_async_remote_copy(
            src_ref=src,
            dst_ref=dst,
            send_sem=self.send_sem.at[index],
            recv_sem=self.recv_sem.at[index],
            device_id=device,
            device_id_type=MESH,
        )
        copy.start()
        self.started[key] = copy

    def landed(self, key, span):
        if key in self.waited:
            return
        self.waited.add(key)
        window = self.window(key[2], span)
        pltpu.make_async_remote_copy(
            src_ref=window,
            dst_ref=window,
            send_sem=self.send_sem.at[self.index(key)],
            recv_sem=self.recv_sem.at[self.index(key)],
            device_id={"replica": self.replica ^ 1},
            device_id_type=MESH,
        ).wait_recv()

    def load(self, source):
        self.loading = pltpu.make_async_copy(source.at[:, self.cols], self.own.at[:, self.cols], self.load_sem)
        self.loading.start()

    def over_shard(self, part, step, mask):
        start, size, order = self.parts[part]
        bit = order[step]
        window = self.window(mask, (start, size))
        src = window
        if mask == 0:
            src = self.own.at[pl.ds(pl.multiple_of(start, 16), size), self.cols]
        self.send(("shard", part, mask | bit), src, window, {"shard": self.shard ^ bit})

    def first(self):
        self.loading.wait()
        for step in range(len(self.bits)):
            for part in range(2):
                self.over_shard(part, step, 0)
        start = pl.multiple_of(self.shard * self.rows, 16)
        self.placing = pltpu.make_async_copy(
            self.own.at[:, self.cols], self.full.at[pl.ds(start, self.rows), self.cols], self.local_sem
        )
        self.placing.start()

    def arrive(self, part, mask):
        span = self.parts[part][:2]
        self.landed(("shard", part, mask), span)
        if part == 0:
            window = self.window(mask, span)
            self.send(("pair", 0, mask), window, window, {"replica": self.replica ^ 2})

    def relay(self):
        for step in range(1, len(self.bits)):
            for part in range(2):
                for mask in submasks(self.parts[part][2], step)[1:]:
                    self.arrive(part, mask)
                    self.over_shard(part, step, mask)

    def pass_on(self):
        for mask in range(1, self.n_shard):
            self.arrive(0, mask)

    def across(self):
        for mask in range(1, self.n_shard):
            self.arrive(1, mask)
            self.landed(("pair", 0, mask), self.mate)
            window = self.window(mask, self.half)
            self.send(("core", 0, mask), window, window, {"replica": self.replica ^ 1})

    def complete(self):
        for mask in range(1, self.n_shard):
            self.landed(("core", 0, mask), self.other_half)
        self.placing.wait()

    def finish(self):
        for copy in self.started.values():
            copy.wait_send()


def round_to(value, unit):
    return max(unit, int(value / unit + 0.5) * unit)


def scaled_rows(field):
    return field * lax.rsqrt(jnp.mean(field * field, axis=-1, keepdims=True) + epsilon)


QUAD = 4 * HEAD
TILE = 512


def forward_kernel(n_shard, plan, stages, *refs):
    refs = list(refs)
    take = lambda n: [refs.pop(0) for _ in range(n)]
    weights, (gain, tokens, cosine, sine, mask) = take(4), take(5)
    fulls = take(4)
    turned_a, turned_o, turned_m, turned_h, lse, middle, gate_up, gains = take(8)
    heads_out = take(3)
    owns, (gain_all, w_qkv, w_out, tiles) = take(4), take(4)
    field, normed, project, q_heads, k_heads, v_heads, mixed = take(7)
    out_a, out_o, out_m, out_h, out_lse, out_gain, pre = take(7)
    load_sem, local_sem, send_sem, recv_sem, gain_send, gain_recv, gain_sem, tile_sem, out_sem = take(9)
    shard, replica = lax.axis_index("shard"), lax.axis_index("replica")
    rows, model = tokens.shape
    owned = gain.shape[1]

    items = []
    for n, (weight, start, size, single) in enumerate(plan):
        item = Item(
            n_shard,
            owns[weight],
            fulls[weight],
            pl.ds(start, size),
            single,
            (load_sem.at[n], local_sem.at[n], send_sem.at[n], recv_sem.at[n]),
        )
        item.load(weights[weight])
        items.append(item)
    gain_own = pltpu.make_async_copy(gain, gain_all.at[shard], gain_sem.at[0])
    gain_own.start()
    greet(
        [{"shard": shard ^ other} for other in range(1, n_shard)]
        + [{"replica": replica ^ 1}, {"replica": replica ^ 2}]
    )

    def gain_copy(other, index):
        return pltpu.make_async_remote_copy(
            src_ref=gain,
            dst_ref=gain_all.at[index],
            send_sem=gain_send.at[other - 1],
            recv_sem=gain_recv.at[other - 1],
            device_id={"shard": shard ^ other},
            device_id_type=MESH,
        )

    for other in range(1, n_shard):
        gain_copy(other, shard).start()

    leaving = []

    def leave(src, dst):
        copy = pltpu.make_async_copy(src, dst, out_sem.at[len(leaving)])
        copy.start()
        leaving.append(copy)

    def norm(row):
        value = scaled_rows(field[...])
        for other in range(n_shard):
            span = slice(other * owned, (other + 1) * owned)
            normed[:, span] = (value[:, span] * out_gain[row : row + 1, span]).astype(jnp.bfloat16)

    def fetch(weight, index, start, dst):
        copy = pltpu.make_async_copy(
            fulls[weight].at[:, pl.ds(start, dst.shape[1])], dst, tile_sem.at[index]
        )
        copy.start()
        return copy

    def begin():
        gain_own.wait()
        for other in range(1, n_shard):
            gain_copy(other, shard ^ other).wait()
        for other in range(n_shard):
            out_gain[:, other * owned : (other + 1) * owned] = gain_all[other]
        leave(out_gain, gains)
        field[...] = tokens[...].astype(jnp.float32)
        norm(0)
        out_a[...] = normed[...].astype(jnp.float32).T.astype(jnp.bfloat16)
        leave(out_a, turned_a)

    def projections():
        loads = [
            fetch(0, n, n * TILE, w_qkv.at[:, pl.ds(n * TILE, TILE)])
            for n in range(w_qkv.shape[1] // TILE)
        ]
        for n, load in enumerate(loads):
            load.wait()
            span = pl.ds(n * TILE, TILE)
            project[:, span] = jnp.dot(
                normed[...], w_qkv[:, span], preferred_element_type=jnp.float32
            )

    lane = lax.broadcasted_iota(jnp.int32, (rows, QUAD), 1)
    first_half = lax.rem(lane, HEAD) < HEAD // 2
    in_head = lax.broadcasted_iota(jnp.int32, (rows, 128), 1) < HEAD

    def rope():
        for quad, heads in enumerate([q_heads] * 4 + [k_heads] * 2 + [v_heads] * 2):
            span = slice(quad * QUAD, (quad + 1) * QUAD)
            value = project[:, span]
            if quad < 6:
                turned = jnp.where(
                    first_half,
                    -pltpu.roll(value, QUAD - HEAD // 2, 1),
                    pltpu.roll(value, HEAD // 2, 1),
                )
                value = value * cosine[...] + turned * sine[...]
            base = [0, 4, 8, 12, 0, 4, 0, 4][quad]
            for n in range(4):
                moved = value if n == 0 else pltpu.roll(value, QUAD - n * HEAD, 1)
                heads[base + n] = jnp.where(in_head, moved[:, :128], 0.0).astype(jnp.bfloat16)
        for src, dst in zip((q_heads, k_heads, v_heads), heads_out):
            leave(src, dst)
        out_lse[...] = jnp.zeros_like(out_lse)

    def attend(quad):
        allowed = mask[...] > 0.5
        spot = lax.broadcasted_iota(jnp.int32, (rows, 128), 1)
        total = jnp.zeros((rows, QUAD), jnp.float32)
        for n in range(4):
            query = q_heads[4 * quad + n]
            key = k_heads[2 * quad + n // 2]
            scores = lax.dot_general(
                query, key, (((1,), (1,)), ((), ())), preferred_element_type=jnp.float32
            ) * HEAD ** (-0.5)
            scores = jnp.where(allowed, scores, -1e30)
            top = jnp.max(scores, axis=-1, keepdims=True)
            size = jnp.log(jnp.sum(jnp.exp(scores - top), axis=-1, keepdims=True)) + top
            share = jnp.exp(scores - size).astype(jnp.bfloat16)
            part = jnp.dot(
                share, v_heads[2 * quad + n // 2], preferred_element_type=jnp.float32
            )
            part = jnp.concatenate([part, jnp.zeros((rows, QUAD - 128), jnp.float32)], axis=1)
            total = total + (part if n == 0 else pltpu.roll(part, n * HEAD, 1))
            out_lse[...] += jnp.where(spot == 4 * quad + n, size, 0.0)
        mixed[:, quad * QUAD : (quad + 1) * QUAD] = total.astype(jnp.bfloat16)
        span = slice(quad * QUAD, (quad + 1) * QUAD)
        out_o[span, :] = total.T.astype(jnp.bfloat16)

    def attended():
        leave(out_o, turned_o)
        leave(out_lse, lse)

    def output():
        load = fetch(1, 0, 0, w_out)
        load.wait()
        for n in range(model // TILE):
            span = pl.ds(n * TILE, TILE)
            field[:, span] += jnp.dot(
                mixed[...], w_out[:, span], preferred_element_type=jnp.float32
            )
        leave(field, middle)
        norm(1)
        out_m[...] = normed[...].astype(jnp.float32).T.astype(jnp.bfloat16)
        leave(out_m, turned_m)

    hidden_units = gate_up.shape[1] // 2
    pairs = {}

    def fetch_pair(n):
        pairs[n] = [
            fetch(2, 2 * (n % 2) + k, k * hidden_units + n * TILE, tiles.at[n % 2, k])
            for k in range(2)
        ]

    def feed(n, last):
        if n not in pairs:
            fetch_pair(n)
        if n < last:
            fetch_pair(n + 1)
        for load in pairs[n]:
            load.wait()
        slot = n % 2
        if n >= 2:
            for copy in stored[n - 2]:
                copy.wait()
        both = []
        for k in range(2):
            value = jnp.dot(normed[...], tiles[slot, k], preferred_element_type=jnp.float32)
            pre[slot, k] = value
            both.append(value)
        gate, upper = both
        hidden = gate * jax.nn.sigmoid(gate) * upper
        out_h[n * TILE : (n + 1) * TILE, :] = hidden.T.astype(jnp.bfloat16)
        stored[n] = []
        for k in range(2):
            copy = pltpu.make_async_copy(
                pre.at[slot, k],
                gate_up.at[:, pl.ds(k * hidden_units + n * TILE, TILE)],
                tile_sem.at[4 + 2 * slot + k],
            )
            copy.start()
            stored[n].append(copy)

    stored = {}
    half = hidden_units // TILE // 2
    work = {
        "begin": begin,
        "project": lambda: (projections(), rope()),
        "attend0": lambda: [attend(n) for n in range(2)],
        "attend1": lambda: ([attend(n) for n in range(2, 4)], attended()),
        "output": output,
        "feed0": lambda: [feed(n, half - 1) for n in range(half)],
        "feed1": lambda: [feed(n, 2 * half - 1) for n in range(half, 2 * half)],
    }
    phases = [Item.first, Item.relay, Item.pass_on, Item.across, Item.complete]
    for time in range(len(items) + len(phases) - 1):
        for late, phase in enumerate(phases):
            if 0 <= time - late < len(items):
                phase(items[time - late])
        for name in stages.get(time, ()):
            work[name]()
    leave(out_h, turned_h)
    for item in items:
        item.finish()
    for copies in list(stored.values())[-2:]:
        for copy in copies:
            copy.wait()
    for copy in leaving:
        copy.wait()


def gather_forward(n_shard, weights, gain, tokens, cosine, sine, mask):
    def single(weight, share):
        return round_to(weight.shape[0] // 2 * share, 16)

    qkv, out, gate_up, down = weights
    part = gate_up.shape[1] // 4
    rows, model = tokens.shape
    wide, hidden = gate_up.shape[1], gate_up.shape[1] // 2
    third = [single(weight, 0.333) for weight in weights]
    plan = [
        (0, 0, qkv.shape[1] // 2, third[0]),
        (0, qkv.shape[1] // 2, qkv.shape[1] // 2, third[0]),
        (1, 0, model, third[1]),
        (2, 0, part, third[2]),
        (2, 2 * part, part, third[2]),
        (2, part, part, third[2]),
        (2, 3 * part, part, third[2]),
        (3, 0, model // 2, third[3]),
        (3, model // 2, model // 2, third[3]),
    ]
    stages = {
        0: ["begin"],
        5: ["project"],
        6: ["attend0"],
        7: ["attend1"],
        8: ["output", "feed0"],
        10: ["feed1"],
    }
    copies = 4 * (n_shard - 1)
    n = len(plan)
    anywhere = pl.BlockSpec(memory_space=pl.ANY)
    whole = pl.BlockSpec(memory_space=pltpu.VMEM)
    bf16, f32 = jnp.bfloat16, jnp.float32
    shape = jax.ShapeDtypeStruct
    heads = lambda count: pltpu.VMEM((count, rows, 128), bf16)
    return pl.pallas_call(
        functools.partial(forward_kernel, n_shard, plan, stages),
        out_shape=[shape((w.shape[0] * n_shard, w.shape[1]), w.dtype) for w in weights]
        + [
            shape((model, rows), bf16),
            shape((model, rows), bf16),
            shape((model, rows), bf16),
            shape((hidden, rows), bf16),
            shape((rows, 128), f32),
            shape((rows, model), f32),
            shape((rows, wide), f32),
            shape((2, model), f32),
        ]
        + [shape((count, rows, 128), bf16) for count in (HEADS, KV_HEADS, KV_HEADS)],
        in_specs=[anywhere] * 4 + [whole] * 5,
        out_specs=[anywhere] * 15,
        scratch_shapes=[pltpu.VMEM(w.shape, w.dtype) for w in weights]
        + [
            pltpu.VMEM((n_shard,) + gain.shape, f32),
            pltpu.VMEM((model, qkv.shape[1]), bf16),
            pltpu.VMEM((model, model), bf16),
            pltpu.VMEM((2, 2, model, TILE), bf16),
            pltpu.VMEM((rows, model), f32),
            pltpu.VMEM((rows, model), bf16),
            pltpu.VMEM((rows, qkv.shape[1]), f32),
            heads(HEADS),
            heads(KV_HEADS),
            heads(KV_HEADS),
            pltpu.VMEM((rows, model), bf16),
            pltpu.VMEM((model, rows), bf16),
            pltpu.VMEM((model, rows), bf16),
            pltpu.VMEM((model, rows), bf16),
            pltpu.VMEM((hidden, rows), bf16),
            pltpu.VMEM((rows, 128), f32),
            pltpu.VMEM((2, model), f32),
            pltpu.VMEM((2, 2, rows, TILE), f32),
            pltpu.SemaphoreType.DMA((n,)),
            pltpu.SemaphoreType.DMA((n,)),
            pltpu.SemaphoreType.DMA((n, copies)),
            pltpu.SemaphoreType.DMA((n, copies)),
            pltpu.SemaphoreType.DMA((n_shard - 1,)),
            pltpu.SemaphoreType.DMA((n_shard - 1,)),
            pltpu.SemaphoreType.DMA((1,)),
            pltpu.SemaphoreType.DMA((8,)),
            pltpu.SemaphoreType.DMA((16,)),
        ],
        compiler_params=pltpu.CompilerParams(
            collective_id=1, has_side_effects=True, vmem_limit_bytes=66_000_000
        ),
        name="gather_forward",
    )(*weights, gain, tokens, cosine, sine, mask)


SLOTS = 5


class Pipe:
    def __init__(self, n_shard, n_replica, begin, count, block, deliver, bufs, sems):
        self.shard, self.replica = lax.axis_index("shard"), lax.axis_index("replica")
        chip = self.replica // 2
        self.inner = lax.rem(chip, 2) != lax.rem(chip // 2, 2)
        self.steps = n_shard.bit_length() - 1
        self.swaps = [6] + [1 << k for k in range(3, n_replica.bit_length() - 1)]
        self.begin, self.count, self.block, self.deliver = begin, count, block, deliver
        bufs = list(bufs)
        self.out = [bufs.pop(0) for _ in range(self.steps)]
        self.into = [bufs.pop(0) for _ in range(self.steps)]
        self.kept = [bufs.pop(0) for _ in range(max(1, self.steps - 1))]
        self.fold_in = bufs.pop(0)
        self.swap_out = [bufs.pop(0) for _ in self.swaps]
        self.fold_out = self.swap_out[0]
        self.swap_in = [bufs.pop(0) for _ in self.swaps]
        self.final, self.across = bufs.pop(0), bufs.pop(0)
        self.send_sem, self.recv_sem, self.local_sem = sems
        self.last = self.steps + 2 + len(self.swaps)

    @staticmethod
    def scratch(n_shard, n_replica, rows, cols, dtype):
        steps = n_shard.bit_length() - 1
        swaps = n_replica.bit_length() - 3
        blocks = [n_shard >> (k + 1) for k in range(steps)]
        shapes = [pltpu.VMEM((SLOTS, b, rows, cols), dtype) for b in blocks * 2]
        shapes += [
            pltpu.VMEM((SLOTS, max(1, b // 2), rows, cols), jnp.float32)
            for b in blocks[: max(1, steps - 1)]
        ]
        one = (SLOTS, rows, cols)
        shapes += [pltpu.VMEM(one, dtype)] * (2 * swaps + 3)
        kinds = steps + swaps + 3
        return shapes, [
            pltpu.SemaphoreType.DMA((kinds, SLOTS)),
            pltpu.SemaphoreType.DMA((kinds, SLOTS)),
            pltpu.SemaphoreType.DMA((2, SLOTS)),
        ]

    def bit(self, chunk, step):
        return 1 << lax.rem(step + lax.rem(chunk, 2), self.steps)

    def mask(self, chunk, entry):
        found = 0
        for step in range(self.steps):
            if (entry >> step) & 1:
                found = found | self.bit(chunk, step)
        return found

    def copy(self, kind, slot, src, dst, device):
        return pltpu.make_async_remote_copy(
            src_ref=src.at[slot],
            dst_ref=dst.at[slot],
            send_sem=self.send_sem.at[kind, slot],
            recv_sem=self.recv_sem.at[kind, slot],
            device_id=device,
            device_id_type=MESH,
        )

    def halving(self, step, chunk, slot):
        device = {"shard": self.shard ^ self.bit(chunk, step)}
        return self.copy(step, slot, self.out[step], self.into[step], device)

    def folding(self, slot):
        return self.copy(
            self.steps, slot, self.fold_out, self.fold_in, {"replica": self.replica ^ 2}
        )

    def swapping(self, number, slot):
        device = {"replica": self.replica ^ self.swaps[number]}
        return self.copy(
            self.steps + 1 + number, slot, self.swap_out[number], self.swap_in[number], device
        )

    def unfolding(self, slot):
        kind = self.steps + 1 + len(self.swaps)
        return self.copy(kind, slot, self.final, self.final, {"replica": self.replica ^ 2})

    def crossing(self, slot):
        kind = self.steps + 2 + len(self.swaps)
        return self.copy(kind, slot, self.final, self.across, {"replica": self.replica ^ 1})

    def stage(self, number, chunk, slot):
        steps, swaps = self.steps, len(self.swaps)
        dtype = self.final.dtype
        if number == 0:
            for entry in range(1, 1 << steps, 2):
                self.out[0][slot, entry >> 1] = self.block(chunk, self.mask(chunk, entry)).astype(dtype)
            self.halving(0, chunk, slot).start()
        elif number <= steps:
            sums = []
            for entry in range(1 << (steps - number)):
                if number == 1:
                    sums.append(self.block(chunk, self.mask(chunk, 2 * entry)))
                else:
                    sums.append(self.kept[number - 2][slot, entry])
            self.halving(number - 1, chunk, slot).wait()
            for entry, value in enumerate(sums):
                value = value + self.into[number - 1][slot, entry].astype(jnp.float32)
                if number == steps:
                    @pl.when(self.inner)
                    def _(value=value):
                        self.kept[-1][slot, 0] = value

                    @pl.when(jnp.logical_not(self.inner))
                    def _(value=value):
                        self.fold_out[slot] = value.astype(dtype)
                        self.folding(slot).start()
                elif entry & 1:
                    self.out[number][slot, entry >> 1] = value.astype(dtype)
                else:
                    self.kept[number - 1][slot, entry >> 1] = value
            if number < steps:
                self.halving(number, chunk, slot).start()
        elif number == steps + 1:
            @pl.when(self.inner)
            def _():
                self.folding(slot).wait_recv()
                value = self.kept[-1][slot, 0] + self.fold_in[slot].astype(jnp.float32)
                self.swap_out[0][slot] = value.astype(dtype)
                self.swapping(0, slot).start()

            @pl.when(jnp.logical_not(self.inner))
            def _():
                self.folding(slot).wait_send()
        elif number <= steps + 1 + swaps:
            @pl.when(self.inner)
            def _():
                done = number - steps - 2
                self.swapping(done, slot).wait()
                value = self.swap_out[done][slot].astype(jnp.float32) + self.swap_in[done][
                    slot
                ].astype(jnp.float32)
                if done + 1 < swaps:
                    self.swap_out[done + 1][slot] = value.astype(dtype)
                    self.swapping(done + 1, slot).start()
                else:
                    self.final[slot] = value.astype(dtype)
                    self.unfolding(slot).start()
        elif number == self.last:
            @pl.when(jnp.logical_not(self.inner))
            def _():
                self.unfolding(slot).wait_recv()

            self.crossing(slot).start()
            self.deliver(chunk, 0, self.final.at[slot], self.local_sem.at[0, slot], True)
        else:
            @pl.when(self.inner)
            def _():
                self.unfolding(slot).wait_send()

            self.crossing(slot).wait()
            self.deliver(chunk, 1, self.across.at[slot], self.local_sem.at[1, slot], True)
            self.deliver(chunk, 0, self.final.at[slot], self.local_sem.at[0, slot], False)
            self.deliver(chunk, 1, self.across.at[slot], self.local_sem.at[1, slot], False)

    def run(self, time):
        for number in range(self.last + 2):
            chunk = time - self.begin - number

            @pl.when((chunk >= 0) & (chunk < self.count))
            def _(number=number, chunk=chunk):
                self.stage(number, chunk, lax.rem(chunk, SLOTS))

    def length(self):
        return self.begin + self.count + self.last + 1


DEEP_COLS = 128
WIDE_COLS = 256
EARLY = 16


def times_rows(left, right):
    return lax.dot_general(
        left, right, (((0,), (0,)), ((), ())), preferred_element_type=jnp.float32
    )


def times_cols(left, right):
    return lax.dot_general(
        left, right, (((1,), (1,)), ((), ())), preferred_element_type=jnp.float32
    )


def backward_kernel(n_shard, n_replica, *refs):
    refs = list(refs)
    take = lambda n: [refs.pop(0) for _ in range(n)]
    lefts, (w_down, w_gate_up, w_out, w_qkv, pre) = take(4), take(5)
    heads_in, middle_in = take(3), take(1)[0]
    grad_last, tokens, gain, lse, cosine, sine, mask = take(7)
    outs, (gain_out, grad_tokens) = take(4), take(2)
    deep_left, deep_right, wide_left, wide_right, other_right = take(5)
    tile_down, tile_up, tile_pre, tile_out = take(4)
    q_heads, k_heads, v_heads, middle, grad_middle, total, branch, joined, parts, gain_in = take(10)
    load_sem, pass_send, pass_recv, tile_send, tile_recv, tile_sem, head_sem, late_sem = take(8)
    n_bufs = (len(refs) - 9) // 3
    deep_bufs, deep_sems = take(n_bufs), take(3)
    wide_bufs, wide_sems = take(n_bufs), take(3)
    gain_bufs, gain_sems = take(n_bufs), take(3)
    shard, replica = lax.axis_index("shard"), lax.axis_index("replica")
    core = lax.rem(replica, 2)
    rows, model = grad_last.shape
    hidden = w_down.shape[0]
    wide = w_qkv.shape[1]
    deep_rows, wide_rows = outs[0].shape[0] // 2, outs[1].shape[0]
    halves = [model // 2, hidden, model // 2, wide // 2]
    starts = [0, 0, hidden, hidden + model // 2]
    n_deep = 2 * halves[0] // DEEP_COLS
    edges = [start // WIDE_COLS for start in starts[1:]] + [wide_right.shape[1] // WIDE_COLS]
    tile = hidden // EARLY
    twin = {"replica": replica ^ 1}

    greet(
        [{"shard": shard ^ (1 << k)} for k in range(n_shard.bit_length() - 1)]
        + [{"replica": replica ^ other} for other in [1, 2, 6]]
        + [{"replica": replica ^ (1 << k)} for k in range(3, n_replica.bit_length() - 1)]
    )

    def pass_over(src, dst, sems, index):
        return pltpu.make_async_remote_copy(
            src_ref=src,
            dst_ref=dst,
            send_sem=sems[0].at[index],
            recv_sem=sems[1].at[index],
            device_id=twin,
            device_id_type=MESH,
        )

    def half_of(which, side):
        return pl.ds(pl.multiple_of(side * halves[which], 128), halves[which])

    place_left = [deep_left] + [wide_left.at[pl.ds(k * model, model)] for k in range(3)]
    loads, passes = [], []
    for k in range(4):
        loads.append(
            pltpu.make_async_copy(lefts[k], place_left[k].at[:, pl.ds(0, rows)], load_sem.at[k])
        )
        passes.append(
            pass_over(lefts[k], place_left[k].at[:, pl.ds(rows, rows)], (pass_send, pass_recv), k)
        )
        if k == 0:
            passes.append(
                pass_over(
                    grad_last.at[:, half_of(0, 1 - core)],
                    deep_right.at[pl.ds(rows, rows)],
                    (pass_send, pass_recv),
                    4,
                )
            )
    for copy in loads + passes:
        copy.start()
    late = [
        pltpu.make_async_copy(src, dst, late_sem.at[n])
        for n, (src, dst) in enumerate(
            zip([*heads_in, middle_in], [q_heads, k_heads, v_heads, middle])
        )
    ]
    for copy in late:
        copy.start()
    deep_right[pl.ds(0, rows), :] = grad_last[:, half_of(0, core)]
    total[...] = jnp.zeros_like(total)
    gain_in[...] = jnp.zeros_like(gain_in)
    tile_out[...] = jnp.zeros_like(tile_out)

    def tile_copies(n, slot):
        start = pl.multiple_of(n * tile, tile)
        cols = [pl.ds(start, tile), pl.ds(pl.multiple_of(hidden + n * tile, tile), tile)]
        pairs = [(w_down.at[cols[0]], tile_down.at[slot])]
        for k in range(2):
            pairs.append((w_gate_up.at[:, cols[k]], tile_up.at[slot, k]))
            pairs.append((pre.at[:, cols[k]], tile_pre.at[slot, k]))
        return [
            pltpu.make_async_copy(src, dst, tile_sem.at[slot, k])
            for k, (src, dst) in enumerate(pairs)
        ]

    def tile_pass(n):
        span = pl.ds(pl.multiple_of(n * tile, tile), tile)
        return pass_over(
            other_right.at[lax.rem(n, 4)],
            wide_right.at[pl.ds(rows, rows), span],
            (tile_send, tile_recv),
            n,
        )

    def hidden_tile(n):
        slot = lax.rem(n, 2)

        @pl.when(n + 1 < EARLY)
        def _():
            for copy in tile_copies(n + 1, 1 - slot):
                copy.start()

        for copy in tile_copies(n, slot):
            copy.wait()
        grad_hidden = times_cols(grad_last[...], tile_down[slot])
        grad_gate, grad_upper = gate_back(grad_hidden, tile_pre[slot, 0], tile_pre[slot, 1])
        span = pl.ds(pl.multiple_of(n * tile, tile), tile)
        first = core == 0
        wide_right[pl.ds(0, rows), span] = jnp.where(first, grad_gate, grad_upper)

        @pl.when(n >= 4)
        def _():
            tile_pass(n - 4).wait_send()

        other_right[lax.rem(n, 4)] = jnp.where(first, grad_upper, grad_gate)
        tile_pass(n).start()
        total[...] += times_cols(grad_gate, tile_up[slot, 0]) + times_cols(
            grad_upper, tile_up[slot, 1]
        )

    def norm_gradient(field, row):
        scale = lax.rsqrt(jnp.mean(field * field, axis=-1, keepdims=True) + epsilon)
        normed = field * scale
        grad = total[...]
        sums = jnp.sum(grad * normed, axis=0, keepdims=True)
        for other in range(n_shard):
            gain_in[other, row : row + 1, :] = sums[:, other * wide_rows : (other + 1) * wide_rows]
        inner = grad * gain[row : row + 1, :]
        return scale * (inner - normed * jnp.mean(inner * normed, axis=-1, keepdims=True))

    def share_right(which, source, index):
        span = pl.ds(starts[which], halves[which])
        wide_right[pl.ds(0, rows), span] = source[:, half_of(which, core)]
        return pass_over(
            source.at[:, half_of(which, 1 - core)],
            wide_right.at[pl.ds(rows, rows), span],
            (pass_send, pass_recv),
            index,
        )

    def between():
        for copy in late:
            copy.wait()
        for n in range(EARLY - 4, EARLY):
            tile_pass(n).wait_send()
        grad_middle[...] = grad_last[...].astype(jnp.float32) + norm_gradient(middle[...], 1)
        branch[...] = grad_middle[...].astype(jnp.bfloat16)
        share_right(2, branch, 5).start()
        total[...] = jnp.zeros_like(total)
        for copy in qkv_copies(0, 0):
            copy.start()

    per = HEADS // KV_HEADS

    def head_copies(key_head, slot):
        return [
            pltpu.make_async_copy(
                w_out.at[pl.ds(pl.multiple_of((per * key_head + n) * HEAD, 32), HEAD)],
                tile_out.at[slot, n, pl.ds(0, HEAD)],
                head_sem.at[slot, n],
            )
            for n in range(per)
        ]

    spot = lax.broadcasted_iota(jnp.int32, (rows, 128), 1)

    def unrope(value):
        moved = value * sine[...]
        turned = jnp.where(
            spot < HEAD // 2,
            -pltpu.roll(moved, 128 - HEAD // 2, 1),
            pltpu.roll(moved, HEAD // 2, 1),
        )
        return jnp.where(spot < HEAD, value * cosine[...] - turned, 0.0).astype(jnp.bfloat16)

    def attention(key_head):
        slot = lax.rem(key_head, 2)

        @pl.when(key_head + 1 < KV_HEADS)
        def _():
            for copy in head_copies(key_head + 1, 1 - slot):
                copy.start()

        for copy in head_copies(key_head, slot):
            copy.wait()
        allowed = mask[...] > 0.5
        factor = HEAD ** (-0.5)
        key, value = k_heads[key_head], v_heads[key_head]
        grad_key = jnp.zeros((rows, 128), jnp.float32)
        grad_value = jnp.zeros((rows, 128), jnp.float32)
        for n in range(per):
            head = per * key_head + n
            query = q_heads[head]
            grad_mixed = times_cols(branch[...], tile_out[slot, n]).astype(jnp.bfloat16)
            size = jnp.sum(jnp.where(spot == head, lse[...], 0.0), axis=-1, keepdims=True)
            scores = jnp.where(allowed, times_cols(query, key) * factor, -1e30)
            share = jnp.exp(scores - size)
            grad_value = grad_value + times_rows(share.astype(jnp.bfloat16), grad_mixed)
            grad_share = times_cols(grad_mixed, value)
            inner = jnp.sum(share * grad_share, axis=-1, keepdims=True)
            grad_scores = (share * (grad_share - inner)).astype(jnp.bfloat16)
            grad_query = jnp.dot(grad_scores, key, preferred_element_type=jnp.float32) * factor
            parts[head] = unrope(grad_query)
            grad_key = grad_key + times_rows(grad_scores, query)
        parts[HEADS + key_head] = unrope(grad_key * factor)
        parts[HEADS + KV_HEADS + key_head] = grad_value.astype(jnp.bfloat16)

    quad = 4 * HEAD

    def join():
        for group in range(wide // quad):
            value = jnp.zeros((rows, quad), jnp.float32)
            for n in range(4):
                part = parts[4 * group + n].astype(jnp.float32)
                part = jnp.concatenate([part, jnp.zeros((rows, quad - 128), jnp.float32)], axis=1)
                value = value + (part if n == 0 else pltpu.roll(part, n * HEAD, 1))
            joined[:, group * quad : (group + 1) * quad] = value.astype(jnp.bfloat16)
        share_right(3, joined, 6).start()

    n_last = wide // (2 * tile)

    def qkv_copies(n, slot):
        return [
            pltpu.make_async_copy(
                w_qkv.at[:, pl.ds(pl.multiple_of((2 * n + k) * tile, tile), tile)],
                tile_up.at[slot, k],
                tile_sem.at[slot, k],
            )
            for k in range(2)
        ]

    def input_tile(n):
        slot = lax.rem(n, 2)

        @pl.when(n + 1 < n_last)
        def _():
            for copy in qkv_copies(n + 1, 1 - slot):
                copy.start()

        for copy in qkv_copies(n, slot):
            copy.wait()
        for k in range(2):
            span = pl.ds(pl.multiple_of((2 * n + k) * tile, tile), tile)
            total[...] += times_cols(joined[:, span], tile_up[slot, k])

    def end():
        grad_tokens[...] = grad_middle[...] + norm_gradient(tokens[...].astype(jnp.float32), 0)

    def deep_block(chunk, other):
        start = (shard ^ other) * (2 * deep_rows) + (chunk // (n_deep // 2)) * deep_rows
        left = deep_left[pl.ds(pl.multiple_of(start, 16), deep_rows), :]
        cols = lax.rem(chunk, n_deep // 2) * DEEP_COLS
        right = deep_right[:, pl.ds(pl.multiple_of(cols, 128), DEEP_COLS)]
        return jnp.dot(left, right, preferred_element_type=jnp.float32)

    def wide_block(chunk, other):
        weight = (chunk >= edges[1]).astype(jnp.int32) + (chunk >= edges[2]).astype(jnp.int32)
        start = weight * model + (shard ^ other) * wide_rows
        left = wide_left[pl.ds(pl.multiple_of(start, 16), wide_rows), :]
        right = wide_right[:, pl.ds(pl.multiple_of(chunk * WIDE_COLS, 128), WIDE_COLS)]
        return jnp.dot(left, right, preferred_element_type=jnp.float32)

    def put(out, span, start, size, src, sem, begin):
        copy = pltpu.make_async_copy(
            src, out.at[span, pl.ds(pl.multiple_of(start, 128), size)], sem
        )
        if begin:
            copy.start()
        else:
            copy.wait()

    def deep_deliver(chunk, side, src, sem, begin):
        half = core if side == 0 else 1 - core
        first = pl.multiple_of((chunk // (n_deep // 2)) * deep_rows, 16)
        start = half * halves[0] + lax.rem(chunk, n_deep // 2) * DEEP_COLS
        put(outs[0], pl.ds(first, deep_rows), start, DEEP_COLS, src, sem, begin)

    def wide_deliver(chunk, side, src, sem, begin):
        half = core if side == 0 else 1 - core
        for k in range(3):
            @pl.when((chunk >= edges[k]) & (chunk < edges[k + 1]))
            def _(k=k):
                start = half * halves[k + 1] + (chunk - edges[k]) * WIDE_COLS
                put(outs[k + 1], slice(None), start, WIDE_COLS, src, sem, begin)

    def gain_deliver(chunk, side, src, sem, begin):
        if side == 1 and begin:
            gain_out[...] = gain_pipe.final[0] + src[...]

    between_at = EARLY
    join_at = between_at + 1 + KV_HEADS
    end_at = join_at + 1 + n_last
    size = (n_shard, n_replica)
    deep = Pipe(*size, 0, n_deep, deep_block, deep_deliver, deep_bufs, deep_sems)
    wide_pipe = Pipe(
        *size, n_deep, edges[3], wide_block, wide_deliver, wide_bufs, wide_sems
    )
    gain_pipe = Pipe(
        *size, end_at + 1, 1, lambda chunk, other: gain_in[shard ^ other], gain_deliver, gain_bufs, gain_sems
    )
    for copy in tile_copies(0, 0):
        copy.start()
    for copy in head_copies(0, 0):
        copy.start()
    loads[0].wait()
    passes[0].wait()
    passes[1].wait()

    def step(time, carry):
        def at(first, count, run):
            @pl.when((time >= first) & (time < first + count))
            def _():
                run(time - first)

        @pl.when(time == n_deep)
        def _():
            for k in range(1, 4):
                loads[k].wait()
                passes[k + 1].wait()

        at(n_deep, EARLY, lambda n: tile_pass(n).wait_recv())
        at(n_deep + edges[1], 1, lambda n: share_wait(2, branch, 5))
        at(n_deep + edges[2], 1, lambda n: share_wait(3, joined, 6))
        deep.run(time)
        wide_pipe.run(time)
        gain_pipe.run(time)
        at(0, EARLY, hidden_tile)
        at(between_at, 1, lambda n: between())
        at(between_at + 1, KV_HEADS, attention)
        at(join_at, 1, lambda n: join())
        at(join_at + 1, n_last, input_tile)
        at(end_at, 1, lambda n: end())
        return carry

    def share_wait(which, source, index):
        span = pl.ds(starts[which], halves[which])
        pass_over(
            source.at[:, half_of(which, 1 - core)],
            wide_right.at[pl.ds(rows, rows), span],
            (pass_send, pass_recv),
            index,
        ).wait()

    lax.fori_loop(0, max(wide_pipe.length(), gain_pipe.length()), step, 0)


def backward_all(n_shard, n_replica, lefts, weights, pre, heads, middle, small):
    grad_last, tokens, gain, lse = small[:4]
    rows, model = grad_last.shape
    w_down, w_gate_up, w_out, w_qkv = weights
    hidden, wide = w_down.shape[0], w_qkv.shape[1]
    tile = hidden // EARLY
    owned = [w.shape[0] // n_shard for w in weights]
    anywhere = pl.BlockSpec(memory_space=pl.ANY)
    whole = pl.BlockSpec(memory_space=pltpu.VMEM)
    bf16, f32 = jnp.bfloat16, jnp.float32
    size = (n_shard, n_replica)
    deep_bufs, deep_sems = Pipe.scratch(*size, owned[0] // 2, DEEP_COLS, bf16)
    wide_bufs, wide_sems = Pipe.scratch(*size, owned[1], WIDE_COLS, bf16)
    gain_bufs, gain_sems = Pipe.scratch(*size, 8, owned[1], f32)
    dma = pltpu.SemaphoreType.DMA
    return pl.pallas_call(
        functools.partial(backward_kernel, n_shard, n_replica),
        out_shape=[
            jax.ShapeDtypeStruct((own, w.shape[1]), bf16) for own, w in zip(owned, weights)
        ]
        + [
            jax.ShapeDtypeStruct((8, owned[1]), f32),
            jax.ShapeDtypeStruct((rows, model), f32),
        ],
        in_specs=[anywhere] * 13 + [whole] * 7,
        out_specs=[anywhere] * 4 + [whole] * 2,
        scratch_shapes=[
            pltpu.VMEM((hidden, 2 * rows), bf16),
            pltpu.VMEM((2 * rows, model // 2), bf16),
            pltpu.VMEM((3 * model, 2 * rows), bf16),
            pltpu.VMEM((2 * rows, hidden + model // 2 + wide // 2), bf16),
            pltpu.VMEM((4, rows, tile), bf16),
            pltpu.VMEM((2, tile, model), bf16),
            pltpu.VMEM((2, 2, model, tile), bf16),
            pltpu.VMEM((2, 2, rows, tile), f32),
            pltpu.VMEM((2, HEADS // KV_HEADS, 128, model), bf16),
            pltpu.VMEM((HEADS, rows, 128), bf16),
            pltpu.VMEM((KV_HEADS, rows, 128), bf16),
            pltpu.VMEM((KV_HEADS, rows, 128), bf16),
            pltpu.VMEM((rows, model), f32),
            pltpu.VMEM((rows, model), f32),
            pltpu.VMEM((rows, model), f32),
            pltpu.VMEM((rows, model), bf16),
            pltpu.VMEM((rows, wide), bf16),
            pltpu.VMEM((HEADS + 2 * KV_HEADS, rows, 128), bf16),
            pltpu.VMEM((n_shard, 8, owned[1]), f32),
            dma((4,)),
            dma((7,)),
            dma((7,)),
            dma((EARLY,)),
            dma((EARLY,)),
            dma((2, 5)),
            dma((2, HEADS // KV_HEADS)),
            dma((4,)),
            *deep_bufs,
            *deep_sems,
            *wide_bufs,
            *wide_sems,
            *gain_bufs,
            *gain_sems,
        ],
        compiler_params=pltpu.CompilerParams(
            collective_id=2, has_side_effects=True, vmem_limit_bytes=67_043_328
        ),
        name="backward_reduce",
    )(*lefts, *weights, pre, *heads, middle, *small)


def body(
    n_shard,
    n_replica,
    tokens,
    cotangent,
    seq_lengths,
    seq_device,
    seq_offsets,
    norm_attn,
    w_qkv,
    w_out,
    norm_mlp,
    w_gate_up,
    w_down,
):
    rows, model = tokens.shape
    w_qkv, w_out, w_gate_up, w_down = w_qkv[0], w_out[0], w_gate_up[0], w_down[0]
    owned_rows = w_qkv.shape[0]

    device = lax.axis_index(("shard", "replica"))
    segment, position = locate(device, seq_lengths, seq_device, seq_offsets, rows)
    live = (segment >= 0).astype(jnp.float32)[:, None]
    cosine, sine = rope_tables(position)
    allowed = mask_of(segment)

    cosine, sine = jnp.tile(cosine, (1, 4)), jnp.tile(sine, (1, 4))
    allowed = allowed.astype(jnp.float32)
    (
        w_qkv,
        w_out,
        w_gate_up,
        w_down,
        normed_a,
        mixed,
        normed_m,
        hidden,
        lse,
        middle,
        pre,
        gains,
        *heads,
    ) = gather_forward(
        n_shard,
        (w_qkv, w_out, w_gate_up, w_down),
        jnp.concatenate([norm_attn, norm_mlp], axis=0).astype(jnp.float32),
        tokens,
        cosine,
        sine,
        allowed,
    )
    result = ((middle + contract_rows(hidden, w_down)) * live).astype(jnp.bfloat16)
    grad_last = (cotangent.astype(jnp.float32) * live).astype(jnp.bfloat16)
    grad_down, grad_gate_up, grad_out, grad_qkv, gain_own, grad_tokens = backward_all(
        n_shard,
        n_replica,
        [hidden, normed_m, mixed, normed_a],
        [w_down, w_gate_up, w_out, w_qkv],
        pre,
        heads,
        middle,
        [grad_last, tokens, gains, lse, cosine[:, :128], sine[:, :128], allowed],
    )
    grad_down, grad_gate_up, grad_qkv, grad_out = [
        grad.astype(jnp.float32) for grad in (grad_down, grad_gate_up, grad_qkv, grad_out)
    ]
    return (
        result,
        grad_tokens,
        gain_own[0:1],
        grad_qkv[None],
        grad_out[None],
        gain_own[1:2],
        grad_gate_up[None],
        grad_down[None],
    )


def solution(mesh):
    n_shard = mesh.shape["shard"]
    n_replica = mesh.shape["replica"]
    placed = (
        P(("shard", "replica"), None),
        P(("shard", "replica"), None),
        P(),
        P(),
        P(),
        P(None, "shard"),
        P(None, "shard", None),
        P(None, "shard", None),
        P(None, "shard"),
        P(None, "shard", None),
        P(None, "shard", None),
    )

    def run(*args):
        return body(n_shard, n_replica, *args)

    return jax.shard_map(
        run,
        mesh=mesh,
        in_specs=placed,
        out_specs=(
            P(("shard", "replica"), None),
            P(("shard", "replica"), None),
            P(None, "shard"),
            P(None, "shard", None),
            P(None, "shard", None),
            P(None, "shard"),
            P(None, "shard", None),
            P(None, "shard", None),
        ),
        check_vma=False,
    )
```

```python
import functools

import jax
import jax.numpy as jnp
from jax import lax
from jax.experimental import pallas as pl
from jax.experimental.pallas import tpu as pltpu
from jax.sharding import PartitionSpec as P

HEADS = 16
KV_HEADS = 8
HEAD = 96
FF = 4096
BLOCK = 128

epsilon = 1e-05
rope_base = 100000.0


def rope_tables(position):
    half = HEAD // 2
    freqs = rope_base ** (-(jnp.arange(half, dtype=jnp.float32) * 2.0) / HEAD)
    angles = position.astype(jnp.float32)[:, None] * freqs[None, :]
    cosine = jnp.cos(angles)
    sine = jnp.sin(angles)
    return (jnp.concatenate([cosine, cosine], axis=-1), jnp.concatenate([sine, sine], axis=-1))


def locate(device, seq_lengths, seq_device, seq_offsets, rows):
    starts = seq_offsets * BLOCK
    local = jnp.arange(rows, dtype=jnp.int32)
    labels = jnp.arange(seq_lengths.shape[0], dtype=jnp.int32)
    hits = (
        (seq_device[None, :] == device)
        & (local[:, None] >= starts[None, :])
        & (local[:, None] < (starts + seq_lengths)[None, :])
    )
    segment = jnp.max(jnp.where(hits, labels[None, :], -1), axis=1)
    begin = jnp.sum(jnp.where(hits, starts[None, :], 0), axis=1)
    return (segment, local - begin)


def mask_of(segment):
    local = jnp.arange(segment.shape[0], dtype=jnp.int32)
    return (segment[:, None] == segment[None, :]) & (local[None, :] <= local[:, None])


def gate_back(grad_hidden, gate, upper):
    sigma = jax.nn.sigmoid(gate)
    grad_gate = grad_hidden * upper * sigma * (1.0 + gate * (1.0 - sigma))
    grad_upper = grad_hidden * (gate * sigma)
    return (grad_gate.astype(jnp.bfloat16), grad_upper.astype(jnp.bfloat16))


MESH = pl.DeviceIdType.MESH


def submasks(order, step):
    masks = [0]
    for bit in order[:step]:
        masks += [mask | bit for mask in masks]
    return masks


def greet(partners):
    barrier = pltpu.get_barrier_semaphore()
    for partner in partners:
        pl.semaphore_signal(barrier, inc=1, device_id=partner, device_id_type=MESH)
    pl.semaphore_wait(barrier, len(partners))


class Item:
    def __init__(self, n_shard, own, full, cols, single, sems):
        self.shard, replica = lax.axis_index("shard"), lax.axis_index("replica")
        self.replica = replica
        core, pair = lax.rem(replica, 2), lax.rem(replica // 2, 2)
        self.bits = [1 << i for i in range(n_shard.bit_length() - 1)]
        self.n_shard = n_shard
        self.own, self.full, self.cols = own, full, cols
        self.rows = own.shape[0]
        self.load_sem, self.local_sem, self.send_sem, self.recv_sem = sems
        half = self.rows // 2
        common = half - 2 * single
        base = core * half
        self.parts = [
            (base + pair * (single + common), single, self.bits),
            (base + single, common, self.bits[1:] + self.bits[:1]),
        ]
        self.mate = (base + (1 - pair) * (single + common), single)
        self.half = (base, half)
        self.other_half = ((1 - core) * half, half)
        self.number = {}
        self.waited, self.started = set(), {}

    def index(self, key):
        return self.number.setdefault(key, len(self.number))

    def window(self, mask, span):
        start = pl.multiple_of((self.shard ^ mask) * self.rows + span[0], 16)
        return self.full.at[pl.ds(start, span[1]), self.cols]

    def send(self, key, src, dst, device):
        if key in self.started:
            return
        index = self.index(key)
        copy = pltpu.make_async_remote_copy(
            src_ref=src,
            dst_ref=dst,
            send_sem=self.send_sem.at[index],
            recv_sem=self.recv_sem.at[index],
            device_id=device,
            device_id_type=MESH,
        )
        copy.start()
        self.started[key] = copy

    def landed(self, key, span):
        if key in self.waited:
            return
        self.waited.add(key)
        window = self.window(key[2], span)
        pltpu.make_async_remote_copy(
            src_ref=window,
            dst_ref=window,
            send_sem=self.send_sem.at[self.index(key)],
            recv_sem=self.recv_sem.at[self.index(key)],
            device_id={"replica": self.replica ^ 1},
            device_id_type=MESH,
        ).wait_recv()

    def load(self, source):
        self.loading = pltpu.make_async_copy(source.at[:, self.cols], self.own.at[:, self.cols], self.load_sem)
        self.loading.start()

    def over_shard(self, part, step, mask):
        start, size, order = self.parts[part]
        bit = order[step]
        window = self.window(mask, (start, size))
        src = window
        if mask == 0:
            src = self.own.at[pl.ds(pl.multiple_of(start, 16), size), self.cols]
        self.send(("shard", part, mask | bit), src, window, {"shard": self.shard ^ bit})

    def first(self):
        self.loading.wait()
        for step in range(len(self.bits)):
            for part in range(2):
                self.over_shard(part, step, 0)
        start = pl.multiple_of(self.shard * self.rows, 16)
        self.placing = pltpu.make_async_copy(
            self.own.at[:, self.cols], self.full.at[pl.ds(start, self.rows), self.cols], self.local_sem
        )
        self.placing.start()

    def arrive(self, part, mask):
        span = self.parts[part][:2]
        self.landed(("shard", part, mask), span)
        if part == 0:
            window = self.window(mask, span)
            self.send(("pair", 0, mask), window, window, {"replica": self.replica ^ 2})

    def relay(self):
        for step in range(1, len(self.bits)):
            for part in range(2):
                for mask in submasks(self.parts[part][2], step)[1:]:
                    self.arrive(part, mask)
                    self.over_shard(part, step, mask)

    def pass_on(self):
        for mask in range(1, self.n_shard):
            self.arrive(0, mask)

    def across(self):
        for mask in range(1, self.n_shard):
            self.arrive(1, mask)
            self.landed(("pair", 0, mask), self.mate)
            window = self.window(mask, self.half)
            self.send(("core", 0, mask), window, window, {"replica": self.replica ^ 1})

    def complete(self):
        for mask in range(1, self.n_shard):
            self.landed(("core", 0, mask), self.other_half)
        self.placing.wait()

    def finish(self):
        for copy in self.started.values():
            copy.wait_send()


def round_to(value, unit):
    return max(unit, int(value / unit + 0.5) * unit)


def scaled_rows(field):
    return field * lax.rsqrt(jnp.mean(field * field, axis=-1, keepdims=True) + epsilon)


QUAD = 4 * HEAD
TILE = 512


def forward_kernel(n_shard, plan, stages, *refs):
    refs = list(refs)
    take = lambda n: [refs.pop(0) for _ in range(n)]
    weights, (gain, tokens, cosine, sine, mask) = take(4), take(5)
    fulls = take(4)
    turned_a, turned_o, turned_m, turned_h, lse, middle, gate_up, gains = take(8)
    heads_out = take(3)
    owns, (gain_all, w_qkv, w_out, tiles) = take(4), take(4)
    field, normed, project, q_heads, k_heads, v_heads, mixed = take(7)
    out_a, out_o, out_m, out_h, out_lse, out_gain, pre = take(7)
    load_sem, local_sem, send_sem, recv_sem, gain_send, gain_recv, gain_sem, tile_sem, out_sem = take(9)
    shard, replica = lax.axis_index("shard"), lax.axis_index("replica")
    rows, model = tokens.shape
    owned = gain.shape[1]

    items = []
    for n, (weight, start, size, single) in enumerate(plan):
        item = Item(
            n_shard,
            owns[weight],
            fulls[weight],
            pl.ds(start, size),
            single,
            (load_sem.at[n], local_sem.at[n], send_sem.at[n], recv_sem.at[n]),
        )
        item.load(weights[weight])
        items.append(item)
    gain_own = pltpu.make_async_copy(gain, gain_all.at[shard], gain_sem.at[0])
    gain_own.start()
    greet(
        [{"shard": shard ^ other} for other in range(1, n_shard)]
        + [{"replica": replica ^ 1}, {"replica": replica ^ 2}]
    )

    def gain_copy(other, index):
        return pltpu.make_async_remote_copy(
            src_ref=gain,
            dst_ref=gain_all.at[index],
            send_sem=gain_send.at[other - 1],
            recv_sem=gain_recv.at[other - 1],
            device_id={"shard": shard ^ other},
            device_id_type=MESH,
        )

    for other in range(1, n_shard):
        gain_copy(other, shard).start()

    leaving = []

    def leave(src, dst):
        copy = pltpu.make_async_copy(src, dst, out_sem.at[len(leaving)])
        copy.start()
        leaving.append(copy)

    def norm(row):
        value = scaled_rows(field[...])
        for other in range(n_shard):
            span = slice(other * owned, (other + 1) * owned)
            normed[:, span] = (value[:, span] * out_gain[row : row + 1, span]).astype(jnp.bfloat16)

    def fetch(weight, index, start, dst):
        copy = pltpu.make_async_copy(
            fulls[weight].at[:, pl.ds(start, dst.shape[1])], dst, tile_sem.at[index]
        )
        copy.start()
        return copy

    def begin():
        gain_own.wait()
        for other in range(1, n_shard):
            gain_copy(other, shard ^ other).wait()
        for other in range(n_shard):
            out_gain[:, other * owned : (other + 1) * owned] = gain_all[other]
        leave(out_gain, gains)
        field[...] = tokens[...].astype(jnp.float32)
        norm(0)
        out_a[...] = normed[...].astype(jnp.float32).T.astype(jnp.bfloat16)
        leave(out_a, turned_a)

    def projections():
        loads = [
            fetch(0, n, n * TILE, w_qkv.at[:, pl.ds(n * TILE, TILE)])
            for n in range(w_qkv.shape[1] // TILE)
        ]
        for n, load in enumerate(loads):
            load.wait()
            span = pl.ds(n * TILE, TILE)
            project[:, span] = jnp.dot(
                normed[...], w_qkv[:, span], preferred_element_type=jnp.float32
            )

    lane = lax.broadcasted_iota(jnp.int32, (rows, QUAD), 1)
    first_half = lax.rem(lane, HEAD) < HEAD // 2
    in_head = lax.broadcasted_iota(jnp.int32, (rows, 128), 1) < HEAD

    def rope():
        for quad, heads in enumerate([q_heads] * 4 + [k_heads] * 2 + [v_heads] * 2):
            span = slice(quad * QUAD, (quad + 1) * QUAD)
            value = project[:, span]
            if quad < 6:
                turned = jnp.where(
                    first_half,
                    -pltpu.roll(value, QUAD - HEAD // 2, 1),
                    pltpu.roll(value, HEAD // 2, 1),
                )
                value = value * cosine[...] + turned * sine[...]
            base = [0, 4, 8, 12, 0, 4, 0, 4][quad]
            for n in range(4):
                moved = value if n == 0 else pltpu.roll(value, QUAD - n * HEAD, 1)
                heads[base + n] = jnp.where(in_head, moved[:, :128], 0.0).astype(jnp.bfloat16)
        for src, dst in zip((q_heads, k_heads, v_heads), heads_out):
            leave(src, dst)
        out_lse[...] = jnp.zeros_like(out_lse)

    def attend(quad):
        allowed = mask[...] > 0.5
        spot = lax.broadcasted_iota(jnp.int32, (rows, 128), 1)
        total = jnp.zeros((rows, QUAD), jnp.float32)
        for n in range(4):
            query = q_heads[4 * quad + n]
            key = k_heads[2 * quad + n // 2]
            scores = lax.dot_general(
                query, key, (((1,), (1,)), ((), ())), preferred_element_type=jnp.float32
            ) * HEAD ** (-0.5)
            scores = jnp.where(allowed, scores, -1e30)
            top = jnp.max(scores, axis=-1, keepdims=True)
            size = jnp.log(jnp.sum(jnp.exp(scores - top), axis=-1, keepdims=True)) + top
            share = jnp.exp(scores - size).astype(jnp.bfloat16)
            part = jnp.dot(
                share, v_heads[2 * quad + n // 2], preferred_element_type=jnp.float32
            )
            part = jnp.concatenate([part, jnp.zeros((rows, QUAD - 128), jnp.float32)], axis=1)
            total = total + (part if n == 0 else pltpu.roll(part, n * HEAD, 1))
            out_lse[...] += jnp.where(spot == 4 * quad + n, size, 0.0)
        mixed[:, quad * QUAD : (quad + 1) * QUAD] = total.astype(jnp.bfloat16)
        span = slice(quad * QUAD, (quad + 1) * QUAD)
        out_o[span, :] = total.T.astype(jnp.bfloat16)

    def attended():
        leave(out_o, turned_o)
        leave(out_lse, lse)

    def output():
        load = fetch(1, 0, 0, w_out)
        load.wait()
        for n in range(model // TILE):
            span = pl.ds(n * TILE, TILE)
            field[:, span] += jnp.dot(
                mixed[...], w_out[:, span], preferred_element_type=jnp.float32
            )
        leave(field, middle)
        norm(1)
        out_m[...] = normed[...].astype(jnp.float32).T.astype(jnp.bfloat16)
        leave(out_m, turned_m)

    hidden_units = gate_up.shape[1] // 2
    pairs = {}

    def fetch_pair(n):
        pairs[n] = [
            fetch(2, 2 * (n % 2) + k, k * hidden_units + n * TILE, tiles.at[n % 2, k])
            for k in range(2)
        ]

    def feed(n, last):
        if n not in pairs:
            fetch_pair(n)
        if n < last:
            fetch_pair(n + 1)
        for load in pairs[n]:
            load.wait()
        slot = n % 2
        if n >= 2:
            for copy in stored[n - 2]:
                copy.wait()
        both = []
        for k in range(2):
            value = jnp.dot(normed[...], tiles[slot, k], preferred_element_type=jnp.float32)
            pre[slot, k] = value
            both.append(value)
        gate, upper = both
        hidden = gate * jax.nn.sigmoid(gate) * upper
        out_h[n * TILE : (n + 1) * TILE, :] = hidden.T.astype(jnp.bfloat16)
        stored[n] = []
        for k in range(2):
            copy = pltpu.make_async_copy(
                pre.at[slot, k],
                gate_up.at[:, pl.ds(k * hidden_units + n * TILE, TILE)],
                tile_sem.at[4 + 2 * slot + k],
            )
            copy.start()
            stored[n].append(copy)

    stored = {}
    half = hidden_units // TILE // 2
    work = {
        "begin": begin,
        "project": lambda: (projections(), rope()),
        "attend0": lambda: [attend(n) for n in range(2)],
        "attend1": lambda: ([attend(n) for n in range(2, 4)], attended()),
        "output": output,
        "feed0": lambda: [feed(n, half - 1) for n in range(half)],
        "feed1": lambda: [feed(n, 2 * half - 1) for n in range(half, 2 * half)],
    }
    phases = [Item.first, Item.relay, Item.pass_on, Item.across, Item.complete]
    for time in range(len(items) + len(phases) - 1):
        for late, phase in enumerate(phases):
            if 0 <= time - late < len(items):
                phase(items[time - late])
        for name in stages.get(time, ()):
            work[name]()
    leave(out_h, turned_h)
    for item in items:
        item.finish()
    for copies in list(stored.values())[-2:]:
        for copy in copies:
            copy.wait()
    for copy in leaving:
        copy.wait()


def gather_forward(n_shard, weights, gain, tokens, cosine, sine, mask):
    def single(weight, share):
        return round_to(weight.shape[0] // 2 * share, 16)

    qkv, out, gate_up, down = weights
    part = gate_up.shape[1] // 4
    rows, model = tokens.shape
    wide, hidden = gate_up.shape[1], gate_up.shape[1] // 2
    third = [single(weight, 0.333) for weight in weights]
    plan = [
        (0, 0, qkv.shape[1] // 2, third[0]),
        (0, qkv.shape[1] // 2, qkv.shape[1] // 2, third[0]),
        (1, 0, model, third[1]),
        (2, 0, part, third[2]),
        (2, 2 * part, part, third[2]),
        (2, part, part, third[2]),
        (2, 3 * part, part, third[2]),
        (3, 0, model // 2, third[3]),
        (3, model // 2, model // 2, third[3]),
    ]
    stages = {
        0: ["begin"],
        5: ["project"],
        6: ["attend0"],
        7: ["attend1"],
        8: ["output", "feed0"],
        10: ["feed1"],
    }
    copies = 4 * (n_shard - 1)
    n = len(plan)
    anywhere = pl.BlockSpec(memory_space=pl.ANY)
    whole = pl.BlockSpec(memory_space=pltpu.VMEM)
    bf16, f32 = jnp.bfloat16, jnp.float32
    shape = jax.ShapeDtypeStruct
    heads = lambda count: pltpu.VMEM((count, rows, 128), bf16)
    return pl.pallas_call(
        functools.partial(forward_kernel, n_shard, plan, stages),
        out_shape=[shape((w.shape[0] * n_shard, w.shape[1]), w.dtype) for w in weights]
        + [
            shape((model, rows), bf16),
            shape((model, rows), bf16),
            shape((model, rows), bf16),
            shape((hidden, rows), bf16),
            shape((rows, 128), f32),
            shape((rows, model), f32),
            shape((rows, wide), f32),
            shape((2, model), f32),
        ]
        + [shape((count, rows, 128), bf16) for count in (HEADS, KV_HEADS, KV_HEADS)],
        in_specs=[anywhere] * 4 + [whole] * 5,
        out_specs=[anywhere] * 15,
        scratch_shapes=[pltpu.VMEM(w.shape, w.dtype) for w in weights]
        + [
            pltpu.VMEM((n_shard,) + gain.shape, f32),
            pltpu.VMEM((model, qkv.shape[1]), bf16),
            pltpu.VMEM((model, model), bf16),
            pltpu.VMEM((2, 2, model, TILE), bf16),
            pltpu.VMEM((rows, model), f32),
            pltpu.VMEM((rows, model), bf16),
            pltpu.VMEM((rows, qkv.shape[1]), f32),
            heads(HEADS),
            heads(KV_HEADS),
            heads(KV_HEADS),
            pltpu.VMEM((rows, model), bf16),
            pltpu.VMEM((model, rows), bf16),
            pltpu.VMEM((model, rows), bf16),
            pltpu.VMEM((model, rows), bf16),
            pltpu.VMEM((hidden, rows), bf16),
            pltpu.VMEM((rows, 128), f32),
            pltpu.VMEM((2, model), f32),
            pltpu.VMEM((2, 2, rows, TILE), f32),
            pltpu.SemaphoreType.DMA((n,)),
            pltpu.SemaphoreType.DMA((n,)),
            pltpu.SemaphoreType.DMA((n, copies)),
            pltpu.SemaphoreType.DMA((n, copies)),
            pltpu.SemaphoreType.DMA((n_shard - 1,)),
            pltpu.SemaphoreType.DMA((n_shard - 1,)),
            pltpu.SemaphoreType.DMA((1,)),
            pltpu.SemaphoreType.DMA((8,)),
            pltpu.SemaphoreType.DMA((16,)),
        ],
        compiler_params=pltpu.CompilerParams(
            collective_id=1, has_side_effects=True, vmem_limit_bytes=66_000_000
        ),
        name="gather_forward",
    )(*weights, gain, tokens, cosine, sine, mask)


SLOTS = 5


class Pipe:
    def __init__(self, n_shard, n_replica, begin, count, block, deliver, bufs, sems, pause=(0, 0)):
        self.pause = pause
        count = count + pause[1]
        self.shard, self.replica = lax.axis_index("shard"), lax.axis_index("replica")
        chip = self.replica // 2
        self.inner = lax.rem(chip, 2) != lax.rem(chip // 2, 2)
        self.steps = n_shard.bit_length() - 1
        self.swaps = [6] + [1 << k for k in range(3, n_replica.bit_length() - 1)]
        self.begin, self.count, self.block, self.deliver = begin, count, block, deliver
        bufs = list(bufs)
        self.out = [bufs.pop(0) for _ in range(self.steps)]
        self.into = [bufs.pop(0) for _ in range(self.steps)]
        self.kept = [bufs.pop(0) for _ in range(max(1, self.steps - 1))]
        self.fold_in = bufs.pop(0)
        self.swap_out = [bufs.pop(0) for _ in self.swaps]
        self.fold_out = self.swap_out[0]
        self.swap_in = [bufs.pop(0) for _ in self.swaps]
        self.final, self.across = bufs.pop(0), bufs.pop(0)
        self.send_sem, self.recv_sem, self.local_sem = sems
        self.last = self.steps + 2 + len(self.swaps)

    @staticmethod
    def scratch(n_shard, n_replica, rows, cols, dtype):
        steps = n_shard.bit_length() - 1
        swaps = n_replica.bit_length() - 3
        blocks = [n_shard >> (k + 1) for k in range(steps)]
        shapes = [pltpu.VMEM((SLOTS, b, rows, cols), dtype) for b in blocks * 2]
        shapes += [
            pltpu.VMEM((SLOTS, max(1, b // 2), rows, cols), jnp.float32)
            for b in blocks[: max(1, steps - 1)]
        ]
        one = (SLOTS, rows, cols)
        shapes += [pltpu.VMEM(one, dtype)] * (2 * swaps + 3)
        kinds = steps + swaps + 3
        return shapes, [
            pltpu.SemaphoreType.DMA((kinds, SLOTS)),
            pltpu.SemaphoreType.DMA((kinds, SLOTS)),
            pltpu.SemaphoreType.DMA((2, SLOTS)),
        ]

    def bit(self, chunk, step):
        return 1 << lax.rem(step + lax.rem(chunk, 2), self.steps)

    def mask(self, chunk, entry):
        found = 0
        for step in range(self.steps):
            if (entry >> step) & 1:
                found = found | self.bit(chunk, step)
        return found

    def copy(self, kind, slot, src, dst, device):
        return pltpu.make_async_remote_copy(
            src_ref=src.at[slot],
            dst_ref=dst.at[slot],
            send_sem=self.send_sem.at[kind, slot],
            recv_sem=self.recv_sem.at[kind, slot],
            device_id=device,
            device_id_type=MESH,
        )

    def halving(self, step, chunk, slot):
        device = {"shard": self.shard ^ self.bit(chunk, step)}
        return self.copy(step, slot, self.out[step], self.into[step], device)

    def folding(self, slot):
        return self.copy(
            self.steps, slot, self.fold_out, self.fold_in, {"replica": self.replica ^ 2}
        )

    def swapping(self, number, slot):
        device = {"replica": self.replica ^ self.swaps[number]}
        return self.copy(
            self.steps + 1 + number, slot, self.swap_out[number], self.swap_in[number], device
        )

    def unfolding(self, slot):
        kind = self.steps + 1 + len(self.swaps)
        return self.copy(kind, slot, self.final, self.final, {"replica": self.replica ^ 2})

    def crossing(self, slot):
        kind = self.steps + 2 + len(self.swaps)
        return self.copy(kind, slot, self.final, self.across, {"replica": self.replica ^ 1})

    def stage(self, number, chunk, slot):
        steps, swaps = self.steps, len(self.swaps)
        dtype = self.final.dtype
        if number == 0:
            for entry in range(1, 1 << steps, 2):
                self.out[0][slot, entry >> 1] = self.block(chunk, self.mask(chunk, entry)).astype(dtype)
            self.halving(0, chunk, slot).start()
        elif number <= steps:
            sums = []
            for entry in range(1 << (steps - number)):
                if number == 1:
                    sums.append(self.block(chunk, self.mask(chunk, 2 * entry)))
                else:
                    sums.append(self.kept[number - 2][slot, entry])
            self.halving(number - 1, chunk, slot).wait()
            for entry, value in enumerate(sums):
                value = value + self.into[number - 1][slot, entry].astype(jnp.float32)
                if number == steps:
                    @pl.when(self.inner)
                    def _(value=value):
                        self.kept[-1][slot, 0] = value

                    @pl.when(jnp.logical_not(self.inner))
                    def _(value=value):
                        self.fold_out[slot] = value.astype(dtype)
                        self.folding(slot).start()
                elif entry & 1:
                    self.out[number][slot, entry >> 1] = value.astype(dtype)
                else:
                    self.kept[number - 1][slot, entry >> 1] = value
            if number < steps:
                self.halving(number, chunk, slot).start()
        elif number == steps + 1:
            @pl.when(self.inner)
            def _():
                self.folding(slot).wait_recv()
                value = self.kept[-1][slot, 0] + self.fold_in[slot].astype(jnp.float32)
                self.swap_out[0][slot] = value.astype(dtype)
                self.swapping(0, slot).start()

            @pl.when(jnp.logical_not(self.inner))
            def _():
                self.folding(slot).wait_send()
        elif number <= steps + 1 + swaps:
            @pl.when(self.inner)
            def _():
                done = number - steps - 2
                self.swapping(done, slot).wait()
                value = self.swap_out[done][slot].astype(jnp.float32) + self.swap_in[done][
                    slot
                ].astype(jnp.float32)
                if done + 1 < swaps:
                    self.swap_out[done + 1][slot] = value.astype(dtype)
                    self.swapping(done + 1, slot).start()
                else:
                    self.final[slot] = value.astype(dtype)
                    self.unfolding(slot).start()
        elif number == self.last:
            @pl.when(jnp.logical_not(self.inner))
            def _():
                self.unfolding(slot).wait_recv()

            self.crossing(slot).start()
            self.deliver(chunk, 0, self.final.at[slot], self.local_sem.at[0, slot], True)
        else:
            @pl.when(self.inner)
            def _():
                self.unfolding(slot).wait_send()

            self.crossing(slot).wait()
            self.deliver(chunk, 1, self.across.at[slot], self.local_sem.at[1, slot], True)
            self.deliver(chunk, 0, self.final.at[slot], self.local_sem.at[0, slot], False)
            self.deliver(chunk, 1, self.across.at[slot], self.local_sem.at[1, slot], False)

    def run(self, time):
        for number in range(self.last + 2):
            chunk = time - self.begin - number

            @pl.when((chunk >= 0) & (chunk < self.count) & self.busy(chunk))
            def _(number=number, chunk=chunk):
                self.stage(number, chunk, lax.rem(chunk, SLOTS))

    def busy(self, chunk):
        first, skip = self.pause
        return (chunk < first) | (chunk >= first + skip)

    def number(self, chunk):
        first, skip = self.pause
        return chunk - jnp.where(chunk < first, 0, skip)

    def length(self):
        return self.begin + self.count + self.last + 1


DEEP_COLS = 128
WIDE_COLS = 256
EARLY = 16


def times_rows(left, right):
    return lax.dot_general(
        left, right, (((0,), (0,)), ((), ())), preferred_element_type=jnp.float32
    )


def times_cols(left, right):
    return lax.dot_general(
        left, right, (((1,), (1,)), ((), ())), preferred_element_type=jnp.float32
    )


def backward_kernel(n_shard, n_replica, *refs):
    refs = list(refs)
    take = lambda n: [refs.pop(0) for _ in range(n)]
    lefts, (w_down, w_gate_up, w_out, w_qkv, pre) = take(4), take(5)
    heads_in, middle_in = take(3), take(1)[0]
    grad_last, tokens, gain, lse, cosine, sine, mask, live = take(8)
    outs, (gain_out, grad_tokens, result) = take(4), take(3)
    deep_left, deep_right, wide_left, wide_right, other_right = take(5)
    tile_down, tile_up, tile_pre, tile_out = take(4)
    q_heads, k_heads, v_heads, middle, grad_middle, total, branch, joined, parts, gain_in = take(10)
    load_sem, pass_send, pass_recv, tile_send, tile_recv, tile_sem, head_sem, late_sem = take(8)
    n_bufs = (len(refs) - 9) // 3
    deep_bufs, deep_sems = take(n_bufs), take(3)
    wide_bufs, wide_sems = take(n_bufs), take(3)
    gain_bufs, gain_sems = take(n_bufs), take(3)
    shard, replica = lax.axis_index("shard"), lax.axis_index("replica")
    core = lax.rem(replica, 2)
    rows, model = grad_last.shape
    hidden = w_down.shape[0]
    wide = w_qkv.shape[1]
    deep_rows, wide_rows = outs[0].shape[0] // 2, outs[1].shape[0]
    halves = [model // 2, hidden, model // 2, wide // 2]
    starts = [0, 0, hidden, hidden + model // 2]
    n_deep = 2 * halves[0] // DEEP_COLS
    edges = [start // WIDE_COLS for start in starts[1:]] + [wide_right.shape[1] // WIDE_COLS]
    tile = hidden // EARLY
    twin = {"replica": replica ^ 1}

    greet(
        [{"shard": shard ^ (1 << k)} for k in range(n_shard.bit_length() - 1)]
        + [{"replica": replica ^ other} for other in [1, 2, 6]]
        + [{"replica": replica ^ (1 << k)} for k in range(3, n_replica.bit_length() - 1)]
    )

    def pass_over(src, dst, sems, index):
        return pltpu.make_async_remote_copy(
            src_ref=src,
            dst_ref=dst,
            send_sem=sems[0].at[index],
            recv_sem=sems[1].at[index],
            device_id=twin,
            device_id_type=MESH,
        )

    def half_of(which, side):
        return pl.ds(pl.multiple_of(side * halves[which], 128), halves[which])

    place_left = [deep_left] + [wide_left.at[pl.ds(k * model, model)] for k in range(3)]
    loads, passes = [], []
    for k in range(4):
        loads.append(
            pltpu.make_async_copy(lefts[k], place_left[k].at[:, pl.ds(0, rows)], load_sem.at[k])
        )
        passes.append(
            pass_over(lefts[k], place_left[k].at[:, pl.ds(rows, rows)], (pass_send, pass_recv), k)
        )
        if k == 0:
            passes.append(
                pass_over(
                    grad_last.at[:, half_of(0, 1 - core)],
                    deep_right.at[pl.ds(rows, rows)],
                    (pass_send, pass_recv),
                    4,
                )
            )
    for copy in loads + passes:
        copy.start()
    late = [
        pltpu.make_async_copy(src, dst, late_sem.at[n])
        for n, (src, dst) in enumerate(
            zip([*heads_in, middle_in], [q_heads, k_heads, v_heads, middle])
        )
    ]
    for copy in late:
        copy.start()
    deep_right[pl.ds(0, rows), :] = grad_last[:, half_of(0, core)]
    total[...] = jnp.zeros_like(total)
    grad_middle[...] = jnp.zeros_like(grad_middle)
    gain_in[...] = jnp.zeros_like(gain_in)
    tile_out[...] = jnp.zeros_like(tile_out)

    def tile_copies(n, slot):
        start = pl.multiple_of(n * tile, tile)
        cols = [pl.ds(start, tile), pl.ds(pl.multiple_of(hidden + n * tile, tile), tile)]
        pairs = [(w_down.at[cols[0]], tile_down.at[slot])]
        for k in range(2):
            pairs.append((w_gate_up.at[:, cols[k]], tile_up.at[slot, k]))
            pairs.append((pre.at[:, cols[k]], tile_pre.at[slot, k]))
        return [
            pltpu.make_async_copy(src, dst, tile_sem.at[slot, k])
            for k, (src, dst) in enumerate(pairs)
        ]

    def tile_pass(n):
        span = pl.ds(pl.multiple_of(n * tile, tile), tile)
        return pass_over(
            other_right.at[lax.rem(n, 4)],
            wide_right.at[pl.ds(rows, rows), span],
            (tile_send, tile_recv),
            n,
        )

    def hidden_tile(n):
        slot = lax.rem(n, 2)

        @pl.when(n + 1 < EARLY)
        def _():
            for copy in tile_copies(n + 1, 1 - slot):
                copy.start()

        for copy in tile_copies(n, slot):
            copy.wait()
        grad_hidden = times_cols(grad_last[...], tile_down[slot])
        grad_gate, grad_upper = gate_back(grad_hidden, tile_pre[slot, 0], tile_pre[slot, 1])
        span = pl.ds(pl.multiple_of(n * tile, tile), tile)
        first = core == 0
        wide_right[pl.ds(0, rows), span] = jnp.where(first, grad_gate, grad_upper)

        @pl.when(n >= 4)
        def _():
            tile_pass(n - 4).wait_send()

        other_right[lax.rem(n, 4)] = jnp.where(first, grad_upper, grad_gate)
        tile_pass(n).start()
        total[...] += times_cols(grad_gate, tile_up[slot, 0]) + times_cols(
            grad_upper, tile_up[slot, 1]
        )
        grad_middle[...] += times_rows(deep_left[span, pl.ds(0, rows)], tile_down[slot])

    showing = pltpu.make_async_copy(joined.at[:, pl.ds(0, model)], result, late_sem.at[4])

    def norm_gradient(field, row):
        scale = lax.rsqrt(jnp.mean(field * field, axis=-1, keepdims=True) + epsilon)
        normed = field * scale
        grad = total[...]
        sums = jnp.sum(grad * normed, axis=0, keepdims=True)
        for other in range(n_shard):
            gain_in[other, row : row + 1, :] = sums[:, other * wide_rows : (other + 1) * wide_rows]
        inner = grad * gain[row : row + 1, :]
        return scale * (inner - normed * jnp.mean(inner * normed, axis=-1, keepdims=True))

    def share_right(which, source, index):
        span = pl.ds(starts[which], halves[which])
        wide_right[pl.ds(0, rows), span] = source[:, half_of(which, core)]
        return pass_over(
            source.at[:, half_of(which, 1 - core)],
            wide_right.at[pl.ds(rows, rows), span],
            (pass_send, pass_recv),
            index,
        )

    def between():
        for copy in late:
            copy.wait()
        for n in range(EARLY - 4, EARLY):
            tile_pass(n).wait_send()
        joined[:, :model] = ((middle[...] + grad_middle[...]) * live[...]).astype(jnp.bfloat16)
        showing.start()
        grad_middle[...] = grad_last[...].astype(jnp.float32) + norm_gradient(middle[...], 1)
        branch[...] = grad_middle[...].astype(jnp.bfloat16)
        share_right(2, branch, 5).start()
        total[...] = jnp.zeros_like(total)
        for copy in qkv_copies(0, 0):
            copy.start()

    per = HEADS // KV_HEADS

    def head_copies(key_head, slot):
        return [
            pltpu.make_async_copy(
                w_out.at[pl.ds(pl.multiple_of((per * key_head + n) * HEAD, 32), HEAD)],
                tile_out.at[slot, n, pl.ds(0, HEAD)],
                head_sem.at[slot, n],
            )
            for n in range(per)
        ]

    spot = lax.broadcasted_iota(jnp.int32, (rows, 128), 1)

    def unrope(value):
        moved = value * sine[...]
        turned = jnp.where(
            spot < HEAD // 2,
            -pltpu.roll(moved, 128 - HEAD // 2, 1),
            pltpu.roll(moved, HEAD // 2, 1),
        )
        return jnp.where(spot < HEAD, value * cosine[...] - turned, 0.0).astype(jnp.bfloat16)

    def attention(key_head):
        slot = lax.rem(key_head, 2)

        @pl.when(key_head + 1 < KV_HEADS)
        def _():
            for copy in head_copies(key_head + 1, 1 - slot):
                copy.start()

        for copy in head_copies(key_head, slot):
            copy.wait()
        allowed = mask[...] > 0.5
        factor = HEAD ** (-0.5)
        key, value = k_heads[key_head], v_heads[key_head]
        grad_key = jnp.zeros((rows, 128), jnp.float32)
        grad_value = jnp.zeros((rows, 128), jnp.float32)
        for n in range(per):
            head = per * key_head + n
            query = q_heads[head]
            grad_mixed = times_cols(branch[...], tile_out[slot, n]).astype(jnp.bfloat16)
            size = jnp.sum(jnp.where(spot == head, lse[...], 0.0), axis=-1, keepdims=True)
            scores = jnp.where(allowed, times_cols(query, key) * factor, -1e30)
            share = jnp.exp(scores - size)
            grad_value = grad_value + times_rows(share.astype(jnp.bfloat16), grad_mixed)
            grad_share = times_cols(grad_mixed, value)
            inner = jnp.sum(share * grad_share, axis=-1, keepdims=True)
            grad_scores = (share * (grad_share - inner)).astype(jnp.bfloat16)
            grad_query = jnp.dot(grad_scores, key, preferred_element_type=jnp.float32) * factor
            parts[head] = unrope(grad_query)
            grad_key = grad_key + times_rows(grad_scores, query)
        parts[HEADS + key_head] = unrope(grad_key * factor)
        parts[HEADS + KV_HEADS + key_head] = grad_value.astype(jnp.bfloat16)

    quad = 4 * HEAD

    def join():
        showing.wait()
        for group in range(wide // quad):
            value = jnp.zeros((rows, quad), jnp.float32)
            for n in range(4):
                part = parts[4 * group + n].astype(jnp.float32)
                part = jnp.concatenate([part, jnp.zeros((rows, quad - 128), jnp.float32)], axis=1)
                value = value + (part if n == 0 else pltpu.roll(part, n * HEAD, 1))
            joined[:, group * quad : (group + 1) * quad] = value.astype(jnp.bfloat16)
        share_right(3, joined, 6).start()

    n_last = wide // (2 * tile)

    def qkv_copies(n, slot):
        return [
            pltpu.make_async_copy(
                w_qkv.at[:, pl.ds(pl.multiple_of((2 * n + k) * tile, tile), tile)],
                tile_up.at[slot, k],
                tile_sem.at[slot, k],
            )
            for k in range(2)
        ]

    def input_tile(n):
        slot = lax.rem(n, 2)

        @pl.when(n + 1 < n_last)
        def _():
            for copy in qkv_copies(n + 1, 1 - slot):
                copy.start()

        for copy in qkv_copies(n, slot):
            copy.wait()
        for k in range(2):
            span = pl.ds(pl.multiple_of((2 * n + k) * tile, tile), tile)
            total[...] += times_cols(joined[:, span], tile_up[slot, k])

    def end():
        grad_tokens[...] = grad_middle[...] + norm_gradient(tokens[...].astype(jnp.float32), 0)

    def deep_block(chunk, other):
        chunk = deep.number(chunk)
        start = (shard ^ other) * (2 * deep_rows) + (chunk // (n_deep // 2)) * deep_rows
        left = deep_left[pl.ds(pl.multiple_of(start, 16), deep_rows), :]
        cols = lax.rem(chunk, n_deep // 2) * DEEP_COLS
        right = deep_right[:, pl.ds(pl.multiple_of(cols, 128), DEEP_COLS)]
        return jnp.dot(left, right, preferred_element_type=jnp.float32)

    def wide_block(chunk, other):
        weight = (chunk >= edges[1]).astype(jnp.int32) + (chunk >= edges[2]).astype(jnp.int32)
        start = weight * model + (shard ^ other) * wide_rows
        left = wide_left[pl.ds(pl.multiple_of(start, 16), wide_rows), :]
        right = wide_right[:, pl.ds(pl.multiple_of(chunk * WIDE_COLS, 128), WIDE_COLS)]
        return jnp.dot(left, right, preferred_element_type=jnp.float32)

    def put(out, span, start, size, src, sem, begin):
        copy = pltpu.make_async_copy(
            src, out.at[span, pl.ds(pl.multiple_of(start, 128), size)], sem
        )
        if begin:
            copy.start()
        else:
            copy.wait()

    def deep_deliver(chunk, side, src, sem, begin):
        chunk = deep.number(chunk)
        half = core if side == 0 else 1 - core
        first = pl.multiple_of((chunk // (n_deep // 2)) * deep_rows, 16)
        start = half * halves[0] + lax.rem(chunk, n_deep // 2) * DEEP_COLS
        put(outs[0], pl.ds(first, deep_rows), start, DEEP_COLS, src, sem, begin)

    def wide_deliver(chunk, side, src, sem, begin):
        half = core if side == 0 else 1 - core
        for k in range(3):
            @pl.when((chunk >= edges[k]) & (chunk < edges[k + 1]))
            def _(k=k):
                start = half * halves[k + 1] + (chunk - edges[k]) * WIDE_COLS
                put(outs[k + 1], slice(None), start, WIDE_COLS, src, sem, begin)

    def gain_deliver(chunk, side, src, sem, begin):
        if side == 1 and begin:
            gain_out[...] = gain_pipe.final[0] + src[...]

    between_at = EARLY
    join_at = between_at + 1 + KV_HEADS
    end_at = join_at + 1 + n_last
    size = (n_shard, n_replica)
    wide_at = 2 * n_deep // 3
    deep = Pipe(
        *size, 0, n_deep, deep_block, deep_deliver, deep_bufs, deep_sems, (wide_at, edges[3])
    )
    wide_pipe = Pipe(
        *size, wide_at, edges[3], wide_block, wide_deliver, wide_bufs, wide_sems
    )
    gain_pipe = Pipe(
        *size, end_at + 1, 1, lambda chunk, other: gain_in[shard ^ other], gain_deliver, gain_bufs, gain_sems
    )
    for copy in tile_copies(0, 0):
        copy.start()
    for copy in head_copies(0, 0):
        copy.start()
    loads[0].wait()
    passes[0].wait()
    passes[1].wait()

    def step(time, carry):
        def at(first, count, run):
            @pl.when((time >= first) & (time < first + count))
            def _():
                run(time - first)

        @pl.when(time == wide_at)
        def _():
            for k in range(1, 4):
                loads[k].wait()
                passes[k + 1].wait()

        at(wide_at, EARLY, lambda n: tile_pass(n).wait_recv())
        at(wide_at + edges[1], 1, lambda n: share_wait(2, branch, 5))
        at(wide_at + edges[2], 1, lambda n: share_wait(3, joined, 6))
        deep.run(time)
        wide_pipe.run(time)
        gain_pipe.run(time)
        at(0, EARLY, hidden_tile)
        at(between_at, 1, lambda n: between())
        at(between_at + 1, KV_HEADS, attention)
        at(join_at, 1, lambda n: join())
        at(join_at + 1, n_last, input_tile)
        at(end_at, 1, lambda n: end())
        return carry

    def share_wait(which, source, index):
        span = pl.ds(starts[which], halves[which])
        pass_over(
            source.at[:, half_of(which, 1 - core)],
            wide_right.at[pl.ds(rows, rows), span],
            (pass_send, pass_recv),
            index,
        ).wait()

    lax.fori_loop(0, max(deep.length(), wide_pipe.length(), gain_pipe.length()), step, 0)


def backward_all(n_shard, n_replica, lefts, weights, pre, heads, middle, small):
    grad_last, tokens, gain, lse = small[:4]
    rows, model = grad_last.shape
    w_down, w_gate_up, w_out, w_qkv = weights
    hidden, wide = w_down.shape[0], w_qkv.shape[1]
    tile = hidden // EARLY
    owned = [w.shape[0] // n_shard for w in weights]
    anywhere = pl.BlockSpec(memory_space=pl.ANY)
    whole = pl.BlockSpec(memory_space=pltpu.VMEM)
    bf16, f32 = jnp.bfloat16, jnp.float32
    size = (n_shard, n_replica)
    deep_bufs, deep_sems = Pipe.scratch(*size, owned[0] // 2, DEEP_COLS, bf16)
    wide_bufs, wide_sems = Pipe.scratch(*size, owned[1], WIDE_COLS, bf16)
    gain_bufs, gain_sems = Pipe.scratch(*size, 8, owned[1], f32)
    dma = pltpu.SemaphoreType.DMA
    return pl.pallas_call(
        functools.partial(backward_kernel, n_shard, n_replica),
        out_shape=[
            jax.ShapeDtypeStruct((own, w.shape[1]), bf16) for own, w in zip(owned, weights)
        ]
        + [
            jax.ShapeDtypeStruct((8, owned[1]), f32),
            jax.ShapeDtypeStruct((rows, model), f32),
            jax.ShapeDtypeStruct((rows, model), bf16),
        ],
        in_specs=[anywhere] * 13 + [whole] * 8,
        out_specs=[anywhere] * 4 + [whole] * 2 + [anywhere],
        scratch_shapes=[
            pltpu.VMEM((hidden, 2 * rows), bf16),
            pltpu.VMEM((2 * rows, model // 2), bf16),
            pltpu.VMEM((3 * model, 2 * rows), bf16),
            pltpu.VMEM((2 * rows, hidden + model // 2 + wide // 2), bf16),
            pltpu.VMEM((4, rows, tile), bf16),
            pltpu.VMEM((2, tile, model), bf16),
            pltpu.VMEM((2, 2, model, tile), bf16),
            pltpu.VMEM((2, 2, rows, tile), f32),
            pltpu.VMEM((2, HEADS // KV_HEADS, 128, model), bf16),
            pltpu.VMEM((HEADS, rows, 128), bf16),
            pltpu.VMEM((KV_HEADS, rows, 128), bf16),
            pltpu.VMEM((KV_HEADS, rows, 128), bf16),
            pltpu.VMEM((rows, model), f32),
            pltpu.VMEM((rows, model), f32),
            pltpu.VMEM((rows, model), f32),
            pltpu.VMEM((rows, model), bf16),
            pltpu.VMEM((rows, wide), bf16),
            pltpu.VMEM((HEADS + 2 * KV_HEADS, rows, 128), bf16),
            pltpu.VMEM((n_shard, 8, owned[1]), f32),
            dma((4,)),
            dma((7,)),
            dma((7,)),
            dma((EARLY,)),
            dma((EARLY,)),
            dma((2, 5)),
            dma((2, HEADS // KV_HEADS)),
            dma((5,)),
            *deep_bufs,
            *deep_sems,
            *wide_bufs,
            *wide_sems,
            *gain_bufs,
            *gain_sems,
        ],
        compiler_params=pltpu.CompilerParams(
            collective_id=2, has_side_effects=True, vmem_limit_bytes=67_043_328
        ),
        name="backward_reduce",
    )(*lefts, *weights, pre, *heads, middle, *small)


def body(
    n_shard,
    n_replica,
    tokens,
    cotangent,
    seq_lengths,
    seq_device,
    seq_offsets,
    norm_attn,
    w_qkv,
    w_out,
    norm_mlp,
    w_gate_up,
    w_down,
):
    rows, model = tokens.shape
    w_qkv, w_out, w_gate_up, w_down = w_qkv[0], w_out[0], w_gate_up[0], w_down[0]
    owned_rows = w_qkv.shape[0]

    device = lax.axis_index(("shard", "replica"))
    segment, position = locate(device, seq_lengths, seq_device, seq_offsets, rows)
    live = (segment >= 0).astype(jnp.float32)[:, None]
    cosine, sine = rope_tables(position)
    allowed = mask_of(segment)

    cosine, sine = jnp.tile(cosine, (1, 4)), jnp.tile(sine, (1, 4))
    allowed = allowed.astype(jnp.float32)
    (
        w_qkv,
        w_out,
        w_gate_up,
        w_down,
        normed_a,
        mixed,
        normed_m,
        hidden,
        lse,
        middle,
        pre,
        gains,
        *heads,
    ) = gather_forward(
        n_shard,
        (w_qkv, w_out, w_gate_up, w_down),
        jnp.concatenate([norm_attn, norm_mlp], axis=0).astype(jnp.float32),
        tokens,
        cosine,
        sine,
        allowed,
    )
    grad_last = (cotangent.astype(jnp.float32) * live).astype(jnp.bfloat16)
    grad_down, grad_gate_up, grad_out, grad_qkv, gain_own, grad_tokens, result = backward_all(
        n_shard,
        n_replica,
        [hidden, normed_m, mixed, normed_a],
        [w_down, w_gate_up, w_out, w_qkv],
        pre,
        heads,
        middle,
        [grad_last, tokens, gains, lse, cosine[:, :128], sine[:, :128], allowed, live],
    )
    grad_down, grad_gate_up, grad_qkv, grad_out = [
        grad.astype(jnp.float32) for grad in (grad_down, grad_gate_up, grad_qkv, grad_out)
    ]
    return (
        result,
        grad_tokens,
        gain_own[0:1],
        grad_qkv[None],
        grad_out[None],
        gain_own[1:2],
        grad_gate_up[None],
        grad_down[None],
    )


def solution(mesh):
    n_shard = mesh.shape["shard"]
    n_replica = mesh.shape["replica"]
    placed = (
        P(("shard", "replica"), None),
        P(("shard", "replica"), None),
        P(),
        P(),
        P(),
        P(None, "shard"),
        P(None, "shard", None),
        P(None, "shard", None),
        P(None, "shard"),
        P(None, "shard", None),
        P(None, "shard", None),
    )

    def run(*args):
        return body(n_shard, n_replica, *args)

    return jax.shard_map(
        run,
        mesh=mesh,
        in_specs=placed,
        out_specs=(
            P(("shard", "replica"), None),
            P(("shard", "replica"), None),
            P(None, "shard"),
            P(None, "shard", None),
            P(None, "shard", None),
            P(None, "shard"),
            P(None, "shard", None),
            P(None, "shard", None),
        ),
        check_vma=False,
    )
```
